32 devices in a mesh: dp: 32 (over z, y, x, core), feat: 1.
Axes of the slice: x: 2, y: 2, z: 4, core: 2. Of those that a mesh axis runs over, the one named last changes fastest.
Arguments:
- grads: bfloat16 [16384, 4096], P('dp', 'feat'), may hold values from -6 to 6
- covariance: float32 [4096, 4096], P('dp', 'feat'), may hold values from -0.16 to 6, as said below
- test_grads: bfloat16 [512, 4096], P('feat', 'dp'), may hold values from -0.09375 to 0.09375
- inverse_factor: bfloat16 [4096, 4096], P('dp'), may hold values from -0.09375 to 0.09375
Outputs:
- scores: float32 [16384, 512], P('dp', 'feat')
- covariance_out: float32 [4096, 4096], P('dp', 'feat')
The draws below stay inside these ranges and needn't reach their ends.
Inputs may be any that keep to these rules, and one draw needn't show every extreme that they name: covariance is symmetric.
All inputs are finite; a program needn't handle non-finite values.
Results may differ from the reference program's by a relative error of at most 0.0029.
Values may be sent and summed in bfloat16 or wider, within the bound.
A program may use at most 256 MiB of HBM per device.

```python
import jax
import jax.numpy as jnp

K = 4096
M = 512
TOKENS = 16384


def draw_covariance(key, part):
    base_key = jax.random.fold_in(key, 11)
    noise_key, diag_key = jax.random.split(base_key, 2)
    noise = jnp.clip(jax.random.normal(noise_key, (K, K), jnp.float32) * 0.007, -0.04, 0.04)
    symmetric = (noise + noise.T) * 0.5
    identity_mat = jnp.eye(K, dtype=jnp.float32)
    diagonal = jax.random.uniform(diag_key, (K,), jnp.float32, 0.5, 1.5)
    result = symmetric * (1.0 - identity_mat) + identity_mat * diagonal[None, :]
    return result


def strengthened(drawn, own_key, source, target, blocks, factor):
    owner, partner = [(jnp.arange(drawn.shape[dim]) // (drawn.shape[dim] // blocks)).reshape([-1 if axis == dim else 1 for axis in range(drawn.ndim)]) for dim in (source, target)]
    chosen = jax.random.permutation(own_key, blocks)[partner]
    strong = (owner == chosen) | (owner == (partner + blocks // 2) % blocks)
    return jnp.where(strong, factor * drawn, drawn)


def shard_levels(key, dims, shards, low, largest):
    gain = 1.0
    for dim, parts in shards:
        steps = jax.random.uniform(jax.random.fold_in(jax.random.fold_in(key, 6), dim), (parts,), jnp.float32, low / len(shards), largest / len(shards))
        gain = gain * jnp.repeat(jnp.exp(steps), dims[dim] // parts).reshape((-1,) + (1,) * (len(dims) - 1 - dim))
    return gain


def scatter_about(own_key, dims, deviation, bound, shards=(), kind=jnp.bfloat16):
    values = deviation * jax.random.normal(own_key, dims, jnp.float32)
    if shards:
        values = values * shard_levels(own_key, dims, shards, -0.22, 0.18)
    return jnp.clip(values, -bound, bound).astype(kind)


def gaussian_with(stream_key, shape, spread, most, cuts, heavy, held_as=jnp.bfloat16):
    drawn = spread * jax.random.normal(stream_key, shape, jnp.float32)
    if cuts:
        drawn = drawn * shard_levels(stream_key, shape, cuts, -0.22, 0.18)
    return jnp.clip(strengthened(drawn, jax.random.fold_in(stream_key, 3), *heavy), -most, most).astype(held_as)


def setup_inputs(seed: int = 0) -> dict:
    seeds = jax.random.split(jax.random.key(seed), 5)
    grads = gaussian_with(seeds[0], (TOKENS, K), 1.0, 6.0, ((0, 32),), (0, 1, 32, 2.75))
    covariance = draw_covariance(jax.random.fold_in(seeds[4], 71), 0)
    test_grads = scatter_about(seeds[2], (M, K), K ** -0.5, 0.09375, ((1, 32),))
    inverse_factor = scatter_about(seeds[3], (K, K), K ** -0.5, 0.09375, ((0, 32),))
    return {"grads": grads, "covariance": covariance, "test_grads": test_grads, "inverse_factor": inverse_factor}


def reference(grads, covariance, test_grads, inverse_factor):
    term = jnp.dot(grads.T, grads, preferred_element_type=jnp.float32)
    covariance_out = 0.9 * covariance + term / TOKENS
    preconditioned = jnp.dot(test_grads, inverse_factor, preferred_element_type=jnp.float32).astype(jnp.bfloat16)
    scores = jnp.dot(grads, preconditioned.T, preferred_element_type=jnp.float32)
    return scores, covariance_out
```

```python
import functools

import jax
import jax.numpy as jnp
from jax import lax
from jax.experimental import pallas as pl
from jax.experimental.pallas import tpu as pltpu
from jax.sharding import PartitionSpec as P

F32 = jnp.float32
BF16 = jnp.bfloat16
MESH = pl.DeviceIdType.MESH


def general(grads, covariance, test_grads, inverse_factor):
    all_features = lax.all_gather(grads, "feat", axis=1, tiled=True)
    examples = grads.shape[0] * lax.axis_size("dp")
    tested = lax.dot_general(
        inverse_factor, test_grads, (((0,), (1,)), ((), ())), preferred_element_type=F32
    )
    term = lax.dot_general(
        all_features, grads, (((0,), (0,)), ((), ())), preferred_element_type=F32
    )
    joined = lax.psum_scatter(
        jnp.concatenate([term, tested], axis=1), "dp", scatter_dimension=0, tiled=True
    )
    width = grads.shape[1]
    owned_pre = joined[:, width:].astype(BF16)
    pre_columns = lax.all_gather(owned_pre, "dp", axis=0, tiled=True)
    scores = jnp.dot(all_features, pre_columns, preferred_element_type=F32)
    return scores, 0.9 * covariance + joined[:, :width] / examples


class Sizes:
    def __init__(self, n, rows, k, tests):
        self.n, self.rows, self.k, self.tests = n, rows, k, tests
        self.chips, self.far, self.w = n // 2, n // 8, k // n
        self.W = 2 * self.w
        self.half = self.chips // 2
        self.each = self.half // 2
        self.ra = self.each // 2 * self.W
        self.rb = (self.each - self.each // 2) * self.W + self.w // 2
        self.mh = tests // 2

    def scratch(self):
        far, w, W, tests = self.far, self.w, self.W, self.tests
        far1 = max(far - 1, 1)
        v = pltpu.VMEM
        return dict(
            gbuf=v((2 * self.rows, self.k), BF16),
            gt=v((W, 2 * self.rows), BF16),
            tmp=v((self.ra + self.rb, W), F32),
            part_a=v((far, 2, self.ra, W), F32),
            part_b=v((far, 2, self.rb, W), F32),
            out_a1=v((far, 2, self.ra, W), BF16),
            out_b1=v((far, 2, self.rb, W), BF16),
            in_a1=v((far, 2, self.ra, W), BF16),
            in_b1=v((far, 2, self.rb, W), BF16),
            out_a2=v((far, self.ra, W), BF16),
            out_b2=v((far, self.rb, W), BF16),
            in_a2=v((far, self.ra, W), BF16),
            in_b2=v((far, self.rb, W), BF16),
            out_az=v((far1, self.ra, W), BF16),
            out_bz=v((far1, self.rb, W), BF16),
            in_az=v((far1, self.ra, W), BF16),
            in_bz=v((far1, self.rb, W), BF16),
            fbuf=v((2 * far * w, 4 * w), BF16),
            tbuf=v((tests, 2 * far * w), BF16),
            pp=v((tests, 4 * w), F32),
            in_p1=v((2, 2, self.mh, w), F32),
            out_p2=v((2, self.mh, w), F32),
            in_p2=v((2, self.mh, w), F32),
            pfull=v((tests, self.k), BF16),
            msend=v((self.each, W, W), BF16),
            mrecv=v((self.half, w, W), BF16),
            xsend=v((w, w), BF16),
            xrecv=v((w, w), BF16),
            dsend=v((w, self.each * W), BF16),
            drecv=v((w, self.each * W), BF16),
            ssem=pltpu.SemaphoreType.DMA((self.slots(),)),
            rsem=pltpu.SemaphoreType.DMA((self.slots(),)),
            msem=pltpu.SemaphoreType.DMA((2 * self.each,)),
            mrsem=pltpu.SemaphoreType.DMA((self.half,)),
            lsem=pltpu.SemaphoreType.DMA((4,)),
        )

    def slots(self):
        return 4 + 2 * self.far + 2 * self.far + 8 * self.far + 2 * self.far + 6 + 6 * self.far + 2 + 32


def kernel(s, names, g_hbm, t_hbm, f_hbm, term_ref, scores_ref, *refs):
    r = dict(zip(names, refs))
    n, far, w, W, chips, half, each = s.n, s.far, s.w, s.W, s.chips, s.half, s.each
    rows, mh, ra, rb = s.rows, s.mh, s.ra, s.rb
    me = lax.axis_index("dp")
    core, x, y, z = me % 2, me // 2 % 2, me // 4 % 2, me // 8
    q = me // 2

    def device(zz, yy, xx, cc):
        return ((zz * 2 + yy) * 2 + xx) * 2 + cc

    def up(g):
        return (z + g) % far

    def down(g):
        return (z + far - g) % far

    mate = device(z, y, x, 1 - core)
    x_to = device(z, y, 1 - x, core)
    y_to = device(z, 1 - y, x, core)
    ssem, rsem = r["ssem"], r["rsem"]
    started = []
    count = [0]

    def to(src, dst, target):
        i = count[0]
        count[0] += 1
        copy = pltpu.make_async_remote_copy(
            src_ref=src, dst_ref=dst, send_sem=ssem.at[i], recv_sem=rsem.at[i],
            device_id={"dp": target}, device_id_type=MESH,
        )
        copy.start()
        started.append(copy)
        return copy

    def lanes(block, width):
        return pl.ds(pl.multiple_of(block * width, width), width)

    barrier = pltpu.get_barrier_semaphore()

    def greet(i, carry):
        pl.semaphore_signal(barrier, inc=1, device_id={"dp": (me + i) % n}, device_id_type=MESH)
        return carry

    lax.fori_loop(1, n, greet, 0)
    pl.semaphore_wait(barrier, n - 1)

    gbuf, fbuf, tbuf = r["gbuf"], r["fbuf"], r["tbuf"]
    quarter = rows // 4
    g_copies = [
        to(g_hbm.at[pl.ds(i * quarter, quarter)], gbuf.at[pl.ds(rows + i * quarter, quarter)], mate)
        for i in range(4)
    ]
    g_own = pltpu.make_async_copy(g_hbm, gbuf.at[pl.ds(0, rows)], r["lsem"].at[0])
    g_own.start()
    t_own = pltpu.make_async_copy(t_hbm, tbuf.at[:, pl.ds(0, w)], r["lsem"].at[1])
    t_own.start()
    f_own = pltpu.make_async_copy(
        f_hbm.at[:, lanes(core * far + z, 4 * w)], fbuf.at[pl.ds(0, w)], r["lsem"].at[2]
    )
    f_own.start()
    t_copies = [
        to(t_hbm, tbuf.at[:, pl.ds(2 * g * w, w)], device(up(g), y, x, core)) for g in range(1, far)
    ]
    f_copies = [
        to(
            f_hbm.at[:, lanes((core + h) % 2 * far + up(g), 4 * w)],
            fbuf.at[pl.ds((2 * g + h) * w, w)],
            device(up(g), y, x, (core + h) % 2),
        )
        for g in range(far)
        for h in range(2)
        if g or h
    ]

    gt, tmp = r["gt"], r["tmp"]
    part_a, part_b, out_a1, out_b1 = r["part_a"], r["part_b"], r["out_a1"], r["out_b1"]

    def compute(g):
        def strip(u, carry):
            oy, ox = u // 2, u % 2
            own = (up(g) * 2 + (y + oy) % 2) * 2 + (x + ox) % 2
            gt[...] = gbuf[:, lanes(own, W)].T
            for e in range(each):
                col = (own + core * each + e) % chips
                tmp[e * W : (e + 1) * W] = jnp.dot(
                    gt[...], gbuf[:, lanes(col, W)], preferred_element_type=F32
                )
            col = 2 * ((own + half) % chips) + (core + own // half) % 2
            extra = jnp.dot(
                gt[pl.ds(pl.multiple_of(core * w, w), w), :], gbuf[:, lanes(col, w)],
                preferred_element_type=F32,
            )
            tmp[each * W :, :w] = extra[: w // 2]
            tmp[each * W :, w:] = extra[w // 2 :]

            @pl.when(ox == 0)
            def _():
                part_a[g, oy] = tmp[:ra]

            @pl.when(ox == 1)
            def _():
                out_a1[g, oy] = tmp[:ra].astype(BF16)

            @pl.when(oy == 0)
            def _():
                part_b[g, ox] = tmp[ra:]

            @pl.when(oy == 1)
            def _():
                out_b1[g, ox] = tmp[ra:].astype(BF16)

            return carry

        lax.fori_loop(0, 4, strip, 0)

    a1, b1, a2, b2, az, bz = {}, {}, {}, {}, {}, {}

    def first(g, o):
        a1[g, o] = to(out_a1.at[g, o], r["in_a1"].at[g, o], x_to)
        b1[g, o] = to(out_b1.at[g, o], r["in_b1"].at[g, o], y_to)

    def second(g):
        a1[g, 1].wait_recv()
        r["out_a2"][g] = (part_a[g, 1] + r["in_a1"][g, 1].astype(F32)).astype(BF16)
        a2[g] = to(r["out_a2"].at[g], r["in_a2"].at[g], y_to)
        b1[g, 1].wait_recv()
        r["out_b2"][g] = (part_b[g, 1] + r["in_b1"][g, 1].astype(F32)).astype(BF16)
        b2[g] = to(r["out_b2"].at[g], r["in_b2"].at[g], x_to)

    def third(g):
        a1[g, 0].wait_recv()
        a2[g].wait_recv()
        total = part_a[g, 0] + r["in_a1"][g, 0].astype(F32) + r["in_a2"][g].astype(F32)
        if g:
            r["out_az"][g - 1] = total.astype(BF16)
            az[g] = to(r["out_az"].at[g - 1], r["in_az"].at[g - 1], device(up(g), y, x, core))
        else:
            part_a[0, 0] = total
        b1[g, 0].wait_recv()
        b2[g].wait_recv()
        total = part_b[g, 0] + r["in_b1"][g, 0].astype(F32) + r["in_b2"][g].astype(F32)
        if g:
            r["out_bz"][g - 1] = total.astype(BF16)
            bz[g] = to(r["out_bz"].at[g - 1], r["in_bz"].at[g - 1], device(up(g), y, x, core))
        else:
            part_b[0, 0] = total

    pp, in_p1, out_p2, in_p2, pfull = r["pp"], r["in_p1"], r["out_p2"], r["in_p2"], r["pfull"]
    sub = lambda oy, ox: (y + oy) % 2 * 2 + (x + ox) % 2
    p1, p2 = {}, {}

    def hand_tests():
        t_own.wait()
        for copy in t_copies:
            copy.wait_recv()
        return [
            to(
                tbuf.at[:, pl.ds(2 * g * w, w)], tbuf.at[:, pl.ds((2 * g + 1) * w, w)], mate
            )
            for g in range(far)
        ]

    def precondition(handed):
        f_own.wait()
        for copy in f_copies + handed:
            copy.wait_recv()
        pp[...] = jnp.dot(tbuf[...], fbuf[...], preferred_element_type=F32)
        for o in (1, 0):
            p1[0, o] = to(pp.at[pl.ds(0, mh), lanes(sub(o, 1), w)], in_p1.at[0, o], x_to)
            p1[1, o] = to(pp.at[pl.ds(mh, mh), lanes(sub(1, o), w)], in_p1.at[1, o], y_to)

    def precondition_second():
        p1[0, 1].wait_recv()
        out_p2[0] = pp[:mh, lanes(sub(1, 0), w)] + in_p1[0, 1]
        p2[0] = to(out_p2.at[0], in_p2.at[0], y_to)
        p1[1, 1].wait_recv()
        out_p2[1] = pp[mh:, lanes(sub(0, 1), w)] + in_p1[1, 1]
        p2[1] = to(out_p2.at[1], in_p2.at[1], x_to)

    def place(zz, oy, ox):
        return lanes((core * far + zz) * 4 + sub(oy, ox), w)

    def pass_on(where, target):
        return to(pfull.at[:, where], pfull.at[:, where], target)

    def gather_first():
        p1[0, 0].wait_recv()
        p2[0].wait_recv()
        own = place(z, 0, 0)
        pfull[:mh, own] = (pp[:mh, lanes(sub(0, 0), w)] + in_p1[0, 0] + in_p2[0]).astype(BF16)
        p1[1, 0].wait_recv()
        p2[1].wait_recv()
        pfull[mh:, own] = (pp[mh:, lanes(sub(0, 0), w)] + in_p1[1, 0] + in_p2[1]).astype(BF16)
        return [pass_on(own, device(up(g), y, x, core)) for g in range(1, far)]

    def gather_second(along_z):
        for copy in along_z:
            copy.wait_recv()
        gx, gy = [], []
        for g in range(far):
            gx.append(pass_on(place(down(g), 0, 0), x_to))
            gy.append(pass_on(place(down(g), 0, 0), y_to))
        return gx, gy

    def gather_third(gx, gy):
        diagonal = []
        for g in range(far):
            gx[g].wait_recv()
            gy[g].wait_recv()
            if g % 2:
                diagonal.append(pass_on(place(down(g), 0, 1), y_to))
            else:
                diagonal.append(pass_on(place(down(g), 1, 0), x_to))
        return diagonal

    def gather_fourth(diagonal):
        mates = []
        for g in range(far):
            diagonal[g].wait_recv()
            where = lanes(core * far + down(g), 4 * w)
            mates.append(pass_on(where, mate))
        return mates

    def score(mates):
        for copy in mates:
            copy.wait_recv()
        scores_ref[...] = jnp.zeros_like(scores_ref)

        def chunk(i, carry):
            where = lanes(i, 4 * w)
            scores_ref[...] += lax.dot_general(
                gbuf[:rows, where], pfull[:, where], (((1,), (1,)), ((), ())),
                preferred_element_type=F32,
            )
            return carry

        lax.fori_loop(0, s.k // (4 * w), chunk, 0)

    msend, mrecv, msem, mrsem = r["msend"], r["mrecv"], r["msem"], r["mrsem"]
    dsend, drecv, xsend, xrecv = r["dsend"], r["drecv"], r["xsend"], r["xrecv"]

    def mirror_copy(e, side):
        d = core * each + e
        return pltpu.make_async_remote_copy(
            src_ref=msend.at[e, pl.ds(side * w, w)], dst_ref=mrecv.at[d],
            send_sem=msem.at[2 * e + side], recv_sem=mrsem.at[d],
            device_id={"dp": 2 * ((q + d) % chips) + side}, device_id_type=MESH,
        )

    def when_sent(e, act):
        if e:
            act()
        else:
            pl.when(core == 1)(act)

    def finish():
        for g in range(1, far):
            az[g].wait_recv()
            bz[g].wait_recv()
        for e in range(each):
            at = e * W
            part, came = (part_a, r["in_az"]) if at < ra else (part_b, r["in_bz"])
            at = at if at < ra else at - ra
            total = part[0, 0, at : at + W]
            for g in range(far - 1):
                total = total + came[g, at : at + W].astype(F32)
            tmp[e * W : (e + 1) * W] = total
            msend[e] = total.T.astype(BF16)

            def send(e=e):
                for side in range(2):
                    mirror_copy(e, side).start()

            when_sent(e, send)
            where = lanes((q + core * each + e) % chips, W)
            term_ref[:, where] = tmp[pl.ds(pl.multiple_of(e * W + core * w, w), w), :]
            other = pl.ds(pl.multiple_of(e * W + (1 - core) * w, w), w)
            dsend[:, e * W : (e + 1) * W] = tmp[other, :].astype(BF16)
        direct = to(dsend, drecv, mate)
        at = rb - w // 2
        total = part_b[0, 0, at:]
        for g in range(far - 1):
            total = total + r["in_bz"][g, at:].astype(F32)
        extra = jnp.concatenate([total[:, :w], total[:, w:]], axis=0)
        col = 2 * ((q + half) % chips) + (core + q // half) % 2
        term_ref[:, lanes(col, w)] = extra
        xsend[...] = extra.T.astype(BF16)
        mirrored = to(xsend, xrecv, col)
        return direct, mirrored

    def close(direct, mirrored):
        direct.wait_recv()
        for e in range(each):
            where = lanes((q + (1 - core) * each + e) % chips, W)
            term_ref[:, where] = drecv[:, e * W : (e + 1) * W].astype(F32)
        for d in range(1, half):
            pltpu.make_async_remote_copy(
                src_ref=mrecv.at[d], dst_ref=mrecv.at[d], send_sem=msem.at[0], recv_sem=mrsem.at[d],
                device_id={"dp": mate}, device_id_type=MESH,
            ).wait_recv()
            term_ref[:, lanes((q + chips - d) % chips, W)] = mrecv[d].astype(F32)
        mirrored.wait_recv()
        far_chip = (q + half) % chips
        col = 2 * far_chip + (core + far_chip // half) % 2
        term_ref[:, lanes(col, w)] = xrecv[...].astype(F32)

    order = list(range(1, far)) + [0]
    g_own.wait()
    for copy in g_copies:
        copy.wait_recv()
    compute(1)
    first(1, 1)
    first(1, 0)
    compute(2)
    first(2, 1)
    second(1)
    first(2, 0)
    handed = hand_tests()
    compute(3)
    first(3, 1)
    precondition(handed)
    third(1)
    second(2)
    first(3, 0)
    precondition_second()
    compute(0)
    first(0, 1)
    third(2)
    along_z = gather_first()
    second(3)
    first(0, 0)
    gx, gy = gather_second(along_z)
    third(3)
    second(0)
    diagonal = gather_third(gx, gy)
    third(0)
    direct, mirrored = finish()
    mates = gather_fourth(diagonal)
    score(mates)
    close(direct, mirrored)
    for copy in started:
        copy.wait_send()
    for e in range(each):

        def sent(e=e):
            for side in range(2):
                mirror_copy(e, side).wait_send()

        when_sent(e, sent)


def window(grads, covariance, test_grads, inverse_factor):
    n = lax.axis_size("dp")
    rows, k = grads.shape
    s = Sizes(n, rows, k, test_grads.shape[0])
    scratch = s.scratch()
    term, scores = pl.pallas_call(
        functools.partial(kernel, s, list(scratch)),
        out_shape=(
            jax.ShapeDtypeStruct((s.w, k), F32),
            jax.ShapeDtypeStruct((rows, s.tests), F32),
        ),
        in_specs=[pl.BlockSpec(memory_space=pl.ANY)] * 3,
        out_specs=(
            pl.BlockSpec(memory_space=pltpu.VMEM),
            pl.BlockSpec(memory_space=pltpu.VMEM),
        ),
        scratch_shapes=list(scratch.values()),
        compiler_params=pltpu.CompilerParams(
            collective_id=0, has_side_effects=True, vmem_limit_bytes=62 * 1024 * 1024
        ),
    )(grads, test_grads, inverse_factor)
    return scores, 0.9 * covariance + term / (rows * n)


def solution(mesh):
    placed = (P("dp", "feat"), P("dp", "feat"), P("feat", "dp"), P("dp", None))
    whole = mesh.shape["feat"] == 1 and mesh.shape["dp"] == 32
    return jax.shard_map(
        window if whole else general,
        mesh=mesh,
        in_specs=placed,
        out_specs=(P("dp", "feat"), P("dp", "feat")),
        check_vma=False,
    )
```

```python
import functools

import jax
import jax.numpy as jnp
from jax import lax
from jax.experimental import pallas as pl
from jax.experimental.pallas import tpu as pltpu
from jax.sharding import PartitionSpec as P

F32 = jnp.float32
BF16 = jnp.bfloat16
MESH = pl.DeviceIdType.MESH


def general(grads, covariance, test_grads, inverse_factor):
    all_features = lax.all_gather(grads, "feat", axis=1, tiled=True)
    examples = grads.shape[0] * lax.axis_size("dp")
    tested = lax.dot_general(
        inverse_factor, test_grads, (((0,), (1,)), ((), ())), preferred_element_type=F32
    )
    term = lax.dot_general(
        all_features, grads, (((0,), (0,)), ((), ())), preferred_element_type=F32
    )
    joined = lax.psum_scatter(
        jnp.concatenate([term, tested], axis=1), "dp", scatter_dimension=0, tiled=True
    )
    width = grads.shape[1]
    owned_pre = joined[:, width:].astype(BF16)
    pre_columns = lax.all_gather(owned_pre, "dp", axis=0, tiled=True)
    scores = jnp.dot(all_features, pre_columns, preferred_element_type=F32)
    return scores, 0.9 * covariance + joined[:, :width] / examples


class Sizes:
    def __init__(self, n, rows, k, tests):
        self.n, self.rows, self.k, self.tests = n, rows, k, tests
        self.chips, self.far, self.w = n // 2, n // 8, k // n
        self.W = 2 * self.w
        self.half = self.chips // 2
        self.each = self.half // 2
        self.ra = self.each // 2 * self.W
        self.rb = (self.each - self.each // 2) * self.W + self.w // 2
        self.mh = tests // 2

    def scratch(self):
        far, w, W, tests = self.far, self.w, self.W, self.tests
        far1 = max(far - 1, 1)
        v = pltpu.VMEM
        return dict(
            gbuf=v((2 * self.rows, self.k), BF16),
            gt=v((W, 2 * self.rows), BF16),
            tmp=v((self.ra + self.rb, W), F32),
            part_a=v((far, 2, self.ra, W), F32),
            part_b=v((far, 2, self.rb, W), F32),
            out_a1=v((far, 2, self.ra, W), BF16),
            out_b1=v((far, 2, self.rb, W), BF16),
            in_a1=v((far, 2, self.ra, W), BF16),
            in_b1=v((far, 2, self.rb, W), BF16),
            out_a2=v((far, self.ra, W), BF16),
            out_b2=v((far, self.rb, W), BF16),
            in_a2=v((far, self.ra, W), BF16),
            in_b2=v((far, self.rb, W), BF16),
            out_az=v((far1, self.ra, W), BF16),
            out_bz=v((far1, self.rb, W), BF16),
            in_az=v((far1, self.ra, W), BF16),
            in_bz=v((far1, self.rb, W), BF16),
            fbuf=v((2 * far * w, 4 * w), BF16),
            tbuf=v((tests, 2 * far * w), BF16),
            pp=v((tests, 4 * w), F32),
            in_p1=v((2, 2, self.mh, w), F32),
            out_p2=v((2, self.mh, w), F32),
            in_p2=v((2, self.mh, w), F32),
            pfull=v((tests, self.k), BF16),
            msend=v((self.each, W, W), BF16),
            mrecv=v((self.half, w, W), BF16),
            xsend=v((w, w), BF16),
            xrecv=v((w, w), BF16),
            dsend=v((w, self.each * W), BF16),
            drecv=v((w, self.each * W), BF16),
            ssem=pltpu.SemaphoreType.DMA((self.slots(),)),
            rsem=pltpu.SemaphoreType.DMA((self.slots(),)),
            msem=pltpu.SemaphoreType.DMA((2 * self.each,)),
            mrsem=pltpu.SemaphoreType.DMA((self.half,)),
            lsem=pltpu.SemaphoreType.DMA((4,)),
        )

    def slots(self):
        return 4 + 2 * self.far + 2 * self.far + 8 * self.far + 2 * self.far + 6 + 6 * self.far + 2 + 32


def kernel(s, names, g_hbm, t_hbm, f_hbm, term_ref, scores_ref, *refs):
    r = dict(zip(names, refs))
    n, far, w, W, chips, half, each = s.n, s.far, s.w, s.W, s.chips, s.half, s.each
    rows, mh, ra, rb = s.rows, s.mh, s.ra, s.rb
    me = lax.axis_index("dp")
    core, x, y, z = me % 2, me // 2 % 2, me // 4 % 2, me // 8
    q = me // 2

    def device(zz, yy, xx, cc):
        return ((zz * 2 + yy) * 2 + xx) * 2 + cc

    def over(g):
        return (z, z + 1 - 2 * (z % 2), (z + 2) % far, far - 1 - z)[g]

    mate = device(z, y, x, 1 - core)
    x_to = device(z, y, 1 - x, core)
    y_to = device(z, 1 - y, x, core)
    ssem, rsem = r["ssem"], r["rsem"]
    started = []
    count = [0]

    def to(src, dst, target):
        i = count[0]
        count[0] += 1
        copy = pltpu.make_async_remote_copy(
            src_ref=src, dst_ref=dst, send_sem=ssem.at[i], recv_sem=rsem.at[i],
            device_id={"dp": target}, device_id_type=MESH,
        )
        copy.start()
        started.append(copy)
        return copy

    def lanes(block, width):
        return pl.ds(pl.multiple_of(block * width, width), width)

    gbuf, fbuf, tbuf = r["gbuf"], r["fbuf"], r["tbuf"]
    quarter = s.k // far
    own_copies = [
        pltpu.make_async_copy(g_hbm, gbuf.at[pl.ds(0, rows)], r["lsem"].at[0]),
        pltpu.make_async_copy(t_hbm, tbuf.at[:, pl.ds(0, w)], r["lsem"].at[1]),
        pltpu.make_async_copy(
            f_hbm.at[:, lanes(core * far + z, 4 * w)], fbuf.at[pl.ds(0, w)], r["lsem"].at[2]
        ),
    ]

    def meet():
        barrier = pltpu.get_barrier_semaphore()

        for target in [mate, x_to, y_to] + [
            device(over(g), y, x, (core + h) % 2) for g in range(1, far) for h in range(2)
        ]:
            pl.semaphore_signal(barrier, inc=1, device_id={"dp": target}, device_id_type=MESH)
        for copy in own_copies:
            copy.start()
        pl.semaphore_wait(barrier, 2 * far + 1)

    def swap_grads():
        parts = [lanes((over(3) + i) % far, quarter) for i in range(far)]
        return [
            to(g_hbm.at[:, part], gbuf.at[pl.ds(rows, rows), part], mate) for part in parts
        ]

    def hand(g, target, came):
        return to(tbuf.at[:, pl.ds(2 * g * w, w)], tbuf.at[:, pl.ds(came * w, w)], target)

    def swap_tests():
        return [
            to(t_hbm, tbuf.at[:, pl.ds(2 * g * w, w)], device(over(g), y, x, core)) for g in (1, 2)
        ]

    def swap_factor(*groups):
        return [
            to(
                f_hbm.at[:, lanes((core + h) % 2 * far + over(g), 4 * w)],
                fbuf.at[pl.ds((2 * g + h) * w, w)],
                device(over(g), y, x, (core + h) % 2),
            )
            for g in groups
            for h in range(2)
            if g or h
        ]

    def relay_tests(copies):
        copies[1].wait_recv()
        return hand(2, device(over(1), y, x, core), 6)

    def hand_tests(copies):
        own_copies[1].wait()
        copies[0].wait_recv()
        return [hand(g, mate, 2 * g + 1) for g in range(3)]

    def hand_relayed(copy):
        copy.wait_recv()
        return [hand(3, mate, 7)]

    def grads_here(copies):
        for copy in copies:
            copy.wait_recv()

    gt, tmp = r["gt"], r["tmp"]
    part_a, part_b, out_a1, out_b1 = r["part_a"], r["part_b"], r["out_a1"], r["out_b1"]

    def compute(g, first=0, last=4):
        def strip(i, carry):
            oy, ox = (3 - i) // 2, (3 - i) % 2
            own = (over(g) * 2 + (y + oy) % 2) * 2 + (x + ox) % 2
            gt[...] = gbuf[:, lanes(own, W)].T
            for e in range(each):
                col = (own + core * each + e) % chips
                tmp[e * W : (e + 1) * W] = jnp.dot(
                    gt[...], gbuf[:, lanes(col, W)], preferred_element_type=F32
                )
            col = 2 * ((own + half) % chips) + (core + own // half) % 2
            extra = jnp.dot(
                gt[pl.ds(pl.multiple_of(core * w, w), w), :], gbuf[:, lanes(col, w)],
                preferred_element_type=F32,
            )
            tmp[each * W :, :w] = extra[: w // 2]
            tmp[each * W :, w:] = extra[w // 2 :]

            @pl.when(ox == 0)
            def _():
                part_a[g, oy] = tmp[:ra]

            @pl.when(ox == 1)
            def _():
                out_a1[g, oy] = tmp[:ra].astype(BF16)

            @pl.when(oy == 0)
            def _():
                part_b[g, ox] = tmp[ra:]

            @pl.when(oy == 1)
            def _():
                out_b1[g, ox] = tmp[ra:].astype(BF16)

            return carry

        lax.fori_loop(first, last, strip, 0)

    a1, b1, a2, b2, az, bz = {}, {}, {}, {}, {}, {}

    def first(g, o):
        a1[g, o] = to(out_a1.at[g, o], r["in_a1"].at[g, o], x_to)
        b1[g, o] = to(out_b1.at[g, o], r["in_b1"].at[g, o], y_to)

    def second(g):
        a1[g, 1].wait_recv()
        r["out_a2"][g] = (part_a[g, 1] + r["in_a1"][g, 1].astype(F32)).astype(BF16)
        a2[g] = to(r["out_a2"].at[g], r["in_a2"].at[g], y_to)
        b1[g, 1].wait_recv()
        r["out_b2"][g] = (part_b[g, 1] + r["in_b1"][g, 1].astype(F32)).astype(BF16)
        b2[g] = to(r["out_b2"].at[g], r["in_b2"].at[g], x_to)

    def third(g):
        a1[g, 0].wait_recv()
        a2[g].wait_recv()
        total_a = part_a[g, 0] + r["in_a1"][g, 0].astype(F32) + r["in_a2"][g].astype(F32)
        b1[g, 0].wait_recv()
        b2[g].wait_recv()
        total_b = part_b[g, 0] + r["in_b1"][g, 0].astype(F32) + r["in_b2"][g].astype(F32)
        if g == 0:
            part_a[0, 0] = total_a
            part_b[0, 0] = total_b
            return
        if g == 2:
            az[3].wait_recv()
            total_a = total_a + r["in_az"][2].astype(F32)
            bz[3].wait_recv()
            total_b = total_b + r["in_bz"][2].astype(F32)
        target = device(over(2 if g == 2 else 1), y, x, core)
        slot = {3: 2, 2: 1, 1: 0}[g]
        r["out_az"][slot] = total_a.astype(BF16)
        az[g] = to(r["out_az"].at[slot], r["in_az"].at[slot], target)
        r["out_bz"][slot] = total_b.astype(BF16)
        bz[g] = to(r["out_bz"].at[slot], r["in_bz"].at[slot], target)

    pp, in_p1, out_p2, in_p2, pfull = r["pp"], r["in_p1"], r["out_p2"], r["in_p2"], r["pfull"]
    sub = lambda oy, ox: (y + oy) % 2 * 2 + (x + ox) % 2
    p1, p2 = {}, {}

    def precondition(handed):
        own_copies[2].wait()
        for copy in handed:
            copy.wait_recv()
        pp[...] = jnp.dot(tbuf[...], fbuf[...], preferred_element_type=F32)
        for o in (1, 0):
            p1[0, o] = to(pp.at[pl.ds(0, mh), lanes(sub(o, 1), w)], in_p1.at[0, o], x_to)
            p1[1, o] = to(pp.at[pl.ds(mh, mh), lanes(sub(1, o), w)], in_p1.at[1, o], y_to)

    def precondition_second():
        p1[0, 1].wait_recv()
        out_p2[0] = pp[:mh, lanes(sub(1, 0), w)] + in_p1[0, 1]
        p2[0] = to(out_p2.at[0], in_p2.at[0], y_to)
        p1[1, 1].wait_recv()
        out_p2[1] = pp[mh:, lanes(sub(0, 1), w)] + in_p1[1, 1]
        p2[1] = to(out_p2.at[1], in_p2.at[1], x_to)

    def place(oy, ox, part=0, parts=1):
        return lanes((core * 4 + sub(oy, ox)) * parts + part, far * w // parts)

    def pass_on(where, target):
        return to(pfull.at[:, where], pfull.at[:, where], target)

    def gather_first():
        p1[0, 0].wait_recv()
        p2[0].wait_recv()
        own = lanes((core * 4 + sub(0, 0)) * far + z, w)
        pfull[:mh, own] = (pp[:mh, lanes(sub(0, 0), w)] + in_p1[0, 0] + in_p2[0]).astype(BF16)
        p1[1, 0].wait_recv()
        p2[1].wait_recv()
        pfull[mh:, own] = (pp[mh:, lanes(sub(0, 0), w)] + in_p1[1, 0] + in_p2[1]).astype(BF16)
        return [pass_on(own, device(over(g), y, x, core)) for g in (1, 2)]

    def gather_relay(along_z):
        along_z[1].wait_recv()
        there = lanes((core * 4 + sub(0, 0)) * far + over(2), w)
        return pass_on(there, device(over(1), y, x, core))

    def gather_second(along_z, relayed):
        along_z[0].wait_recv()
        relayed.wait_recv()
        own = place(0, 0)
        return pass_on(own, x_to), pass_on(own, y_to), pass_on(own, mate)

    def gather_third(gx, gy):
        gx.wait_recv()
        diagonal = [pass_on(place(0, 1, 0, 2), y_to)]
        mates = [pass_on(place(0, 1), mate)]
        gy.wait_recv()
        diagonal.append(pass_on(place(1, 0, 1, 2), x_to))
        mates.append(pass_on(place(1, 0), mate))
        return diagonal, mates

    def gather_fourth(diagonal):
        for copy in diagonal:
            copy.wait_recv()
        return pass_on(place(1, 1), mate)

    def score(other, first, last):
        def chunk(i, carry):
            cc, at = (core + other) % 2, sub(i // 2, i % 2)
            left = jnp.concatenate(
                [gbuf[:rows, lanes((cc * far + zz) * 4 + at, w)] for zz in range(far)], axis=1
            )
            scores_ref[...] += lax.dot_general(
                left, pfull[:, lanes(cc * 4 + at, far * w)], (((1,), (1,)), ((), ())),
                preferred_element_type=F32,
            )
            return carry

        lax.fori_loop(first, last, chunk, 0)

    def scores_start():
        scores_ref[...] = jnp.zeros_like(scores_ref)

    msend, mrecv, msem, mrsem = r["msend"], r["mrecv"], r["msem"], r["mrsem"]
    dsend, drecv, xsend, xrecv = r["dsend"], r["drecv"], r["xsend"], r["xrecv"]

    def mirror_copy(e, side):
        d = core * each + e
        return pltpu.make_async_remote_copy(
            src_ref=msend.at[e, pl.ds(side * w, w)], dst_ref=mrecv.at[d],
            send_sem=msem.at[2 * e + side], recv_sem=mrsem.at[d],
            device_id={"dp": 2 * ((q + d) % chips) + side}, device_id_type=MESH,
        )

    def when_sent(e, act):
        if e:
            act()
        else:
            pl.when(core == 1)(act)

    def finish():
        for g in (1, 2):
            az[g].wait_recv()
            bz[g].wait_recv()
        for e in range(each):
            at = e * W
            part, came = (part_a, r["in_az"]) if at < ra else (part_b, r["in_bz"])
            at = at if at < ra else at - ra
            total = part[0, 0, at : at + W]
            for g in range(2):
                total = total + came[g, at : at + W].astype(F32)
            tmp[e * W : (e + 1) * W] = total
            msend[e] = total.T.astype(BF16)

            def send(e=e):
                for side in range(2):
                    mirror_copy(e, side).start()

            when_sent(e, send)
            where = lanes((q + core * each + e) % chips, W)
            term_ref[:, where] = tmp[pl.ds(pl.multiple_of(e * W + core * w, w), w), :]
            other = pl.ds(pl.multiple_of(e * W + (1 - core) * w, w), w)
            dsend[:, e * W : (e + 1) * W] = tmp[other, :].astype(BF16)
        direct = to(dsend, drecv, mate)
        at = rb - w // 2
        total = part_b[0, 0, at:]
        for g in range(2):
            total = total + r["in_bz"][g, at:].astype(F32)
        extra = jnp.concatenate([total[:, :w], total[:, w:]], axis=0)
        col = 2 * ((q + half) % chips) + (core + q // half) % 2
        term_ref[:, lanes(col, w)] = extra
        xsend[...] = extra.T.astype(BF16)
        mirrored = to(xsend, xrecv, col)
        return direct, mirrored

    def close(direct, mirrored):
        direct.wait_recv()
        for e in range(each):
            where = lanes((q + (1 - core) * each + e) % chips, W)
            term_ref[:, where] = drecv[:, e * W : (e + 1) * W].astype(F32)
        for d in range(1, half):
            pltpu.make_async_remote_copy(
                src_ref=mrecv.at[d], dst_ref=mrecv.at[d], send_sem=msem.at[0], recv_sem=mrsem.at[d],
                device_id={"dp": mate}, device_id_type=MESH,
            ).wait_recv()
            term_ref[:, lanes((q + chips - d) % chips, W)] = mrecv[d].astype(F32)
        mirrored.wait_recv()
        far_chip = (q + half) % chips
        col = 2 * far_chip + (core + far_chip // half) % 2
        term_ref[:, lanes(col, w)] = xrecv[...].astype(F32)

    def wait_sends():
        for copy in started:
            copy.wait_send()
        for e in range(each):

            def sent(e=e):
                for side in range(2):
                    mirror_copy(e, side).wait_send()

            when_sent(e, sent)

    meet()
    swapped = swap_grads()
    t_copies = swap_tests()
    own_copies[0].wait()
    grads_here(swapped[:3])
    early = swap_factor(0, 3, 2, 1)
    compute(3, 0, 1)
    first(3, 1)
    relayed = relay_tests(t_copies)
    compute(3, 1, 3)
    first(3, 0)
    compute(3, 3, 4)
    grads_here(swapped[3:])
    compute(2)
    first(2, 1)
    early += hand_tests(t_copies)
    second(3)
    first(2, 0)
    early += hand_relayed(relayed)
    compute(1)
    precondition(early)
    first(1, 1)
    third(3)
    precondition_second()
    second(2)
    first(1, 0)
    compute(0)
    along_z = gather_first()
    third(2)
    first(0, 1)
    relayed = gather_relay(along_z)
    second(1)
    first(0, 0)
    second(0)
    gx, gy, mate_own = gather_second(along_z, relayed)
    third(1)
    scores_start()
    score(0, 0, 1)
    third(0)
    direct, mirrored = finish()
    diagonal, mates = gather_third(gx, gy)
    score(0, 1, 3)
    mate_diagonal = gather_fourth(diagonal)
    grads_here([mate_own] + mates)
    score(1, 0, 3)
    score(0, 3, 4)
    grads_here([mate_diagonal])
    score(1, 3, 4)
    close(direct, mirrored)
    wait_sends()

def window(grads, covariance, test_grads, inverse_factor):
    n = lax.axis_size("dp")
    rows, k = grads.shape
    s = Sizes(n, rows, k, test_grads.shape[0])
    scratch = s.scratch()
    term, scores = pl.pallas_call(
        functools.partial(kernel, s, list(scratch)),
        out_shape=(
            jax.ShapeDtypeStruct((s.w, k), F32),
            jax.ShapeDtypeStruct((rows, s.tests), F32),
        ),
        in_specs=[pl.BlockSpec(memory_space=pltpu.HBM)] * 3,
        out_specs=(
            pl.BlockSpec(memory_space=pltpu.VMEM),
            pl.BlockSpec(memory_space=pltpu.VMEM),
        ),
        scratch_shapes=list(scratch.values()),
        compiler_params=pltpu.CompilerParams(
            collective_id=0, has_side_effects=True, vmem_limit_bytes=49 * 1024 * 1024
        ),
    )(*(pltpu.with_memory_space_constraint(a, pltpu.HBM) for a in (grads, test_grads, inverse_factor)))
    return scores, 0.9 * covariance + term / (rows * n)


def solution(mesh):
    placed = (P("dp", "feat"), P("dp", "feat"), P("feat", "dp"), P("dp", None))
    whole = mesh.shape["feat"] == 1 and mesh.shape["dp"] == 32
    return jax.shard_map(
        window if whole else general,
        mesh=mesh,
        in_specs=placed,
        out_specs=(P("dp", "feat"), P("dp", "feat")),
        check_vma=False,
    )
```

```python
import functools

import jax
import jax.numpy as jnp
from jax import lax
from jax.experimental import pallas as pl
from jax.experimental.pallas import tpu as pltpu
from jax.sharding import PartitionSpec as P

F32 = jnp.float32
BF16 = jnp.bfloat16
MESH = pl.DeviceIdType.MESH


def general(grads, covariance, test_grads, inverse_factor):
    all_features = lax.all_gather(grads, "feat", axis=1, tiled=True)
    examples = grads.shape[0] * lax.axis_size("dp")
    tested = lax.dot_general(
        inverse_factor, test_grads, (((0,), (1,)), ((), ())), preferred_element_type=F32
    )
    term = lax.dot_general(
        all_features, grads, (((0,), (0,)), ((), ())), preferred_element_type=F32
    )
    joined = lax.psum_scatter(
        jnp.concatenate([term, tested], axis=1), "dp", scatter_dimension=0, tiled=True
    )
    width = grads.shape[1]
    owned_pre = joined[:, width:].astype(BF16)
    pre_columns = lax.all_gather(owned_pre, "dp", axis=0, tiled=True)
    scores = jnp.dot(all_features, pre_columns, preferred_element_type=F32)
    return scores, 0.9 * covariance + joined[:, :width] / examples


class Sizes:
    def __init__(self, n, rows, k, tests):
        self.n, self.rows, self.k, self.tests = n, rows, k, tests
        self.chips, self.far, self.w = n // 2, n // 8, k // n
        self.W = 2 * self.w
        self.half = self.chips // 2
        self.each = self.half // 2
        self.ra = self.each // 2 * self.W
        self.rb = (self.each - self.each // 2) * self.W + self.w // 2
        self.mh = tests // 2

    def scratch(self):
        far, w, W, tests = self.far, self.w, self.W, self.tests
        far1 = max(far - 1, 1)
        v = pltpu.VMEM
        return dict(
            gbuf=v((2 * self.rows, self.k), BF16),
            gt=v((W, 2 * self.rows), BF16),
            tmp=v((self.ra + self.rb, W), F32),
            part_a=v((far, 2, self.ra, W), F32),
            part_b=v((far, 2, self.rb, W), F32),
            out_a1=v((far, 2, self.ra, W), BF16),
            out_b1=v((far, 2, self.rb, W), BF16),
            in_a1=v((far, 2, self.ra, W), BF16),
            in_b1=v((far, 2, self.rb, W), BF16),
            out_a2=v((far, self.ra, W), BF16),
            out_b2=v((far, self.rb, W), BF16),
            in_a2=v((far, self.ra, W), BF16),
            in_b2=v((far, self.rb, W), BF16),
            out_az=v((far1, self.ra, W), BF16),
            out_bz=v((far1, self.rb, W), BF16),
            in_az=v((far1, self.ra, W), BF16),
            in_bz=v((far1, self.rb, W), BF16),
            fbuf=v((2 * far * w, 4 * w), BF16),
            tbuf=v((tests, 2 * far * w), BF16),
            pp=v((tests, 4 * w), F32),
            in_p1=v((2, 2, self.mh, w), F32),
            out_p2=v((2, self.mh, w), F32),
            in_p2=v((2, self.mh, w), F32),
            pfull=v((tests, self.k), BF16),
            msend=v((self.each, W, W), BF16),
            mrecv=v((self.half, w, W), BF16),
            xsend=v((w, w), BF16),
            xrecv=v((w, w), BF16),
            dsend=v((w, self.each * W), BF16),
            drecv=v((w, self.each * W), BF16),
            ssem=pltpu.SemaphoreType.DMA((self.slots(),)),
            rsem=pltpu.SemaphoreType.DMA((self.slots(),)),
            msem=pltpu.SemaphoreType.DMA((2 * self.each,)),
            mrsem=pltpu.SemaphoreType.DMA((self.half,)),
            lsem=pltpu.SemaphoreType.DMA((4,)),
        )

    def slots(self):
        return 63 + self.chips + 2


def kernel(s, names, g_hbm, t_hbm, f_hbm, term_ref, scores_ref, *refs):
    r = dict(zip(names, refs))
    n, far, w, W, chips, half, each = s.n, s.far, s.w, s.W, s.chips, s.half, s.each
    rows, mh, ra, rb = s.rows, s.mh, s.ra, s.rb
    me = lax.axis_index("dp")
    core, x, y, z = me % 2, me // 2 % 2, me // 4 % 2, me // 8
    q = me // 2

    def device(zz, yy, xx, cc):
        return ((zz * 2 + yy) * 2 + xx) * 2 + cc

    def over(g):
        return (z, z + 1 - 2 * (z % 2), (z + 2) % far, far - 1 - z)[g]

    mate = device(z, y, x, 1 - core)
    x_to = device(z, y, 1 - x, core)
    y_to = device(z, 1 - y, x, core)
    ssem, rsem = r["ssem"], r["rsem"]
    started = []
    count = [0]

    def to(src, dst, target):
        i = count[0]
        count[0] += 1
        copy = pltpu.make_async_remote_copy(
            src_ref=src, dst_ref=dst, send_sem=ssem.at[i], recv_sem=rsem.at[i],
            device_id={"dp": target}, device_id_type=MESH,
        )
        copy.start()
        started.append(copy)
        return copy

    def lanes(block, width):
        return pl.ds(pl.multiple_of(block * width, width), width)

    gbuf, fbuf, tbuf = r["gbuf"], r["fbuf"], r["tbuf"]
    own_copies = [
        pltpu.make_async_copy(g_hbm, gbuf.at[pl.ds(0, rows)], r["lsem"].at[0]),
        pltpu.make_async_copy(t_hbm, tbuf.at[:, pl.ds(0, w)], r["lsem"].at[1]),
        pltpu.make_async_copy(
            f_hbm.at[:, lanes(core * far + z, 4 * w)], fbuf.at[pl.ds(0, w)], r["lsem"].at[2]
        ),
    ]

    def meet():
        barrier = pltpu.get_barrier_semaphore()

        for target in [mate, x_to, y_to] + [
            device(over(g), y, x, (core + h) % 2) for g in range(1, far) for h in range(2)
        ]:
            pl.semaphore_signal(barrier, inc=1, device_id={"dp": target}, device_id_type=MESH)
        for copy in own_copies:
            copy.start()
        pl.semaphore_wait(barrier, 2 * far + 1)

    def swap_grads():
        there = 1 - core
        begin = (over(3) * 2 + 1 - y) * 2 + 1 - x
        last = half // 2
        steps = [0] + [i + last * there for i in range(1, last)]
        steps += [half - last * there, last + last * there]
        steps += [i - last * there for i in range(last + 1, half)] + list(range(half + 1, chips))
        parts = [lanes((begin + i) % chips, W) for i in steps]
        return [
            to(g_hbm.at[:, part], gbuf.at[pl.ds(rows, rows), part], mate) for part in parts
        ]

    def hand(g, target, came):
        return to(tbuf.at[:, pl.ds(2 * g * w, w)], tbuf.at[:, pl.ds(came * w, w)], target)

    def swap_tests():
        return [
            to(t_hbm, tbuf.at[:, pl.ds(2 * g * w, w)], device(over(g), y, x, core)) for g in (1, 2)
        ]

    def swap_factor(*groups):
        return [
            to(
                f_hbm.at[:, lanes((core + h) % 2 * far + over(g), 4 * w)],
                fbuf.at[pl.ds((2 * g + h) * w, w)],
                device(over(g), y, x, (core + h) % 2),
            )
            for g in groups
            for h in range(2)
            if g or h
        ]

    def relay_tests(copies):
        copies[1].wait_recv()
        return hand(2, device(over(1), y, x, core), 6)

    def hand_tests(copies):
        own_copies[1].wait()
        copies[0].wait_recv()
        return [hand(g, mate, 2 * g + 1) for g in range(3)]

    def hand_relayed(copy):
        copy.wait_recv()
        return [hand(3, mate, 7)]

    def grads_here(copies):
        for copy in copies:
            copy.wait_recv()

    gt, tmp = r["gt"], r["tmp"]
    part_a, part_b, out_a1, out_b1 = r["part_a"], r["part_b"], r["out_a1"], r["out_b1"]

    def compute(g, first=0, last=4):
        def strip(i, carry):
            oy, ox = (3 - i) // 2, (3 - i) % 2
            own = (over(g) * 2 + (y + oy) % 2) * 2 + (x + ox) % 2
            gt[...] = gbuf[:, lanes(own, W)].T
            for e in range(each):
                col = (own + core * each + e) % chips
                tmp[e * W : (e + 1) * W] = jnp.dot(
                    gt[...], gbuf[:, lanes(col, W)], preferred_element_type=F32
                )
            col = 2 * ((own + half) % chips) + (core + own // half) % 2
            extra = jnp.dot(
                gt[pl.ds(pl.multiple_of(core * w, w), w), :], gbuf[:, lanes(col, w)],
                preferred_element_type=F32,
            )
            tmp[each * W :, :w] = extra[: w // 2]
            tmp[each * W :, w:] = extra[w // 2 :]

            @pl.when(ox == 0)
            def _():
                part_a[g, oy] = tmp[:ra]

            @pl.when(ox == 1)
            def _():
                out_a1[g, oy] = tmp[:ra].astype(BF16)

            @pl.when(oy == 0)
            def _():
                part_b[g, ox] = tmp[ra:]

            @pl.when(oy == 1)
            def _():
                out_b1[g, ox] = tmp[ra:].astype(BF16)

            return carry

        lax.fori_loop(first, last, strip, 0)

    a1, b1, a2, b2, az, bz = {}, {}, {}, {}, {}, {}

    def first(g, o):
        a1[g, o] = to(out_a1.at[g, o], r["in_a1"].at[g, o], x_to)
        b1[g, o] = to(out_b1.at[g, o], r["in_b1"].at[g, o], y_to)

    def second(g):
        a1[g, 1].wait_recv()
        r["out_a2"][g] = (part_a[g, 1] + r["in_a1"][g, 1].astype(F32)).astype(BF16)
        a2[g] = to(r["out_a2"].at[g], r["in_a2"].at[g], y_to)
        b1[g, 1].wait_recv()
        r["out_b2"][g] = (part_b[g, 1] + r["in_b1"][g, 1].astype(F32)).astype(BF16)
        b2[g] = to(r["out_b2"].at[g], r["in_b2"].at[g], x_to)

    def third(g):
        a1[g, 0].wait_recv()
        a2[g].wait_recv()
        total_a = part_a[g, 0] + r["in_a1"][g, 0].astype(F32) + r["in_a2"][g].astype(F32)
        b1[g, 0].wait_recv()
        b2[g].wait_recv()
        total_b = part_b[g, 0] + r["in_b1"][g, 0].astype(F32) + r["in_b2"][g].astype(F32)
        if g == 0:
            part_a[0, 0] = total_a
            part_b[0, 0] = total_b
            return
        if g == 2:
            az[3].wait_recv()
            total_a = total_a + r["in_az"][2].astype(F32)
            bz[3].wait_recv()
            total_b = total_b + r["in_bz"][2].astype(F32)
        target = device(over(2 if g == 2 else 1), y, x, core)
        slot = {3: 2, 2: 1, 1: 0}[g]
        r["out_az"][slot] = total_a.astype(BF16)
        az[g] = to(r["out_az"].at[slot], r["in_az"].at[slot], target)
        r["out_bz"][slot] = total_b.astype(BF16)
        bz[g] = to(r["out_bz"].at[slot], r["in_bz"].at[slot], target)

    pp, in_p1, out_p2, in_p2, pfull = r["pp"], r["in_p1"], r["out_p2"], r["in_p2"], r["pfull"]
    sub = lambda oy, ox: (y + oy) % 2 * 2 + (x + ox) % 2
    p1, p2 = {}, {}

    def precondition(handed):
        own_copies[2].wait()
        for copy in handed:
            copy.wait_recv()
        pp[...] = jnp.dot(tbuf[...], fbuf[...], preferred_element_type=F32)
        for o in (1, 0):
            p1[0, o] = to(pp.at[pl.ds(0, mh), lanes(sub(o, 1), w)], in_p1.at[0, o], x_to)
            p1[1, o] = to(pp.at[pl.ds(mh, mh), lanes(sub(1, o), w)], in_p1.at[1, o], y_to)

    def precondition_second():
        p1[0, 1].wait_recv()
        out_p2[0] = pp[:mh, lanes(sub(1, 0), w)] + in_p1[0, 1]
        p2[0] = to(out_p2.at[0], in_p2.at[0], y_to)
        p1[1, 1].wait_recv()
        out_p2[1] = pp[mh:, lanes(sub(0, 1), w)] + in_p1[1, 1]
        p2[1] = to(out_p2.at[1], in_p2.at[1], x_to)

    def place(oy, ox, part=0, parts=1):
        return lanes((core * 4 + sub(oy, ox)) * parts + part, far * w // parts)

    def pass_on(where, target):
        return to(pfull.at[:, where], pfull.at[:, where], target)

    def gather_first():
        p1[0, 0].wait_recv()
        p2[0].wait_recv()
        own = lanes((core * 4 + sub(0, 0)) * far + z, w)
        pfull[:mh, own] = (pp[:mh, lanes(sub(0, 0), w)] + in_p1[0, 0] + in_p2[0]).astype(BF16)
        p1[1, 0].wait_recv()
        p2[1].wait_recv()
        pfull[mh:, own] = (pp[mh:, lanes(sub(0, 0), w)] + in_p1[1, 0] + in_p2[1]).astype(BF16)
        return [pass_on(own, device(over(g), y, x, core)) for g in (1, 2)]

    def gather_relay(along_z):
        along_z[1].wait_recv()
        there = lanes((core * 4 + sub(0, 0)) * far + over(2), w)
        return pass_on(there, device(over(1), y, x, core))

    def gather_second(along_z, relayed):
        along_z[0].wait_recv()
        relayed.wait_recv()
        gx = [pass_on(place(0, 0, i, 2), x_to) for i in range(2)]
        gy = [pass_on(place(0, 0, i, 2), y_to) for i in (1, 0)]
        return gx, gy, pass_on(place(0, 0), mate)

    def gather_third(gx, gy):
        gx[0].wait_recv()
        diagonal = [pass_on(place(0, 1, 0, 2), y_to)]
        gy[0].wait_recv()
        diagonal.append(pass_on(place(1, 0, 1, 2), x_to))
        gx[1].wait_recv()
        mates = [pass_on(place(0, 1), mate)]
        gy[1].wait_recv()
        mates.append(pass_on(place(1, 0), mate))
        return diagonal, mates

    def gather_fourth(diagonal):
        for copy in diagonal:
            copy.wait_recv()
        return pass_on(place(1, 1), mate)

    def score(other, first, last):
        def chunk(i, carry):
            cc, at = (core + other) % 2, sub(i // 2, i % 2)
            left = jnp.concatenate(
                [gbuf[:rows, lanes((cc * far + zz) * 4 + at, w)] for zz in range(far)], axis=1
            )
            scores_ref[...] += lax.dot_general(
                left, pfull[:, lanes(cc * 4 + at, far * w)], (((1,), (1,)), ((), ())),
                preferred_element_type=F32,
            )
            return carry

        lax.fori_loop(first, last, chunk, 0)

    def scores_start():
        scores_ref[...] = jnp.zeros_like(scores_ref)

    msend, mrecv, msem, mrsem = r["msend"], r["mrecv"], r["msem"], r["mrsem"]
    dsend, drecv, xsend, xrecv = r["dsend"], r["drecv"], r["xsend"], r["xrecv"]

    def mirror_copy(e, side):
        d = core * each + e
        return pltpu.make_async_remote_copy(
            src_ref=msend.at[e, pl.ds(side * w, w)], dst_ref=mrecv.at[d],
            send_sem=msem.at[2 * e + side], recv_sem=mrsem.at[d],
            device_id={"dp": 2 * ((q + d) % chips) + side}, device_id_type=MESH,
        )

    def when_sent(e, act):
        if e:
            act()
        else:
            pl.when(core == 1)(act)

    def finish():
        for g in (1, 2):
            az[g].wait_recv()
            bz[g].wait_recv()
        for e in range(each):
            at = e * W
            part, came = (part_a, r["in_az"]) if at < ra else (part_b, r["in_bz"])
            at = at if at < ra else at - ra
            total = part[0, 0, at : at + W]
            for g in range(2):
                total = total + came[g, at : at + W].astype(F32)
            tmp[e * W : (e + 1) * W] = total
            msend[e] = total.T.astype(BF16)

            def send(e=e):
                for side in range(2):
                    mirror_copy(e, side).start()

            when_sent(e, send)
            where = lanes((q + core * each + e) % chips, W)
            term_ref[:, where] = tmp[pl.ds(pl.multiple_of(e * W + core * w, w), w), :]
            other = pl.ds(pl.multiple_of(e * W + (1 - core) * w, w), w)
            dsend[:, e * W : (e + 1) * W] = tmp[other, :].astype(BF16)
        direct = to(dsend, drecv, mate)
        at = rb - w // 2
        total = part_b[0, 0, at:]
        for g in range(2):
            total = total + r["in_bz"][g, at:].astype(F32)
        extra = jnp.concatenate([total[:, :w], total[:, w:]], axis=0)
        col = 2 * ((q + half) % chips) + (core + q // half) % 2
        term_ref[:, lanes(col, w)] = extra
        xsend[...] = extra.T.astype(BF16)
        mirrored = to(xsend, xrecv, col)
        return direct, mirrored

    def close(direct, mirrored):
        direct.wait_recv()
        for e in range(each):
            where = lanes((q + (1 - core) * each + e) % chips, W)
            term_ref[:, where] = drecv[:, e * W : (e + 1) * W].astype(F32)
        for d in range(1, half):
            pltpu.make_async_remote_copy(
                src_ref=mrecv.at[d], dst_ref=mrecv.at[d], send_sem=msem.at[0], recv_sem=mrsem.at[d],
                device_id={"dp": mate}, device_id_type=MESH,
            ).wait_recv()
            term_ref[:, lanes((q + chips - d) % chips, W)] = mrecv[d].astype(F32)
        mirrored.wait_recv()
        far_chip = (q + half) % chips
        col = 2 * far_chip + (core + far_chip // half) % 2
        term_ref[:, lanes(col, w)] = xrecv[...].astype(F32)

    def wait_sends():
        assert count[0] == s.slots()
        for copy in started:
            copy.wait_send()
        for e in range(each):

            def sent(e=e):
                for side in range(2):
                    mirror_copy(e, side).wait_send()

            when_sent(e, sent)

    meet()
    swapped = swap_grads()
    t_copies = swap_tests()
    own_copies[0].wait()
    grads_here(swapped[: half // 2 + 2])
    early = swap_factor(0, 3, 2, 1)
    compute(3, 0, 1)
    first(3, 1)
    relayed = relay_tests(t_copies)
    grads_here(swapped[half // 2 + 2 :])
    compute(3, 1, 3)
    first(3, 0)
    compute(3, 3, 4)
    compute(2)
    first(2, 1)
    early += hand_tests(t_copies)
    second(3)
    first(2, 0)
    early += hand_relayed(relayed)
    compute(1)
    precondition(early)
    first(1, 1)
    third(3)
    precondition_second()
    second(2)
    first(1, 0)
    compute(0)
    along_z = gather_first()
    third(2)
    first(0, 1)
    relayed = gather_relay(along_z)
    second(1)
    first(0, 0)
    second(0)
    gx, gy, mate_own = gather_second(along_z, relayed)
    third(1)
    scores_start()
    score(0, 0, 1)
    third(0)
    direct, mirrored = finish()
    diagonal, mates = gather_third(gx, gy)
    score(0, 1, 3)
    grads_here([mate_own] + mates)
    score(1, 0, 3)
    mate_diagonal = gather_fourth(diagonal)
    score(0, 3, 4)
    grads_here([mate_diagonal])
    score(1, 3, 4)
    close(direct, mirrored)
    wait_sends()

def window(grads, covariance, test_grads, inverse_factor):
    n = lax.axis_size("dp")
    rows, k = grads.shape
    s = Sizes(n, rows, k, test_grads.shape[0])
    scratch = s.scratch()
    term, scores = pl.pallas_call(
        functools.partial(kernel, s, list(scratch)),
        out_shape=(
            jax.ShapeDtypeStruct((s.w, k), F32),
            jax.ShapeDtypeStruct((rows, s.tests), F32),
        ),
        in_specs=[pl.BlockSpec(memory_space=pltpu.HBM)] * 3,
        out_specs=(
            pl.BlockSpec(memory_space=pltpu.VMEM),
            pl.BlockSpec(memory_space=pltpu.VMEM),
        ),
        scratch_shapes=list(scratch.values()),
        compiler_params=pltpu.CompilerParams(
            collective_id=0, has_side_effects=True, vmem_limit_bytes=49 * 1024 * 1024
        ),
    )(*(pltpu.with_memory_space_constraint(a, pltpu.HBM) for a in (grads, test_grads, inverse_factor)))
    return scores, 0.9 * covariance + term / (rows * n)


def solution(mesh):
    placed = (P("dp", "feat"), P("dp", "feat"), P("feat", "dp"), P("dp", None))
    whole = mesh.shape["feat"] == 1 and mesh.shape["dp"] == 32
    return jax.shard_map(
        window if whole else general,
        mesh=mesh,
        in_specs=placed,
        out_specs=(P("dp", "feat"), P("dp", "feat")),
        check_vma=False,
    )
```

```python
import functools

import jax
import jax.numpy as jnp
from jax import lax
from jax.experimental import pallas as pl
from jax.experimental.pallas import tpu as pltpu
from jax.sharding import PartitionSpec as P

F32 = jnp.float32
BF16 = jnp.bfloat16
MESH = pl.DeviceIdType.MESH


def general(grads, covariance, test_grads, inverse_factor):
    all_features = lax.all_gather(grads, "feat", axis=1, tiled=True)
    examples = grads.shape[0] * lax.axis_size("dp")
    tested = lax.dot_general(
        inverse_factor, test_grads, (((0,), (1,)), ((), ())), preferred_element_type=F32
    )
    term = lax.dot_general(
        all_features, grads, (((0,), (0,)), ((), ())), preferred_element_type=F32
    )
    joined = lax.psum_scatter(
        jnp.concatenate([term, tested], axis=1), "dp", scatter_dimension=0, tiled=True
    )
    width = grads.shape[1]
    owned_pre = joined[:, width:].astype(BF16)
    pre_columns = lax.all_gather(owned_pre, "dp", axis=0, tiled=True)
    scores = jnp.dot(all_features, pre_columns, preferred_element_type=F32)
    return scores, 0.9 * covariance + joined[:, :width] / examples


class Sizes:
    def __init__(self, n, rows, k, tests):
        self.n, self.rows, self.k, self.tests = n, rows, k, tests
        self.chips, self.far, self.w = n // 2, n // 8, k // n
        self.W = 2 * self.w
        self.half = self.chips // 2
        self.each = self.half // 2
        self.strip = self.each * self.W + self.w // 2
        self.rc = self.w // 2
        self.ra = (self.strip - self.rc) // 2
        self.rb = self.ra
        self.mh = tests // 2

    def scratch(self):
        far, w, W, tests = self.far, self.w, self.W, self.tests
        far1 = max(far - 1, 1)
        v = pltpu.VMEM
        return dict(
            gbuf=v((2 * self.rows, self.k), BF16),
            gt=v((W, 2 * self.rows), BF16),
            tmp=v((self.strip, W), F32),
            part_a=v((far, 2, self.ra, W), F32),
            part_b=v((far, 2, self.rb, W), F32),
            out_a1=v((far, 2, self.ra, W), BF16),
            out_b1=v((far, 2, self.rb, W), BF16),
            in_a1=v((far, 2, self.ra, W), BF16),
            in_b1=v((far, 2, self.rb, W), BF16),
            out_a2=v((far, self.ra, W), BF16),
            out_b2=v((far, self.rb, W), BF16),
            in_a2=v((far, self.ra, W), BF16),
            in_b2=v((far, self.rb, W), BF16),
            out_az=v((far1, self.ra, W), BF16),
            out_bz=v((far1, self.rb, W), BF16),
            in_az=v((far1, self.ra, W), BF16),
            in_bz=v((far1, self.rb, W), BF16),
            part_c=v((2, 4, self.rc, W), F32),
            out_c1=v((2, 4, self.rc, W), BF16),
            in_c1=v((2, 4, self.rc, W), BF16),
            out_c2=v((4, self.rc, W), BF16),
            in_c2=v((4, self.rc, W), BF16),
            out_c3=v((2, 2, self.rc // 2, W), BF16),
            in_c3=v((2, 2, self.rc // 2, W), BF16),
            out_c4=v((2, self.rc // 2, W), BF16),
            in_c4=v((2, self.rc // 2, W), BF16),
            fbuf=v((2 * far * w, 4 * w), BF16),
            tbuf=v((tests, 2 * far * w), BF16),
            pp=v((tests, 4 * w), F32),
            in_p1=v((2, 2, self.mh, w), F32),
            out_p2=v((2, self.mh, w), F32),
            in_p2=v((2, self.mh, w), F32),
            pfull=v((tests, self.k), BF16),
            msend=v((self.each, W, W), BF16),
            mrecv=v((self.half, w, W), BF16),
            xsend=v((w, w), BF16),
            xrecv=v((w, w), BF16),
            dsend=v((w, self.each * W), BF16),
            drecv=v((w, self.each * W), BF16),
            ssem=pltpu.SemaphoreType.DMA((self.slots(),)),
            rsem=pltpu.SemaphoreType.DMA((self.slots(),)),
            msem=pltpu.SemaphoreType.DMA((2 * self.each,)),
            mrsem=pltpu.SemaphoreType.DMA((self.half,)),
            lsem=pltpu.SemaphoreType.DMA((4,)),
        )

    def slots(self):
        return 72 + self.chips


def kernel(s, names, g_hbm, t_hbm, f_hbm, term_ref, scores_ref, *refs):
    r = dict(zip(names, refs))
    n, far, w, W, chips, half, each = s.n, s.far, s.w, s.W, s.chips, s.half, s.each
    rows, mh, ra, rb = s.rows, s.mh, s.ra, s.rb
    me = lax.axis_index("dp")
    core, x, y, z = me % 2, me // 2 % 2, me // 4 % 2, me // 8
    q = me // 2

    def device(zz, yy, xx, cc):
        return ((zz * 2 + yy) * 2 + xx) * 2 + cc

    def over(g):
        return (z, z + 1 - 2 * (z % 2), (z + 2) % far, far - 1 - z)[g]

    mate = device(z, y, x, 1 - core)
    x_to = device(z, y, 1 - x, core)
    y_to = device(z, 1 - y, x, core)
    ssem, rsem = r["ssem"], r["rsem"]
    started = []
    count = [0]

    def to(src, dst, target):
        i = count[0]
        count[0] += 1
        copy = pltpu.make_async_remote_copy(
            src_ref=src, dst_ref=dst, send_sem=ssem.at[i], recv_sem=rsem.at[i],
            device_id={"dp": target}, device_id_type=MESH,
        )
        copy.start()
        started.append(copy)
        return copy

    def lanes(block, width):
        return pl.ds(pl.multiple_of(block * width, width), width)

    gbuf, fbuf, tbuf = r["gbuf"], r["fbuf"], r["tbuf"]
    own_copies = [
        pltpu.make_async_copy(g_hbm, gbuf.at[pl.ds(0, rows)], r["lsem"].at[0]),
        pltpu.make_async_copy(t_hbm, tbuf.at[:, pl.ds(0, w)], r["lsem"].at[1]),
        pltpu.make_async_copy(
            f_hbm.at[:, lanes(core * far + z, 4 * w)], fbuf.at[pl.ds(0, w)], r["lsem"].at[2]
        ),
    ]

    def meet():
        barrier = pltpu.get_barrier_semaphore()

        for target in [mate, x_to, y_to] + [
            device(over(g), y, x, (core + h) % 2) for g in range(1, far) for h in range(2)
        ]:
            pl.semaphore_signal(barrier, inc=1, device_id={"dp": target}, device_id_type=MESH)
        for copy in own_copies:
            copy.start()
        pl.semaphore_wait(barrier, 2 * far + 1)

    def swap_grads():
        there = 1 - core
        begin = (over(3) * 2 + 1 - y) * 2 + 1 - x
        last = half // 2
        steps = [0] + [i + last * there for i in range(1, last)]
        steps += [half - last * there, last + last * there]
        steps += [i - last * there for i in range(last + 1, half)] + list(range(half + 1, chips))
        parts = [lanes((begin + i) % chips, W) for i in steps]
        return [
            to(g_hbm.at[:, part], gbuf.at[pl.ds(rows, rows), part], mate) for part in parts
        ]

    def hand(g, target, came):
        return to(tbuf.at[:, pl.ds(2 * g * w, w)], tbuf.at[:, pl.ds(came * w, w)], target)

    def swap_tests():
        return [
            to(t_hbm, tbuf.at[:, pl.ds(2 * g * w, w)], device(over(g), y, x, core)) for g in (1, 2)
        ]

    def swap_factor(*groups):
        return [
            to(
                f_hbm.at[:, lanes((core + h) % 2 * far + over(g), 4 * w)],
                fbuf.at[pl.ds((2 * g + h) * w, w)],
                device(over(g), y, x, (core + h) % 2),
            )
            for g in groups
            for h in range(2)
            if g or h
        ]

    def relay_tests(copies):
        copies[1].wait_recv()
        return hand(2, device(over(1), y, x, core), 6)

    def hand_tests(copies):
        own_copies[1].wait()
        copies[0].wait_recv()
        return [hand(g, mate, 2 * g + 1) for g in range(3)]

    def hand_relayed(copy):
        copy.wait_recv()
        return [hand(3, mate, 7)]

    def grads_here(copies):
        for copy in copies:
            copy.wait_recv()

    gt, tmp = r["gt"], r["tmp"]
    part_c, out_c1, in_c1, out_c2, in_c2 = (
        r["part_c"], r["out_c1"], r["in_c1"], r["out_c2"], r["in_c2"]
    )
    out_c3, in_c3, out_c4, in_c4 = r["out_c3"], r["in_c3"], r["out_c4"], r["in_c4"]
    part_a, part_b, out_a1, out_b1 = r["part_a"], r["part_b"], r["out_a1"], r["out_b1"]

    def compute(g, first=0, last=4):
        def strip(i, carry):
            oy, ox = (3 - i) // 2, (3 - i) % 2
            own = (over(g) * 2 + (y + oy) % 2) * 2 + (x + ox) % 2
            gt[...] = gbuf[:, lanes(own, W)].T
            for e in range(each):
                col = (own + core * each + e) % chips
                tmp[e * W : (e + 1) * W] = jnp.dot(
                    gt[...], gbuf[:, lanes(col, W)], preferred_element_type=F32
                )
            col = 2 * ((own + half) % chips) + (core + own // half) % 2
            extra = jnp.dot(
                gt[pl.ds(pl.multiple_of(core * w, w), w), :], gbuf[:, lanes(col, w)],
                preferred_element_type=F32,
            )
            tmp[each * W :, :w] = extra[: w // 2]
            tmp[each * W :, w:] = extra[w // 2 :]

            @pl.when(ox == 0)
            def _():
                part_a[g, oy] = tmp[:ra]

            @pl.when(ox == 1)
            def _():
                out_a1[g, oy] = tmp[:ra].astype(BF16)

            @pl.when(oy == 0)
            def _():
                part_b[g, ox] = tmp[ra : ra + rb]

            @pl.when(oy == 1)
            def _():
                out_b1[g, ox] = tmp[ra : ra + rb].astype(BF16)

            if g % 2:
                out_c1[g // 2, 3 - i] = tmp[ra + rb :].astype(BF16)
            else:
                part_c[g // 2, 3 - i] = tmp[ra + rb :]
            return carry

        lax.fori_loop(first, last, strip, 0)

    a1, b1, a2, b2, az, bz = {}, {}, {}, {}, {}, {}

    def first(g, o):
        a1[g, o] = to(out_a1.at[g, o], r["in_a1"].at[g, o], x_to)
        b1[g, o] = to(out_b1.at[g, o], r["in_b1"].at[g, o], y_to)

    def second(g):
        a1[g, 1].wait_recv()
        r["out_a2"][g] = (part_a[g, 1] + r["in_a1"][g, 1].astype(F32)).astype(BF16)
        a2[g] = to(r["out_a2"].at[g], r["in_a2"].at[g], y_to)
        b1[g, 1].wait_recv()
        r["out_b2"][g] = (part_b[g, 1] + r["in_b1"][g, 1].astype(F32)).astype(BF16)
        b2[g] = to(r["out_b2"].at[g], r["in_b2"].at[g], x_to)

    def third(g):
        a1[g, 0].wait_recv()
        a2[g].wait_recv()
        total_a = part_a[g, 0] + r["in_a1"][g, 0].astype(F32) + r["in_a2"][g].astype(F32)
        b1[g, 0].wait_recv()
        b2[g].wait_recv()
        total_b = part_b[g, 0] + r["in_b1"][g, 0].astype(F32) + r["in_b2"][g].astype(F32)
        if g == 0:
            part_a[0, 0] = total_a
            part_b[0, 0] = total_b
            return
        if g == 2:
            az[3].wait_recv()
            total_a = total_a + r["in_az"][2].astype(F32)
            bz[3].wait_recv()
            total_b = total_b + r["in_bz"][2].astype(F32)
        target = device(over(2 if g == 2 else 1), y, x, core)
        slot = {3: 2, 2: 1, 1: 0}[g]
        r["out_az"][slot] = total_a.astype(BF16)
        az[g] = to(r["out_az"].at[slot], r["in_az"].at[slot], target)
        r["out_bz"][slot] = total_b.astype(BF16)
        bz[g] = to(r["out_bz"].at[slot], r["in_bz"].at[slot], target)

    c1, c2, c3, c4 = {}, [], {}, {}
    hc = s.rc // 2

    def c_first():
        for slot in (1, 0):
            c1[slot] = to(out_c1.at[slot], in_c1.at[slot], device(over(1), y, x, core))

    def c_second():
        c1[1].wait_recv()
        out_c2[...] = (part_c[1] + in_c1[1].astype(F32)).astype(BF16)
        c2.append(to(out_c2, in_c2, device(over(2), y, x, core)))

    def c_third():
        c1[0].wait_recv()
        c2[0].wait_recv()
        part_c[0] = part_c[0] + in_c1[0].astype(F32) + in_c2[...].astype(F32)
        for o in range(2):
            out_c3[0, o] = part_c[0, 2 * o + 1, :hc].astype(BF16)
            out_c3[1, o] = part_c[0, 2 + o, hc:].astype(BF16)
        c3[0] = to(out_c3.at[0], in_c3.at[0], x_to)
        c3[1] = to(out_c3.at[1], in_c3.at[1], y_to)

    def c_fourth():
        c3[0].wait_recv()
        out_c4[0] = (part_c[0, 2, :hc] + in_c3[0, 1].astype(F32)).astype(BF16)
        c4[0] = to(out_c4.at[0], in_c4.at[0], y_to)
        c3[1].wait_recv()
        out_c4[1] = (part_c[0, 1, hc:] + in_c3[1, 1].astype(F32)).astype(BF16)
        c4[1] = to(out_c4.at[1], in_c4.at[1], x_to)

    pp, in_p1, out_p2, in_p2, pfull = r["pp"], r["in_p1"], r["out_p2"], r["in_p2"], r["pfull"]
    sub = lambda oy, ox: (y + oy) % 2 * 2 + (x + ox) % 2
    p1, p2 = {}, {}

    def precondition(handed):
        own_copies[2].wait()
        for copy in handed:
            copy.wait_recv()
        pp[...] = jnp.dot(tbuf[...], fbuf[...], preferred_element_type=F32)
        for o in (1, 0):
            p1[0, o] = to(pp.at[pl.ds(0, mh), lanes(sub(o, 1), w)], in_p1.at[0, o], x_to)
            p1[1, o] = to(pp.at[pl.ds(mh, mh), lanes(sub(1, o), w)], in_p1.at[1, o], y_to)

    def precondition_second():
        p1[0, 1].wait_recv()
        out_p2[0] = pp[:mh, lanes(sub(1, 0), w)] + in_p1[0, 1]
        p2[0] = to(out_p2.at[0], in_p2.at[0], y_to)
        p1[1, 1].wait_recv()
        out_p2[1] = pp[mh:, lanes(sub(0, 1), w)] + in_p1[1, 1]
        p2[1] = to(out_p2.at[1], in_p2.at[1], x_to)

    def place(oy, ox, part=0, parts=1):
        return lanes((core * 4 + sub(oy, ox)) * parts + part, far * w // parts)

    def pass_on(where, target):
        return to(pfull.at[:, where], pfull.at[:, where], target)

    def gather_first():
        p1[0, 0].wait_recv()
        p2[0].wait_recv()
        own = lanes((core * 4 + sub(0, 0)) * far + z, w)
        pfull[:mh, own] = (pp[:mh, lanes(sub(0, 0), w)] + in_p1[0, 0] + in_p2[0]).astype(BF16)
        p1[1, 0].wait_recv()
        p2[1].wait_recv()
        pfull[mh:, own] = (pp[mh:, lanes(sub(0, 0), w)] + in_p1[1, 0] + in_p2[1]).astype(BF16)
        return [pass_on(own, device(over(g), y, x, core)) for g in (1, 2)]

    def gather_relay(along_z):
        along_z[1].wait_recv()
        there = lanes((core * 4 + sub(0, 0)) * far + over(2), w)
        return pass_on(there, device(over(1), y, x, core))

    def gather_second(along_z, relayed):
        along_z[0].wait_recv()
        relayed.wait_recv()
        gx = [pass_on(place(0, 0, i, 2), x_to) for i in range(2)]
        gy = [pass_on(place(0, 0, i, 2), y_to) for i in (1, 0)]
        return gx, gy, pass_on(place(0, 0), mate)

    def gather_third(gx, gy):
        gx[0].wait_recv()
        diagonal = [pass_on(place(0, 1, 0, 2), y_to)]
        gy[0].wait_recv()
        return diagonal + [pass_on(place(1, 0, 1, 2), x_to)]

    def gather_mates(gx, gy):
        gx[1].wait_recv()
        mates = [pass_on(place(0, 1), mate)]
        gy[1].wait_recv()
        return mates + [pass_on(place(1, 0), mate)]

    def gather_fourth(diagonal):
        for copy in diagonal:
            copy.wait_recv()
        return pass_on(place(1, 1), mate)

    def score(other, first, last):
        def chunk(i, carry):
            cc, at = (core + other) % 2, sub(i // 2, i % 2)
            left = jnp.concatenate(
                [gbuf[:rows, lanes((cc * far + zz) * 4 + at, w)] for zz in range(far)], axis=1
            )
            scores_ref[...] += lax.dot_general(
                left, pfull[:, lanes(cc * 4 + at, far * w)], (((1,), (1,)), ((), ())),
                preferred_element_type=F32,
            )
            return carry

        lax.fori_loop(first, last, chunk, 0)

    def scores_start():
        scores_ref[...] = jnp.zeros_like(scores_ref)

    msend, mrecv, msem, mrsem = r["msend"], r["mrecv"], r["msem"], r["mrsem"]
    dsend, drecv, xsend, xrecv = r["dsend"], r["drecv"], r["xsend"], r["xrecv"]

    def mirror_copy(e, side):
        d = core * each + e
        return pltpu.make_async_remote_copy(
            src_ref=msend.at[e, pl.ds(side * w, w)], dst_ref=mrecv.at[d],
            send_sem=msem.at[2 * e + side], recv_sem=mrsem.at[d],
            device_id={"dp": 2 * ((q + d) % chips) + side}, device_id_type=MESH,
        )

    def when_sent(e, act):
        if e:
            act()
        else:
            pl.when(core == 1)(act)

    def finish(part):
        if part < 2:
            sums, came, copies, size = (
                (part_a, r["in_az"], az, ra), (part_b, r["in_bz"], bz, rb)
            )[part]
            at = part * ra
            for g in (1, 2):
                copies[g].wait_recv()
            tmp[at : at + size] = sums[0, 0] + came[0].astype(F32) + came[1].astype(F32)
        else:
            at, size = ra + rb, s.rc
            for i in range(2):
                c4[i].wait_recv()
                tmp[at + i * hc : at + (i + 1) * hc] = (
                    part_c[0, 0, i * hc : (i + 1) * hc]
                    + in_c3[i, 0].astype(F32)
                    + in_c4[i].astype(F32)
                )
        for e in range(each):
            if not at < (e + 1) * W <= at + size:
                continue
            msend[e] = tmp[e * W : (e + 1) * W].T.astype(BF16)

            def send(e=e):
                for side in range(2):
                    mirror_copy(e, side).start()

            when_sent(e, send)
            where = lanes((q + core * each + e) % chips, W)
            term_ref[:, where] = tmp[pl.ds(pl.multiple_of(e * W + core * w, w), w), :]
            other = pl.ds(pl.multiple_of(e * W + (1 - core) * w, w), w)
            dsend[:, e * W : (e + 1) * W] = tmp[other, :].astype(BF16)
        if part < 2:
            return None
        direct = to(dsend, drecv, mate)
        extra = jnp.concatenate([tmp[each * W :, :w], tmp[each * W :, w:]], axis=0)
        col = 2 * ((q + half) % chips) + (core + q // half) % 2
        term_ref[:, lanes(col, w)] = extra
        xsend[...] = extra.T.astype(BF16)
        mirrored = to(xsend, xrecv, col)
        return direct, mirrored

    def close(direct, mirrored):
        direct.wait_recv()
        for e in range(each):
            where = lanes((q + (1 - core) * each + e) % chips, W)
            term_ref[:, where] = drecv[:, e * W : (e + 1) * W].astype(F32)
        for d in range(1, half):
            pltpu.make_async_remote_copy(
                src_ref=mrecv.at[d], dst_ref=mrecv.at[d], send_sem=msem.at[0], recv_sem=mrsem.at[d],
                device_id={"dp": mate}, device_id_type=MESH,
            ).wait_recv()
            term_ref[:, lanes((q + chips - d) % chips, W)] = mrecv[d].astype(F32)
        mirrored.wait_recv()
        far_chip = (q + half) % chips
        col = 2 * far_chip + (core + far_chip // half) % 2
        term_ref[:, lanes(col, w)] = xrecv[...].astype(F32)

    def wait_sends():
        assert count[0] == s.slots()
        for copy in started:
            copy.wait_send()
        for e in range(each):

            def sent(e=e):
                for side in range(2):
                    mirror_copy(e, side).wait_send()

            when_sent(e, sent)

    meet()
    swapped = swap_grads()
    t_copies = swap_tests()
    own_copies[0].wait()
    grads_here(swapped[: half // 2 + 2])
    early = swap_factor(0, 3, 2, 1)
    compute(3, 0, 1)
    first(3, 1)
    relayed = relay_tests(t_copies)
    grads_here(swapped[half // 2 + 2 :])
    compute(3, 1, 3)
    first(3, 0)
    compute(3, 3, 4)
    compute(2)
    first(2, 1)
    early += hand_tests(t_copies)
    second(3)
    first(2, 0)
    early += hand_relayed(relayed)
    compute(1)
    c_first()
    third(3)
    precondition(early)
    first(1, 1)
    precondition_second()
    second(2)
    first(1, 0)
    compute(0)
    c_second()
    along_z = gather_first()
    third(2)
    first(0, 1)
    second(1)
    c_third()
    first(0, 0)
    relayed = gather_relay(along_z)
    second(0)
    c_fourth()
    gx, gy, mate_own = gather_second(along_z, relayed)
    third(1)
    scores_start()
    score(0, 0, 1)
    third(0)
    diagonal = gather_third(gx, gy)
    finish(0)
    finish(1)
    direct, mirrored = finish(2)
    mates = gather_mates(gx, gy)
    score(0, 1, 3)
    grads_here([mate_own] + mates)
    score(1, 0, 3)
    mate_diagonal = gather_fourth(diagonal)
    score(0, 3, 4)
    grads_here([mate_diagonal])
    score(1, 3, 4)
    close(direct, mirrored)
    wait_sends()

def window(grads, covariance, test_grads, inverse_factor):
    n = lax.axis_size("dp")
    rows, k = grads.shape
    s = Sizes(n, rows, k, test_grads.shape[0])
    scratch = s.scratch()
    term, scores = pl.pallas_call(
        functools.partial(kernel, s, list(scratch)),
        out_shape=(
            jax.ShapeDtypeStruct((s.w, k), F32),
            jax.ShapeDtypeStruct((rows, s.tests), F32),
        ),
        in_specs=[pl.BlockSpec(memory_space=pltpu.HBM)] * 3,
        out_specs=(
            pl.BlockSpec(memory_space=pltpu.VMEM),
            pl.BlockSpec(memory_space=pltpu.VMEM),
        ),
        scratch_shapes=list(scratch.values()),
        compiler_params=pltpu.CompilerParams(
            collective_id=0, has_side_effects=True, vmem_limit_bytes=49 * 1024 * 1024
        ),
    )(*(pltpu.with_memory_space_constraint(a, pltpu.HBM) for a in (grads, test_grads, inverse_factor)))
    return scores, 0.9 * covariance + term / (rows * n)


def solution(mesh):
    placed = (P("dp", "feat"), P("dp", "feat"), P("feat", "dp"), P("dp", None))
    whole = mesh.shape["feat"] == 1 and mesh.shape["dp"] == 32
    return jax.shard_map(
        window if whole else general,
        mesh=mesh,
        in_specs=placed,
        out_specs=(P("dp", "feat"), P("dp", "feat")),
        check_vma=False,
    )
```

```python
import functools

import jax
import jax.numpy as jnp
from jax import lax
from jax.experimental import pallas as pl
from jax.experimental.pallas import tpu as pltpu
from jax.sharding import PartitionSpec as P

F32 = jnp.float32
BF16 = jnp.bfloat16
MESH = pl.DeviceIdType.MESH


def general(grads, covariance, test_grads, inverse_factor):
    all_features = lax.all_gather(grads, "feat", axis=1, tiled=True)
    examples = grads.shape[0] * lax.axis_size("dp")
    tested = lax.dot_general(
        inverse_factor, test_grads, (((0,), (1,)), ((), ())), preferred_element_type=F32
    )
    term = lax.dot_general(
        all_features, grads, (((0,), (0,)), ((), ())), preferred_element_type=F32
    )
    joined = lax.psum_scatter(
        jnp.concatenate([term, tested], axis=1), "dp", scatter_dimension=0, tiled=True
    )
    width = grads.shape[1]
    owned_pre = joined[:, width:].astype(BF16)
    pre_columns = lax.all_gather(owned_pre, "dp", axis=0, tiled=True)
    scores = jnp.dot(all_features, pre_columns, preferred_element_type=F32)
    return scores, 0.9 * covariance + joined[:, :width] / examples


class Sizes:
    def __init__(self, n, rows, k, tests):
        self.n, self.rows, self.k, self.tests = n, rows, k, tests
        self.chips, self.far, self.w = n // 2, n // 8, k // n
        self.W = 2 * self.w
        self.half = self.chips // 2
        self.each = self.half // 2
        self.strip = self.each * self.W + self.w // 2
        self.rc = self.w // 2
        self.ra = (self.strip - self.rc) // 2
        self.rb = self.ra
        self.mh = tests // 2

    def scratch(self):
        far, w, W, tests = self.far, self.w, self.W, self.tests
        far1 = max(far - 1, 1)
        v = pltpu.VMEM
        return dict(
            gbuf=v((2 * self.rows, self.k), BF16),
            gt=v((W, 2 * self.rows), BF16),
            tmp=v((self.strip, W), F32),
            part_a=v((far, 2, self.ra, W), F32),
            part_b=v((far, 2, self.rb, W), F32),
            out_a1=v((far, 2, self.ra, W), BF16),
            out_b1=v((far, 2, self.rb, W), BF16),
            in_a1=v((far, 2, self.ra, W), BF16),
            in_b1=v((far, 2, self.rb, W), BF16),
            out_a2=v((far, self.ra, W), BF16),
            out_b2=v((far, self.rb, W), BF16),
            in_a2=v((far, self.ra, W), BF16),
            in_b2=v((far, self.rb, W), BF16),
            out_az=v((far1, self.ra, W), BF16),
            out_bz=v((far1, self.rb, W), BF16),
            in_az=v((far1, self.ra, W), BF16),
            in_bz=v((far1, self.rb, W), BF16),
            part_c=v((2, 4, self.rc, W), F32),
            out_c1=v((2, 4, self.rc, W), BF16),
            in_c1=v((2, 4, self.rc, W), BF16),
            out_c2=v((4, self.rc, W), BF16),
            in_c2=v((4, self.rc, W), BF16),
            out_c3=v((2, 2, self.rc // 2, W), BF16),
            in_c3=v((2, 2, self.rc // 2, W), BF16),
            out_c4=v((2, self.rc // 2, W), BF16),
            in_c4=v((2, self.rc // 2, W), BF16),
            fbuf=v((2 * far * w, 4 * w), BF16),
            tbuf=v((tests, 2 * far * w), BF16),
            pp=v((tests, 4 * w), F32),
            in_p1=v((2, 2, self.mh, w), F32),
            out_p2=v((2, self.mh, w), F32),
            in_p2=v((2, self.mh, w), F32),
            pfull=v((tests, self.k), BF16),
            msend=v((self.each, W, W), BF16),
            mrecv=v((self.half, w, W), BF16),
            xsend=v((w, w), BF16),
            xrecv=v((w, w), BF16),
            dsend=v((w, self.each * W), BF16),
            drecv=v((w, self.each * W), BF16),
            ssem=pltpu.SemaphoreType.DMA((self.slots(),)),
            rsem=pltpu.SemaphoreType.DMA((self.slots(),)),
            msem=pltpu.SemaphoreType.DMA((2 * self.each,)),
            mrsem=pltpu.SemaphoreType.DMA((self.half,)),
            lsem=pltpu.SemaphoreType.DMA((4,)),
        )

    def slots(self):
        return 72 + self.chips


def kernel(s, names, g_hbm, t_hbm, f_hbm, term_ref, scores_ref, *refs):
    r = dict(zip(names, refs))
    n, far, w, W, chips, half, each = s.n, s.far, s.w, s.W, s.chips, s.half, s.each
    rows, mh, ra, rb = s.rows, s.mh, s.ra, s.rb
    me = lax.axis_index("dp")
    core, x, y, z = me % 2, me // 2 % 2, me // 4 % 2, me // 8
    q = me // 2

    def device(zz, yy, xx, cc):
        return ((zz * 2 + yy) * 2 + xx) * 2 + cc

    def over(g):
        return (z, z + 1 - 2 * (z % 2), (z + 2) % far, far - 1 - z)[g]

    mate = device(z, y, x, 1 - core)
    x_to = device(z, y, 1 - x, core)
    y_to = device(z, 1 - y, x, core)
    ssem, rsem = r["ssem"], r["rsem"]
    started = []
    count = [0]

    def to(src, dst, target, start=True):
        i = count[0]
        count[0] += 1
        copy = pltpu.make_async_remote_copy(
            src_ref=src, dst_ref=dst, send_sem=ssem.at[i], recv_sem=rsem.at[i],
            device_id={"dp": target}, device_id_type=MESH,
        )
        if start:
            copy.start()
        started.append(copy)
        return copy

    def lanes(block, width):
        return pl.ds(pl.multiple_of(block * width, width), width)

    gbuf, fbuf, tbuf = r["gbuf"], r["fbuf"], r["tbuf"]
    own_copies = [
        pltpu.make_async_copy(g_hbm, gbuf.at[pl.ds(0, rows)], r["lsem"].at[0]),
        pltpu.make_async_copy(t_hbm, tbuf.at[:, pl.ds(0, w)], r["lsem"].at[1]),
        pltpu.make_async_copy(
            f_hbm.at[:, lanes(core * far + z, 4 * w)], fbuf.at[pl.ds(0, w)], r["lsem"].at[2]
        ),
    ]

    barrier = pltpu.get_barrier_semaphore()

    def greet(targets):
        for target in targets:
            pl.semaphore_signal(barrier, inc=1, device_id={"dp": target}, device_id_type=MESH)

    def meet_plane():
        greet([mate, x_to, y_to])
        for copy in own_copies:
            copy.start()
        pl.semaphore_wait(barrier, 3 + z)
        greet([device(over(g), y, x, core) for g in range(1, far)])

    t_copies = []

    def meet_line():
        @pl.when(z < far - 1)
        def _():
            pl.semaphore_wait(barrier, far - 1 - z)

        for copy in t_copies:
            copy.start()

    def swap_grads():
        there = 1 - core
        begin = (over(3) * 2 + 1 - y) * 2 + 1 - x
        last = half // 2
        steps = [0] + [i + last * there for i in range(1, last)]
        steps += [half - last * there, last + last * there]
        steps += [i - last * there for i in range(last + 1, half)] + list(range(half + 1, chips))
        parts = [lanes((begin + i) % chips, W) for i in steps]
        return [
            to(g_hbm.at[:, part], gbuf.at[pl.ds(rows, rows), part], mate) for part in parts
        ]

    def hand(g, target, came):
        return to(tbuf.at[:, pl.ds(2 * g * w, w)], tbuf.at[:, pl.ds(came * w, w)], target)

    def swap_tests():
        return [
            to(t_hbm, tbuf.at[:, pl.ds(2 * g * w, w)], device(over(g), y, x, core), False)
            for g in (1, 2)
        ]

    def swap_factor(*groups):
        return [
            to(
                f_hbm.at[:, lanes((core + h) % 2 * far + over(g), 4 * w)],
                fbuf.at[pl.ds((2 * g + h) * w, w)],
                device(over(g), y, x, (core + h) % 2),
            )
            for g in groups
            for h in range(2)
            if g or h
        ]

    def relay_tests(copies):
        copies[1].wait_recv()
        return hand(2, device(over(1), y, x, core), 6)

    def hand_tests(copies):
        own_copies[1].wait()
        copies[0].wait_recv()
        return [hand(g, mate, 2 * g + 1) for g in range(3)]

    def hand_relayed(copy):
        copy.wait_recv()
        return [hand(3, mate, 7)]

    def grads_here(copies):
        for copy in copies:
            copy.wait_recv()

    gt, tmp = r["gt"], r["tmp"]
    part_c, out_c1, in_c1, out_c2, in_c2 = (
        r["part_c"], r["out_c1"], r["in_c1"], r["out_c2"], r["in_c2"]
    )
    out_c3, in_c3, out_c4, in_c4 = r["out_c3"], r["in_c3"], r["out_c4"], r["in_c4"]
    part_a, part_b, out_a1, out_b1 = r["part_a"], r["part_b"], r["out_a1"], r["out_b1"]

    def compute(g, first=0, last=4):
        def strip(i, carry):
            oy, ox = (3 - i) // 2, (3 - i) % 2
            own = (over(g) * 2 + (y + oy) % 2) * 2 + (x + ox) % 2
            gt[...] = gbuf[:, lanes(own, W)].T
            for e in range(each):
                col = (own + core * each + e) % chips
                tmp[e * W : (e + 1) * W] = jnp.dot(
                    gt[...], gbuf[:, lanes(col, W)], preferred_element_type=F32
                )
            col = 2 * ((own + half) % chips) + (core + own // half) % 2
            extra = jnp.dot(
                gt[pl.ds(pl.multiple_of(core * w, w), w), :], gbuf[:, lanes(col, w)],
                preferred_element_type=F32,
            )
            tmp[each * W :, :w] = extra[: w // 2]
            tmp[each * W :, w:] = extra[w // 2 :]

            @pl.when(ox == 0)
            def _():
                part_a[g, oy] = tmp[:ra]

            @pl.when(ox == 1)
            def _():
                out_a1[g, oy] = tmp[:ra].astype(BF16)

            @pl.when(oy == 0)
            def _():
                part_b[g, ox] = tmp[ra : ra + rb]

            @pl.when(oy == 1)
            def _():
                out_b1[g, ox] = tmp[ra : ra + rb].astype(BF16)

            if g % 2:
                out_c1[g // 2, 3 - i] = tmp[ra + rb :].astype(BF16)
            else:
                part_c[g // 2, 3 - i] = tmp[ra + rb :]
            return carry

        lax.fori_loop(first, last, strip, 0)

    a1, b1, a2, b2, az, bz = {}, {}, {}, {}, {}, {}

    def first(g, o):
        a1[g, o] = to(out_a1.at[g, o], r["in_a1"].at[g, o], x_to)
        b1[g, o] = to(out_b1.at[g, o], r["in_b1"].at[g, o], y_to)

    def second(g):
        a1[g, 1].wait_recv()
        r["out_a2"][g] = (part_a[g, 1] + r["in_a1"][g, 1].astype(F32)).astype(BF16)
        a2[g] = to(r["out_a2"].at[g], r["in_a2"].at[g], y_to)
        b1[g, 1].wait_recv()
        r["out_b2"][g] = (part_b[g, 1] + r["in_b1"][g, 1].astype(F32)).astype(BF16)
        b2[g] = to(r["out_b2"].at[g], r["in_b2"].at[g], x_to)

    def third(g):
        a1[g, 0].wait_recv()
        a2[g].wait_recv()
        total_a = part_a[g, 0] + r["in_a1"][g, 0].astype(F32) + r["in_a2"][g].astype(F32)
        b1[g, 0].wait_recv()
        b2[g].wait_recv()
        total_b = part_b[g, 0] + r["in_b1"][g, 0].astype(F32) + r["in_b2"][g].astype(F32)
        if g == 0:
            part_a[0, 0] = total_a
            part_b[0, 0] = total_b
            return
        if g == 2:
            az[3].wait_recv()
            total_a = total_a + r["in_az"][2].astype(F32)
            bz[3].wait_recv()
            total_b = total_b + r["in_bz"][2].astype(F32)
        target = device(over(2 if g == 2 else 1), y, x, core)
        slot = {3: 2, 2: 1, 1: 0}[g]
        r["out_az"][slot] = total_a.astype(BF16)
        az[g] = to(r["out_az"].at[slot], r["in_az"].at[slot], target)
        r["out_bz"][slot] = total_b.astype(BF16)
        bz[g] = to(r["out_bz"].at[slot], r["in_bz"].at[slot], target)

    c1, c2, c3, c4 = {}, [], {}, {}
    hc = s.rc // 2

    def c_first():
        for slot in (1, 0):
            c1[slot] = to(out_c1.at[slot], in_c1.at[slot], device(over(1), y, x, core))

    def c_second():
        c1[1].wait_recv()
        out_c2[...] = (part_c[1] + in_c1[1].astype(F32)).astype(BF16)
        c2.append(to(out_c2, in_c2, device(over(2), y, x, core)))

    def c_third():
        c1[0].wait_recv()
        c2[0].wait_recv()
        part_c[0] = part_c[0] + in_c1[0].astype(F32) + in_c2[...].astype(F32)
        for o in range(2):
            out_c3[0, o] = part_c[0, 2 * o + 1, :hc].astype(BF16)
            out_c3[1, o] = part_c[0, 2 + o, hc:].astype(BF16)
        c3[0] = to(out_c3.at[0], in_c3.at[0], x_to)
        c3[1] = to(out_c3.at[1], in_c3.at[1], y_to)

    def c_fourth():
        c3[0].wait_recv()
        out_c4[0] = (part_c[0, 2, :hc] + in_c3[0, 1].astype(F32)).astype(BF16)
        c4[0] = to(out_c4.at[0], in_c4.at[0], y_to)
        c3[1].wait_recv()
        out_c4[1] = (part_c[0, 1, hc:] + in_c3[1, 1].astype(F32)).astype(BF16)
        c4[1] = to(out_c4.at[1], in_c4.at[1], x_to)

    pp, in_p1, out_p2, in_p2, pfull = r["pp"], r["in_p1"], r["out_p2"], r["in_p2"], r["pfull"]
    sub = lambda oy, ox: (y + oy) % 2 * 2 + (x + ox) % 2
    p1, p2 = {}, {}

    def precondition(handed):
        own_copies[2].wait()
        for copy in handed:
            copy.wait_recv()
        pp[...] = jnp.dot(tbuf[...], fbuf[...], preferred_element_type=F32)
        for o in (1, 0):
            p1[0, o] = to(pp.at[pl.ds(0, mh), lanes(sub(o, 1), w)], in_p1.at[0, o], x_to)
            p1[1, o] = to(pp.at[pl.ds(mh, mh), lanes(sub(1, o), w)], in_p1.at[1, o], y_to)

    def precondition_second():
        p1[0, 1].wait_recv()
        out_p2[0] = pp[:mh, lanes(sub(1, 0), w)] + in_p1[0, 1]
        p2[0] = to(out_p2.at[0], in_p2.at[0], y_to)
        p1[1, 1].wait_recv()
        out_p2[1] = pp[mh:, lanes(sub(0, 1), w)] + in_p1[1, 1]
        p2[1] = to(out_p2.at[1], in_p2.at[1], x_to)

    def place(oy, ox, part=0, parts=1):
        return lanes((core * 4 + sub(oy, ox)) * parts + part, far * w // parts)

    def pass_on(where, target):
        return to(pfull.at[:, where], pfull.at[:, where], target)

    def gather_first():
        p1[0, 0].wait_recv()
        p2[0].wait_recv()
        own = lanes((core * 4 + sub(0, 0)) * far + z, w)
        pfull[:mh, own] = (pp[:mh, lanes(sub(0, 0), w)] + in_p1[0, 0] + in_p2[0]).astype(BF16)
        p1[1, 0].wait_recv()
        p2[1].wait_recv()
        pfull[mh:, own] = (pp[mh:, lanes(sub(0, 0), w)] + in_p1[1, 0] + in_p2[1]).astype(BF16)
        return [pass_on(own, device(over(g), y, x, core)) for g in (1, 2)]

    def gather_relay(along_z):
        along_z[1].wait_recv()
        there = lanes((core * 4 + sub(0, 0)) * far + over(2), w)
        return pass_on(there, device(over(1), y, x, core))

    def gather_second(along_z, relayed):
        along_z[0].wait_recv()
        relayed.wait_recv()
        gx = [pass_on(place(0, 0, i, 2), x_to) for i in range(2)]
        gy = [pass_on(place(0, 0, i, 2), y_to) for i in (1, 0)]
        return gx, gy, pass_on(place(0, 0), mate)

    def gather_third(gx, gy):
        gx[0].wait_recv()
        diagonal = [pass_on(place(0, 1, 0, 2), y_to)]
        gy[0].wait_recv()
        return diagonal + [pass_on(place(1, 0, 1, 2), x_to)]

    def gather_mates(gx, gy):
        gx[1].wait_recv()
        mates = [pass_on(place(0, 1), mate)]
        gy[1].wait_recv()
        return mates + [pass_on(place(1, 0), mate)]

    def gather_fourth(diagonal):
        for copy in diagonal:
            copy.wait_recv()
        return pass_on(place(1, 1), mate)

    def score(other, first, last):
        def chunk(i, carry):
            cc, at = (core + other) % 2, sub(i // 2, i % 2)
            left = jnp.concatenate(
                [gbuf[:rows, lanes((cc * far + zz) * 4 + at, w)] for zz in range(far)], axis=1
            )
            scores_ref[...] += lax.dot_general(
                left, pfull[:, lanes(cc * 4 + at, far * w)], (((1,), (1,)), ((), ())),
                preferred_element_type=F32,
            )
            return carry

        lax.fori_loop(first, last, chunk, 0)

    def scores_start():
        scores_ref[...] = jnp.zeros_like(scores_ref)

    msend, mrecv, msem, mrsem = r["msend"], r["mrecv"], r["msem"], r["mrsem"]
    dsend, drecv, xsend, xrecv = r["dsend"], r["drecv"], r["xsend"], r["xrecv"]

    def mirror_copy(e, side):
        d = core * each + e
        return pltpu.make_async_remote_copy(
            src_ref=msend.at[e, pl.ds(side * w, w)], dst_ref=mrecv.at[d],
            send_sem=msem.at[2 * e + side], recv_sem=mrsem.at[d],
            device_id={"dp": 2 * ((q + d) % chips) + side}, device_id_type=MESH,
        )

    def when_sent(e, act):
        if e:
            act()
        else:
            pl.when(core == 1)(act)

    def finish(part):
        if part < 2:
            sums, came, copies, size = (
                (part_a, r["in_az"], az, ra), (part_b, r["in_bz"], bz, rb)
            )[part]
            at = part * ra
            for g in (1, 2):
                copies[g].wait_recv()
            tmp[at : at + size] = sums[0, 0] + came[0].astype(F32) + came[1].astype(F32)
        else:
            at, size = ra + rb, s.rc
            for i in range(2):
                c4[i].wait_recv()
                tmp[at + i * hc : at + (i + 1) * hc] = (
                    part_c[0, 0, i * hc : (i + 1) * hc]
                    + in_c3[i, 0].astype(F32)
                    + in_c4[i].astype(F32)
                )
        for e in range(each):
            if not at < (e + 1) * W <= at + size:
                continue
            msend[e] = tmp[e * W : (e + 1) * W].T.astype(BF16)

            def send(e=e):
                for side in range(2):
                    mirror_copy(e, side).start()

            when_sent(e, send)
            where = lanes((q + core * each + e) % chips, W)
            term_ref[:, where] = tmp[pl.ds(pl.multiple_of(e * W + core * w, w), w), :]
            other = pl.ds(pl.multiple_of(e * W + (1 - core) * w, w), w)
            dsend[:, e * W : (e + 1) * W] = tmp[other, :].astype(BF16)
        if part < 2:
            return None
        direct = to(dsend, drecv, mate)
        extra = jnp.concatenate([tmp[each * W :, :w], tmp[each * W :, w:]], axis=0)
        col = 2 * ((q + half) % chips) + (core + q // half) % 2
        term_ref[:, lanes(col, w)] = extra
        xsend[...] = extra.T.astype(BF16)
        mirrored = to(xsend, xrecv, col)
        return direct, mirrored

    def close(direct, mirrored):
        direct.wait_recv()
        for e in range(each):
            where = lanes((q + (1 - core) * each + e) % chips, W)
            term_ref[:, where] = drecv[:, e * W : (e + 1) * W].astype(F32)
        for d in range(1, half):
            pltpu.make_async_remote_copy(
                src_ref=mrecv.at[d], dst_ref=mrecv.at[d], send_sem=msem.at[0], recv_sem=mrsem.at[d],
                device_id={"dp": mate}, device_id_type=MESH,
            ).wait_recv()
            term_ref[:, lanes((q + chips - d) % chips, W)] = mrecv[d].astype(F32)
        mirrored.wait_recv()
        far_chip = (q + half) % chips
        col = 2 * far_chip + (core + far_chip // half) % 2
        term_ref[:, lanes(col, w)] = xrecv[...].astype(F32)

    def wait_sends():
        assert count[0] == s.slots()
        for copy in started:
            copy.wait_send()
        for e in range(each):

            def sent(e=e):
                for side in range(2):
                    mirror_copy(e, side).wait_send()

            when_sent(e, sent)

    meet_plane()
    swapped = swap_grads()
    t_copies += swap_tests()
    pl.when(z >= far // 2)(meet_line)
    own_copies[0].wait()
    grads_here(swapped[: half // 2 + 2])
    compute(3, 0, 1)
    first(3, 1)
    pl.when(z < far // 2)(meet_line)
    grads_here(swapped[half // 2 + 2 :])
    compute(3, 1, 3)
    first(3, 0)
    compute(3, 3, 4)
    relayed = relay_tests(t_copies)
    early = swap_factor(0, 3, 2, 1)
    compute(2)
    first(2, 1)
    early += hand_tests(t_copies)
    second(3)
    first(2, 0)
    early += hand_relayed(relayed)
    compute(1)
    first(1, 1)
    c_first()
    third(3)
    precondition(early)
    precondition_second()
    second(2)
    first(1, 0)
    compute(0)
    c_second()
    first(0, 1)
    along_z = gather_first()
    second(1)
    relayed = gather_relay(along_z)
    third(2)
    first(0, 0)
    c_third()
    second(0)
    c_fourth()
    gx, gy, mate_own = gather_second(along_z, relayed)
    third(1)
    scores_start()
    score(0, 0, 1)
    third(0)
    diagonal = gather_third(gx, gy)
    finish(0)
    finish(1)
    direct, mirrored = finish(2)
    mates = gather_mates(gx, gy)
    score(0, 1, 3)
    grads_here([mate_own] + mates)
    score(1, 0, 3)
    mate_diagonal = gather_fourth(diagonal)
    score(0, 3, 4)
    grads_here([mate_diagonal])
    score(1, 3, 4)
    close(direct, mirrored)
    wait_sends()

def window(grads, covariance, test_grads, inverse_factor):
    n = lax.axis_size("dp")
    rows, k = grads.shape
    s = Sizes(n, rows, k, test_grads.shape[0])
    scratch = s.scratch()
    term, scores = pl.pallas_call(
        functools.partial(kernel, s, list(scratch)),
        out_shape=(
            jax.ShapeDtypeStruct((s.w, k), F32),
            jax.ShapeDtypeStruct((rows, s.tests), F32),
        ),
        in_specs=[pl.BlockSpec(memory_space=pltpu.HBM)] * 3,
        out_specs=(
            pl.BlockSpec(memory_space=pltpu.VMEM),
            pl.BlockSpec(memory_space=pltpu.VMEM),
        ),
        scratch_shapes=list(scratch.values()),
        compiler_params=pltpu.CompilerParams(
            collective_id=0, has_side_effects=True, vmem_limit_bytes=49 * 1024 * 1024
        ),
    )(*(pltpu.with_memory_space_constraint(a, pltpu.HBM) for a in (grads, test_grads, inverse_factor)))
    return scores, 0.9 * covariance + term / (rows * n)


def solution(mesh):
    placed = (P("dp", "feat"), P("dp", "feat"), P("feat", "dp"), P("dp", None))
    whole = mesh.shape["feat"] == 1 and mesh.shape["dp"] == 32
    return jax.shard_map(
        window if whole else general,
        mesh=mesh,
        in_specs=placed,
        out_specs=(P("dp", "feat"), P("dp", "feat")),
        check_vma=False,
    )
```

```python
import functools

import jax
import jax.numpy as jnp
from jax import lax
from jax.experimental import pallas as pl
from jax.experimental.pallas import tpu as pltpu
from jax.sharding import PartitionSpec as P

F32 = jnp.float32
BF16 = jnp.bfloat16
MESH = pl.DeviceIdType.MESH


def general(grads, covariance, test_grads, inverse_factor):
    all_features = lax.all_gather(grads, "feat", axis=1, tiled=True)
    examples = grads.shape[0] * lax.axis_size("dp")
    tested = lax.dot_general(
        inverse_factor, test_grads, (((0,), (1,)), ((), ())), preferred_element_type=F32
    )
    term = lax.dot_general(
        all_features, grads, (((0,), (0,)), ((), ())), preferred_element_type=F32
    )
    joined = lax.psum_scatter(
        jnp.concatenate([term, tested], axis=1), "dp", scatter_dimension=0, tiled=True
    )
    width = grads.shape[1]
    owned_pre = joined[:, width:].astype(BF16)
    pre_columns = lax.all_gather(owned_pre, "dp", axis=0, tiled=True)
    scores = jnp.dot(all_features, pre_columns, preferred_element_type=F32)
    return scores, 0.9 * covariance + joined[:, :width] / examples


class Sizes:
    def __init__(self, n, rows, k, tests):
        self.n, self.rows, self.k, self.tests = n, rows, k, tests
        self.chips, self.far, self.w = n // 2, n // 8, k // n
        self.W = 2 * self.w
        self.half = self.chips // 2
        self.each = self.half // 2
        self.strip = self.each * self.W + self.w // 2
        self.rc = 3 * self.w // 4
        self.hc = self.rc // 2
        self.hs = self.hc - self.w // 4
        self.ra = (self.strip - self.rc) // 2
        self.rb = self.ra
        self.mh = tests // 2

    def scratch(self):
        far, w, W, tests = self.far, self.w, self.W, self.tests
        far1 = max(far - 1, 1)
        v = pltpu.VMEM
        return dict(
            gbuf=v((2 * self.rows, self.k), BF16),
            gt=v((W, 2 * self.rows), BF16),
            tmp=v((self.strip, W), F32),
            part_a=v((far, 2, self.ra, W), F32),
            part_b=v((far, 2, self.rb, W), F32),
            out_a1=v((far, 2, self.ra, W), BF16),
            out_b1=v((far, 2, self.rb, W), BF16),
            in_a1=v((far, 2, self.ra, W), BF16),
            in_b1=v((far, 2, self.rb, W), BF16),
            out_a2=v((far, self.ra, W), BF16),
            out_b2=v((far, self.rb, W), BF16),
            in_a2=v((far, self.ra, W), BF16),
            in_b2=v((far, self.rb, W), BF16),
            out_az=v((far1, self.ra, W), BF16),
            out_bz=v((far1, self.rb, W), BF16),
            in_az=v((far1, self.ra, W), BF16),
            in_bz=v((far1, self.rb, W), BF16),
            part_c=v((2, 2, 4, self.hc, W), F32),
            out_c1=v((2, 2, 4, self.hc, W), BF16),
            in_c1=v((2, 2, 4, self.hc, W), BF16),
            out_c2=v((2, 4, self.hc, W), BF16),
            in_c2=v((2, 4, self.hc, W), BF16),
            out_c3=v((2, 2, self.hc, W), BF16),
            in_c3=v((2, 2, self.hc, W), BF16),
            out_c4=v((2, self.hc, W), BF16),
            in_c4=v((2, self.hc, W), BF16),
            extra=v((w, w), F32),
            fbuf=v((2 * far * w, 4 * w), BF16),
            tbuf=v((tests, 2 * far * w), BF16),
            pp=v((tests, 4 * w), F32),
            in_p1=v((2, 2, self.mh, w), F32),
            out_p2=v((2, self.mh, w), F32),
            in_p2=v((2, self.mh, w), F32),
            pfull=v((tests, self.k), BF16),
            msend=v((self.each, W, W), BF16),
            mrecv=v((self.half, w, W), BF16),
            xsend=v((w, w), BF16),
            xrecv=v((w, w), BF16),
            dsend=v((w, self.each * W), BF16),
            drecv=v((w, self.each * W), BF16),
            ssem=pltpu.SemaphoreType.DMA((self.sends,)),
            rsem=pltpu.SemaphoreType.DMA((self.receipts,)),
            msem=pltpu.SemaphoreType.DMA((2 * self.each,)),
            mrsem=pltpu.SemaphoreType.DMA((self.half,)),
            lsem=pltpu.SemaphoreType.DMA((4,)),
        )

    sends, receipts = 43, 68


def kernel(s, names, g_hbm, t_hbm, f_hbm, term_ref, scores_ref, *refs):
    r = dict(zip(names, refs))
    n, far, w, W, chips, half, each = s.n, s.far, s.w, s.W, s.chips, s.half, s.each
    rows, mh, ra, rb, hc, hs = s.rows, s.mh, s.ra, s.rb, s.hc, s.hs
    mid = ra + rb + hc
    me = lax.axis_index("dp")
    core, x, y, z = me % 2, me // 2 % 2, me // 4 % 2, me // 8
    q = me // 2

    def device(zz, yy, xx, cc):
        return ((zz * 2 + yy) * 2 + xx) * 2 + cc

    def over(g):
        return (z, z + 1 - 2 * (z % 2), (z + 2) % far, far - 1 - z)[g]

    mate = device(z, y, x, 1 - core)
    x_to = device(z, y, 1 - x, core)
    y_to = device(z, 1 - y, x, core)
    ssem, rsem = r["ssem"], r["rsem"]
    started = []
    count = [0, 0]
    shared = [{}, {}]

    def slot(kind, name):
        if name in shared[kind]:
            return shared[kind][name]
        i = count[kind]
        count[kind] += 1
        if name:
            shared[kind][name] = i
        return i

    def to(src, dst, target, start=True, sent=None, came=None):
        copy = pltpu.make_async_remote_copy(
            src_ref=src, dst_ref=dst, send_sem=ssem.at[slot(0, sent)],
            recv_sem=rsem.at[slot(1, came)], device_id={"dp": target}, device_id_type=MESH,
        )
        if start:
            copy.start()
        if not sent:
            started.append(copy)
        return copy

    def bytes_of(ref, sent=None, came=None):
        return pltpu.make_async_remote_copy(
            src_ref=ref, dst_ref=ref, send_sem=ssem.at[shared[0][sent] if sent else 0],
            recv_sem=rsem.at[shared[1][came] if came else 0],
            device_id={"dp": mate}, device_id_type=MESH,
        )

    class Either:
        def __init__(self, src, dst, small, target):
            i, j = slot(0, None), slot(1, None)
            self.copies = [
                pltpu.make_async_remote_copy(
                    src_ref=a, dst_ref=b, send_sem=ssem.at[i], recv_sem=rsem.at[j],
                    device_id={"dp": target}, device_id_type=MESH,
                )
                for a, b in ((src.at[small], dst.at[small]), (src, dst))
            ]
            started.append(self)
            self.each(lambda copy: copy.start())

        def each(self, act):
            for i in range(2):
                pl.when(core == i)(functools.partial(act, self.copies[i]))

        def wait_recv(self):
            self.each(lambda copy: copy.wait_recv())

        def wait_send(self):
            self.each(lambda copy: copy.wait_send())

    def lanes(block, width):
        return pl.ds(pl.multiple_of(block * width, width), width)

    gbuf, fbuf, tbuf = r["gbuf"], r["fbuf"], r["tbuf"]
    own_copies = [
        pltpu.make_async_copy(g_hbm, gbuf.at[pl.ds(0, rows)], r["lsem"].at[0]),
        pltpu.make_async_copy(t_hbm, tbuf.at[:, pl.ds(0, w)], r["lsem"].at[1]),
        pltpu.make_async_copy(
            f_hbm.at[:, lanes(core * far + z, 4 * w)], fbuf.at[pl.ds(0, w)], r["lsem"].at[2]
        ),
    ]

    barrier = pltpu.get_barrier_semaphore()

    def greet(targets):
        for target in targets:
            pl.semaphore_signal(barrier, inc=1, device_id={"dp": target}, device_id_type=MESH)

    def meet_plane():
        greet([mate, x_to, y_to])
        for copy in own_copies:
            copy.start()
        pl.semaphore_wait(barrier, 3 + z)
        greet([device(over(g), y, x, core) for g in range(1, far)])

    t_copies = []

    def meet_line():
        @pl.when(z < far - 1)
        def _():
            pl.semaphore_wait(barrier, far - 1 - z)

        for copy in t_copies:
            copy.start()

    soon = half // 2 + 2

    def swap_grads():
        there = 1 - core
        begin = (over(3) * 2 + 1 - y) * 2 + 1 - x
        last = half // 2
        steps = [0] + [i + last * there for i in range(1, last)]
        steps += [half - last * there, last + last * there]
        steps += [i - last * there for i in range(last + 1, half)] + list(range(half + 1, chips))
        parts = [lanes((begin + i) % chips, W) for i in steps]
        for i, part in enumerate(parts):
            to(
                g_hbm.at[:, part], gbuf.at[pl.ds(rows, rows), part], mate,
                sent="g", came="g0" if i < soon else "g1",
            )

    def hand(g, target, came):
        return to(tbuf.at[:, pl.ds(2 * g * w, w)], tbuf.at[:, pl.ds(came * w, w)], target)

    def swap_tests():
        return [
            to(t_hbm, tbuf.at[:, pl.ds(2 * g * w, w)], device(over(g), y, x, core), False)
            for g in (1, 2)
        ]

    def swap_factor(*groups):
        return [
            to(
                f_hbm.at[:, lanes((core + h) % 2 * far + over(g), 4 * w)],
                fbuf.at[pl.ds((2 * g + h) * w, w)],
                device(over(g), y, x, (core + h) % 2),
                sent="f", came="f",
            )
            for g in groups
            for h in range(2)
            if g or h
        ]

    def relay_tests(copies):
        copies[1].wait_recv()
        return hand(2, device(over(1), y, x, core), 6)

    def hand_tests(copies):
        own_copies[1].wait()
        copies[0].wait_recv()
        return [hand(g, mate, 2 * g + 1) for g in range(3)]

    def hand_relayed(copy):
        copy.wait_recv()
        return [hand(3, mate, 7)]

    def arrived(copies):
        for copy in copies:
            copy.wait_recv()

    gt, tmp = r["gt"], r["tmp"]
    part_c, out_c1, in_c1, out_c2, in_c2 = (
        r["part_c"], r["out_c1"], r["in_c1"], r["out_c2"], r["in_c2"]
    )
    out_c3, in_c3, out_c4, in_c4 = r["out_c3"], r["in_c3"], r["out_c4"], r["in_c4"]
    part_a, part_b, out_a1, out_b1 = r["part_a"], r["part_b"], r["out_a1"], r["out_b1"]

    def compute(g, first=0, last=4):
        def strip(i, carry):
            oy, ox = (3 - i) // 2, (3 - i) % 2
            own = (over(g) * 2 + (y + oy) % 2) * 2 + (x + ox) % 2
            gt[...] = gbuf[:, lanes(own, W)].T
            for e in range(each):
                col = (own + core * each + e) % chips
                tmp[e * W : (e + 1) * W] = jnp.dot(
                    gt[...], gbuf[:, lanes(col, W)], preferred_element_type=F32
                )
            col = 2 * ((own + half) % chips) + (core + own // half) % 2
            extra = jnp.dot(
                gt[pl.ds(pl.multiple_of(core * w, w), w), :], gbuf[:, lanes(col, w)],
                preferred_element_type=F32,
            )

            @pl.when(core == 0)
            def _():
                tmp[w:W, :w] = extra
                tmp[mid : mid + hs] = tmp[each * W - hs : each * W]

            @pl.when(core == 1)
            def _():
                tmp[each * W :, :w] = extra[: w // 2]
                tmp[each * W :, w:] = extra[w // 2 :]


            @pl.when(ox == 0)
            def _():
                part_a[g, oy] = tmp[:ra]

            @pl.when(ox == 1)
            def _():
                out_a1[g, oy] = tmp[:ra].astype(BF16)

            @pl.when(oy == 0)
            def _():
                part_b[g, ox] = tmp[ra : ra + rb]

            @pl.when(oy == 1)
            def _():
                out_b1[g, ox] = tmp[ra : ra + rb].astype(BF16)

            for h in range(2):
                ends = tmp[ra + rb + h * hc : ra + rb + (h + 1) * hc]
                if g % 2:
                    out_c1[g // 2, h, 3 - i] = ends.astype(BF16)
                else:
                    part_c[g // 2, h, 3 - i] = ends
            return carry

        lax.fori_loop(first, last, strip, 0)

    a1, b1, a2, b2, az, bz = {}, {}, {}, {}, {}, {}

    def first(g, o):
        a1[g, o] = to(out_a1.at[g, o], r["in_a1"].at[g, o], x_to, sent="a1")
        b1[g, o] = to(out_b1.at[g, o], r["in_b1"].at[g, o], y_to, sent="b1")

    def second(g):
        a1[g, 1].wait_recv()
        r["out_a2"][g] = (part_a[g, 1] + r["in_a1"][g, 1].astype(F32)).astype(BF16)
        a2[g] = to(r["out_a2"].at[g], r["in_a2"].at[g], y_to, sent="a2")
        b1[g, 1].wait_recv()
        r["out_b2"][g] = (part_b[g, 1] + r["in_b1"][g, 1].astype(F32)).astype(BF16)
        b2[g] = to(r["out_b2"].at[g], r["in_b2"].at[g], x_to, sent="b2")

    def third(g):
        a1[g, 0].wait_recv()
        a2[g].wait_recv()
        total_a = part_a[g, 0] + r["in_a1"][g, 0].astype(F32) + r["in_a2"][g].astype(F32)
        b1[g, 0].wait_recv()
        b2[g].wait_recv()
        total_b = part_b[g, 0] + r["in_b1"][g, 0].astype(F32) + r["in_b2"][g].astype(F32)
        if g == 0:
            part_a[0, 0] = total_a
            part_b[0, 0] = total_b
            return
        if g == 2:
            az[3].wait_recv()
            total_a = total_a + r["in_az"][2].astype(F32)
            bz[3].wait_recv()
            total_b = total_b + r["in_bz"][2].astype(F32)
        target = device(over(2 if g == 2 else 1), y, x, core)
        at = {3: 2, 2: 1, 1: 0}[g]
        r["out_az"][at] = total_a.astype(BF16)
        az[g] = to(r["out_az"].at[at], r["in_az"].at[at], target, sent="az")
        r["out_bz"][at] = total_b.astype(BF16)
        bz[g] = to(r["out_bz"].at[at], r["in_bz"].at[at], target, sent="bz")

    c1, c2, c3, c4 = {}, [], {}, {}
    few = pl.ds(0, hs)

    def c_first():
        for at in (1, 0):
            c1[at] = Either(
                out_c1.at[at], in_c1.at[at], (slice(None), slice(None), few),
                device(over(1), y, x, core),
            )

    def c_second():
        c1[1].wait_recv()
        out_c2[...] = (part_c[1] + in_c1[1].astype(F32)).astype(BF16)
        c2.append(
            Either(out_c2, in_c2, (slice(None), slice(None), few), device(over(2), y, x, core))
        )

    def c_third():
        c1[0].wait_recv()
        c2[0].wait_recv()
        part_c[0] = part_c[0] + in_c1[0].astype(F32) + in_c2[...].astype(F32)
        for o in range(2):
            out_c3[0, o] = part_c[0, 0, 2 * o + 1].astype(BF16)
            out_c3[1, o] = part_c[0, 1, 2 + o].astype(BF16)
        for h, target in ((0, x_to), (1, y_to)):
            c3[h] = Either(out_c3.at[h], in_c3.at[h], (slice(None), few), target)

    def c_fourth():
        for h, target in ((0, y_to), (1, x_to)):
            c3[h].wait_recv()
            out_c4[h] = (part_c[0, h, 2 - h] + in_c3[h, 1].astype(F32)).astype(BF16)
            c4[h] = Either(out_c4.at[h], in_c4.at[h], (few,), target)

    pp, in_p1, out_p2, in_p2, pfull = r["pp"], r["in_p1"], r["out_p2"], r["in_p2"], r["pfull"]
    sub = lambda oy, ox: (y + oy) % 2 * 2 + (x + ox) % 2
    p1, p2 = {}, {}

    def precondition(handed):
        own_copies[2].wait()
        bytes_of(fbuf.at[pl.ds(0, (2 * far - 1) * w)], came="f").wait_recv()
        for copy in handed:
            copy.wait_recv()
        pp[...] = jnp.dot(tbuf[...], fbuf[...], preferred_element_type=F32)
        for o in (1, 0):
            p1[0, o] = to(pp.at[pl.ds(0, mh), lanes(sub(o, 1), w)], in_p1.at[0, o], x_to)
            p1[1, o] = to(pp.at[pl.ds(mh, mh), lanes(sub(1, o), w)], in_p1.at[1, o], y_to)

    def precondition_second():
        p1[0, 1].wait_recv()
        out_p2[0] = pp[:mh, lanes(sub(1, 0), w)] + in_p1[0, 1]
        p2[0] = to(out_p2.at[0], in_p2.at[0], y_to)
        p1[1, 1].wait_recv()
        out_p2[1] = pp[mh:, lanes(sub(0, 1), w)] + in_p1[1, 1]
        p2[1] = to(out_p2.at[1], in_p2.at[1], x_to)

    def place(oy, ox, part=0, parts=1):
        return lanes((core * 4 + sub(oy, ox)) * parts + part, far * w // parts)

    def pass_on(where, target):
        return to(pfull.at[:, where], pfull.at[:, where], target)

    def gather_first():
        p1[0, 0].wait_recv()
        p2[0].wait_recv()
        own = lanes((core * 4 + sub(0, 0)) * far + z, w)
        pfull[:mh, own] = (pp[:mh, lanes(sub(0, 0), w)] + in_p1[0, 0] + in_p2[0]).astype(BF16)
        p1[1, 0].wait_recv()
        p2[1].wait_recv()
        pfull[mh:, own] = (pp[mh:, lanes(sub(0, 0), w)] + in_p1[1, 0] + in_p2[1]).astype(BF16)
        return [pass_on(own, device(over(g), y, x, core)) for g in (1, 2)]

    def gather_relay(along_z):
        along_z[1].wait_recv()
        there = lanes((core * 4 + sub(0, 0)) * far + over(2), w)
        return pass_on(there, device(over(1), y, x, core))

    def gather_second(along_z, relayed):
        along_z[0].wait_recv()
        relayed.wait_recv()
        gx = [pass_on(place(0, 0, i, 2), x_to) for i in range(2)]
        gy = [pass_on(place(0, 0, i, 2), y_to) for i in (1, 0)]
        return gx, gy, pass_on(place(0, 0), mate)

    def gather_third(gx, gy):
        gx[0].wait_recv()
        diagonal = [pass_on(place(0, 1, 0, 2), y_to)]
        gy[0].wait_recv()
        return diagonal + [pass_on(place(1, 0, 1, 2), x_to)]

    def gather_mates(gx, gy):
        gx[1].wait_recv()
        mates = [pass_on(place(0, 1), mate)]
        gy[1].wait_recv()
        return mates + [pass_on(place(1, 0), mate)]

    def gather_fourth(diagonal):
        for copy in diagonal:
            copy.wait_recv()
        return pass_on(place(1, 1), mate)

    def score(other, first, last):
        def chunk(i, carry):
            cc, at = (core + other) % 2, sub(i // 2, i % 2)
            left = jnp.concatenate(
                [gbuf[:rows, lanes((cc * far + zz) * 4 + at, w)] for zz in range(far)], axis=1
            )
            scores_ref[...] += lax.dot_general(
                left, pfull[:, lanes(cc * 4 + at, far * w)], (((1,), (1,)), ((), ())),
                preferred_element_type=F32,
            )
            return carry

        lax.fori_loop(first, last, chunk, 0)

    def scores_start():
        scores_ref[...] = jnp.zeros_like(scores_ref)

    msend, mrecv, msem, mrsem = r["msend"], r["mrecv"], r["msem"], r["mrsem"]
    dsend, drecv, xsend, xrecv = r["dsend"], r["drecv"], r["xsend"], r["xrecv"]

    def mirror_copy(e, side):
        d = core * each + e
        return pltpu.make_async_remote_copy(
            src_ref=msend.at[e, pl.ds(side * w, w)], dst_ref=mrecv.at[d],
            send_sem=msem.at[2 * e + side], recv_sem=mrsem.at[d],
            device_id={"dp": 2 * ((q + d) % chips) + side}, device_id_type=MESH,
        )

    def when_sent(e, act):
        if e:
            act()
        else:
            pl.when(core == 1)(act)

    def finish(part):
        if part < 2:
            sums, came, copies, size = (
                (part_a, r["in_az"], az, ra), (part_b, r["in_bz"], bz, rb)
            )[part]
            at = part * ra
            for g in (1, 2):
                copies[g].wait_recv()
            tmp[at : at + size] = sums[0, 0] + came[0].astype(F32) + came[1].astype(F32)
        else:
            at, size = ra + rb, s.rc
            for h in range(2):
                c4[h].wait_recv()
                tmp[at + h * hc : at + (h + 1) * hc] = (
                    part_c[0, h, 0] + in_c3[h, 0].astype(F32) + in_c4[h].astype(F32)
                )
            extra = r["extra"]

            @pl.when(core == 0)
            def _():
                tmp[each * W - hs : each * W] = tmp[mid : mid + hs]
                extra[...] = tmp[w:W, :w]

            @pl.when(core == 1)
            def _():
                extra[: w // 2] = tmp[each * W :, :w]
                extra[w // 2 :] = tmp[each * W :, w:]

        for e in range(each):
            if not at < (e + 1) * W <= at + size:
                continue
            msend[e] = tmp[e * W : (e + 1) * W].T.astype(BF16)

            def send(e=e):
                for side in range(2):
                    mirror_copy(e, side).start()

            when_sent(e, send)
            where = lanes((q + core * each + e) % chips, W)
            term_ref[:, where] = tmp[pl.ds(pl.multiple_of(e * W + core * w, w), w), :]
            other = pl.ds(pl.multiple_of(e * W + (1 - core) * w, w), w)
            dsend[:, e * W : (e + 1) * W] = tmp[other, :].astype(BF16)
            if e == 0:

                @pl.when(core == 0)
                def _():
                    dsend[:, :w] = tmp[:w, w:W].T.astype(BF16)

        if part < 2:
            return None
        direct = to(dsend, drecv, mate)
        col = 2 * ((q + half) % chips) + (core + q // half) % 2
        term_ref[:, lanes(col, w)] = extra[...]
        xsend[...] = extra[...].T.astype(BF16)
        mirrored = to(xsend, xrecv, col)
        return direct, mirrored

    def close(direct, mirrored):
        direct.wait_recv()
        for e in range(each):
            where = lanes((q + (1 - core) * each + e) % chips, W)
            term_ref[:, where] = drecv[:, e * W : (e + 1) * W].astype(F32)
        for d in range(1, half):
            pltpu.make_async_remote_copy(
                src_ref=mrecv.at[d], dst_ref=mrecv.at[d], send_sem=msem.at[0], recv_sem=mrsem.at[d],
                device_id={"dp": mate}, device_id_type=MESH,
            ).wait_recv()
            term_ref[:, lanes((q + chips - d) % chips, W)] = mrecv[d].astype(F32)
        mirrored.wait_recv()
        far_chip = (q + half) % chips
        col = 2 * far_chip + (core + far_chip // half) % 2
        term_ref[:, lanes(col, w)] = xrecv[...].astype(F32)

    def wait_sends():
        assert count == [s.sends, s.receipts]
        for copy in started:
            copy.wait_send()
        for name in ("a1", "b1", "a2", "b2", "az", "bz"):
            bytes_of(r["out_" + name], sent=name).wait_send()
        bytes_of(g_hbm, sent="g").wait_send()
        bytes_of(fbuf.at[pl.ds(0, (2 * far - 1) * w)], sent="f").wait_send()
        for e in range(each):

            def sent(e=e):
                for side in range(2):
                    mirror_copy(e, side).wait_send()

            when_sent(e, sent)

    meet_plane()
    swap_grads()
    t_copies += swap_tests()
    pl.when(z >= far // 2)(meet_line)
    own_copies[0].wait()
    bytes_of(gbuf.at[pl.ds(rows, rows), pl.ds(0, soon * W)], came="g0").wait_recv()
    compute(3, 0, 1)
    first(3, 1)
    pl.when(z < far // 2)(meet_line)
    swap_factor(0, 3)
    bytes_of(gbuf.at[pl.ds(rows, rows), pl.ds(soon * W, s.k - soon * W)], came="g1").wait_recv()
    compute(3, 1, 3)
    first(3, 0)
    compute(3, 3, 4)
    compute(2)
    first(2, 1)
    second(3)
    first(2, 0)
    relayed = relay_tests(t_copies)
    swap_factor(2, 1)
    early = hand_tests(t_copies)
    compute(1)
    early += hand_relayed(relayed)
    first(1, 1)
    c_first()
    third(3)
    precondition(early)
    precondition_second()
    second(2)
    first(1, 0)
    compute(0)
    c_second()
    first(0, 1)
    along_z = gather_first()
    second(1)
    relayed = gather_relay(along_z)
    third(2)
    c_third()
    first(0, 0)
    second(0)
    third(1)
    gx, gy, mate_own = gather_second(along_z, relayed)
    c_fourth()
    scores_start()
    score(0, 0, 1)
    third(0)
    diagonal = gather_third(gx, gy)
    finish(0)
    finish(1)
    direct, mirrored = finish(2)
    mates = gather_mates(gx, gy)
    score(0, 1, 3)
    arrived([mate_own] + mates)
    score(1, 0, 3)
    mate_diagonal = gather_fourth(diagonal)
    score(0, 3, 4)
    arrived([mate_diagonal])
    score(1, 3, 4)
    close(direct, mirrored)
    wait_sends()

def window(grads, covariance, test_grads, inverse_factor):
    n = lax.axis_size("dp")
    rows, k = grads.shape
    s = Sizes(n, rows, k, test_grads.shape[0])
    scratch = s.scratch()
    term, scores = pl.pallas_call(
        functools.partial(kernel, s, list(scratch)),
        out_shape=(
            jax.ShapeDtypeStruct((s.w, k), F32),
            jax.ShapeDtypeStruct((rows, s.tests), F32),
        ),
        in_specs=[pl.BlockSpec(memory_space=pltpu.HBM)] * 3,
        out_specs=(
            pl.BlockSpec(memory_space=pltpu.VMEM),
            pl.BlockSpec(memory_space=pltpu.VMEM),
        ),
        scratch_shapes=list(scratch.values()),
        compiler_params=pltpu.CompilerParams(
            collective_id=0, has_side_effects=True, vmem_limit_bytes=49 * 1024 * 1024
        ),
    )(*(pltpu.with_memory_space_constraint(a, pltpu.HBM) for a in (grads, test_grads, inverse_factor)))
    return scores, 0.9 * covariance + term / (rows * n)


def solution(mesh):
    placed = (P("dp", "feat"), P("dp", "feat"), P("feat", "dp"), P("dp", None))
    whole = mesh.shape["feat"] == 1 and mesh.shape["dp"] == 32
    return jax.shard_map(
        window if whole else general,
        mesh=mesh,
        in_specs=placed,
        out_specs=(P("dp", "feat"), P("dp", "feat")),
        check_vma=False,
    )
```

```python
import functools

import jax
import jax.numpy as jnp
from jax import lax
from jax.experimental import pallas as pl
from jax.experimental.pallas import tpu as pltpu
from jax.sharding import PartitionSpec as P

F32 = jnp.float32
BF16 = jnp.bfloat16
MESH = pl.DeviceIdType.MESH


def general(grads, covariance, test_grads, inverse_factor):
    all_features = lax.all_gather(grads, "feat", axis=1, tiled=True)
    examples = grads.shape[0] * lax.axis_size("dp")
    tested = lax.dot_general(
        inverse_factor, test_grads, (((0,), (1,)), ((), ())), preferred_element_type=F32
    )
    term = lax.dot_general(
        all_features, grads, (((0,), (0,)), ((), ())), preferred_element_type=F32
    )
    joined = lax.psum_scatter(
        jnp.concatenate([term, tested], axis=1), "dp", scatter_dimension=0, tiled=True
    )
    width = grads.shape[1]
    owned_pre = joined[:, width:].astype(BF16)
    pre_columns = lax.all_gather(owned_pre, "dp", axis=0, tiled=True)
    scores = jnp.dot(all_features, pre_columns, preferred_element_type=F32)
    return scores, 0.9 * covariance + joined[:, :width] / examples


class Sizes:
    def __init__(self, n, rows, k, tests):
        self.n, self.rows, self.k, self.tests = n, rows, k, tests
        self.chips, self.far, self.w = n // 2, n // 8, k // n
        self.W = 2 * self.w
        self.half = self.chips // 2
        self.each = self.half // 2
        self.strip = self.each * self.W + self.w // 2
        self.rc = self.w
        self.hc = self.rc // 2
        self.hs = self.hc - self.w // 4
        self.ra = (self.strip - self.rc) // 2
        self.rb = self.ra
        self.mh = tests // 2

    def scratch(self):
        far, w, W, tests = self.far, self.w, self.W, self.tests
        far1 = max(far - 1, 1)
        v = pltpu.VMEM
        return dict(
            gbuf=v((2 * self.rows, self.k), BF16),
            gt=v((W, 2 * self.rows), BF16),
            tmp=v((self.strip, W), F32),
            part_a=v((far, 2, self.ra, W), F32),
            part_b=v((far, 2, self.rb, W), F32),
            out_a1=v((far, 2, self.ra, W), BF16),
            out_b1=v((far, 2, self.rb, W), BF16),
            in_a1=v((far, 2, self.ra, W), BF16),
            in_b1=v((far, 2, self.rb, W), BF16),
            out_a2=v((far, self.ra, W), BF16),
            out_b2=v((far, self.rb, W), BF16),
            in_a2=v((far, self.ra, W), BF16),
            in_b2=v((far, self.rb, W), BF16),
            out_az=v((far1, self.ra, W), BF16),
            out_bz=v((far1, self.rb, W), BF16),
            in_az=v((far1, self.ra, W), BF16),
            in_bz=v((far1, self.rb, W), BF16),
            part_c=v((2, 2, 4, self.hc, W), F32),
            out_c1=v((2, 2, 4, self.hc, W), BF16),
            in_c1=v((2, 2, 4, self.hc, W), BF16),
            out_c2=v((2, 4, self.hc, W), BF16),
            in_c2=v((2, 4, self.hc, W), BF16),
            out_c3=v((2, 2, self.hc, W), BF16),
            in_c3=v((2, 2, self.hc, W), BF16),
            out_c4=v((2, self.hc, W), BF16),
            in_c4=v((2, self.hc, W), BF16),
            extra=v((w, w), F32),
            fbuf=v((2 * far * w, 4 * w), BF16),
            tbuf=v((tests, 2 * far * w), BF16),
            pp=v((tests, 4 * w), F32),
            in_p1=v((2, 2, self.mh, w), F32),
            out_p2=v((2, self.mh, w), F32),
            in_p2=v((2, self.mh, w), F32),
            pfull=v((tests, self.k), BF16),
            msend=v((self.each, W, W), BF16),
            mrecv=v((self.half, w, W), BF16),
            xsend=v((w, w), BF16),
            xrecv=v((w, w), BF16),
            dsend=v((w, self.each * W), BF16),
            drecv=v((w, self.each * W), BF16),
            ssem=pltpu.SemaphoreType.DMA((self.sends,)),
            rsem=pltpu.SemaphoreType.DMA((self.receipts,)),
            msem=pltpu.SemaphoreType.DMA((2 * self.each,)),
            mrsem=pltpu.SemaphoreType.DMA((self.half,)),
            lsem=pltpu.SemaphoreType.DMA((4,)),
        )

    sends, receipts = 43, 68


def kernel(s, names, g_hbm, t_hbm, f_hbm, term_ref, scores_ref, *refs):
    r = dict(zip(names, refs))
    n, far, w, W, chips, half, each = s.n, s.far, s.w, s.W, s.chips, s.half, s.each
    rows, mh, ra, rb, hc, hs = s.rows, s.mh, s.ra, s.rb, s.hc, s.hs
    mid = ra + rb + hc
    me = lax.axis_index("dp")
    core, x, y, z = me % 2, me // 2 % 2, me // 4 % 2, me // 8
    q = me // 2

    def device(zz, yy, xx, cc):
        return ((zz * 2 + yy) * 2 + xx) * 2 + cc

    def over(g):
        return (z, z + 1 - 2 * (z % 2), (z + 2) % far, far - 1 - z)[g]

    mate = device(z, y, x, 1 - core)
    x_to = device(z, y, 1 - x, core)
    y_to = device(z, 1 - y, x, core)
    ssem, rsem = r["ssem"], r["rsem"]
    started = []
    count = [0, 0]
    shared = [{}, {}]

    def slot(kind, name):
        if name in shared[kind]:
            return shared[kind][name]
        i = count[kind]
        count[kind] += 1
        if name:
            shared[kind][name] = i
        return i

    def to(src, dst, target, start=True, sent=None, came=None):
        copy = pltpu.make_async_remote_copy(
            src_ref=src, dst_ref=dst, send_sem=ssem.at[slot(0, sent)],
            recv_sem=rsem.at[slot(1, came)], device_id={"dp": target}, device_id_type=MESH,
        )
        if start:
            copy.start()
        if not sent:
            started.append(copy)
        return copy

    def bytes_of(ref, sent=None, came=None):
        return pltpu.make_async_remote_copy(
            src_ref=ref, dst_ref=ref, send_sem=ssem.at[shared[0][sent] if sent else 0],
            recv_sem=rsem.at[shared[1][came] if came else 0],
            device_id={"dp": mate}, device_id_type=MESH,
        )

    class Either:
        def __init__(self, src, dst, small, target):
            i, j = slot(0, None), slot(1, None)
            self.copies = [
                pltpu.make_async_remote_copy(
                    src_ref=a, dst_ref=b, send_sem=ssem.at[i], recv_sem=rsem.at[j],
                    device_id={"dp": target}, device_id_type=MESH,
                )
                for a, b in ((src.at[small], dst.at[small]), (src, dst))
            ]
            started.append(self)
            self.each(lambda copy: copy.start())

        def each(self, act):
            for i in range(2):
                pl.when(core == i)(functools.partial(act, self.copies[i]))

        def wait_recv(self):
            self.each(lambda copy: copy.wait_recv())

        def wait_send(self):
            self.each(lambda copy: copy.wait_send())

    def lanes(block, width):
        return pl.ds(pl.multiple_of(block * width, width), width)

    gbuf, fbuf, tbuf = r["gbuf"], r["fbuf"], r["tbuf"]
    own_copies = [
        pltpu.make_async_copy(g_hbm, gbuf.at[pl.ds(0, rows)], r["lsem"].at[0]),
        pltpu.make_async_copy(t_hbm, tbuf.at[:, pl.ds(0, w)], r["lsem"].at[1]),
        pltpu.make_async_copy(
            f_hbm.at[:, lanes(core * far + z, 4 * w)], fbuf.at[pl.ds(0, w)], r["lsem"].at[2]
        ),
    ]

    barrier = pltpu.get_barrier_semaphore()

    def greet(targets):
        for target in targets:
            pl.semaphore_signal(barrier, inc=1, device_id={"dp": target}, device_id_type=MESH)

    def meet_plane():
        greet([mate, x_to, y_to])
        for copy in own_copies:
            copy.start()
        pl.semaphore_wait(barrier, 3 + z)
        greet([device(over(g), y, x, core) for g in range(1, far)])

    t_copies = []

    def meet_line():
        @pl.when(z < far - 1)
        def _():
            pl.semaphore_wait(barrier, far - 1 - z)

        for copy in t_copies:
            copy.start()

    soon = half // 2 + 2

    def swap_grads():
        there = 1 - core
        begin = (over(3) * 2 + 1 - y) * 2 + 1 - x
        last = half // 2
        steps = [0] + [i + last * there for i in range(1, last)]
        steps += [half - last * there, last + last * there]
        steps += [i - last * there for i in range(last + 1, half)] + list(range(half + 1, chips))
        parts = [lanes((begin + i) % chips, W) for i in steps]
        for i, part in enumerate(parts):
            to(
                g_hbm.at[:, part], gbuf.at[pl.ds(rows, rows), part], mate,
                sent="g", came="g0" if i < soon else "g1",
            )

    def hand(g, target, came):
        return to(tbuf.at[:, pl.ds(2 * g * w, w)], tbuf.at[:, pl.ds(came * w, w)], target)

    def swap_tests():
        return [
            to(t_hbm, tbuf.at[:, pl.ds(2 * g * w, w)], device(over(g), y, x, core), False)
            for g in (1, 2)
        ]

    def swap_factor(*groups):
        return [
            to(
                f_hbm.at[:, lanes((core + h) % 2 * far + over(g), 4 * w)],
                fbuf.at[pl.ds((2 * g + h) * w, w)],
                device(over(g), y, x, (core + h) % 2),
                sent="f", came="f",
            )
            for g in groups
            for h in range(2)
            if g or h
        ]

    def relay_tests(copies):
        copies[1].wait_recv()
        return hand(2, device(over(1), y, x, core), 6)

    def hand_tests(copies):
        own_copies[1].wait()
        copies[0].wait_recv()
        return [hand(g, mate, 2 * g + 1) for g in range(3)]

    def hand_relayed(copy):
        copy.wait_recv()
        return [hand(3, mate, 7)]

    def arrived(copies):
        for copy in copies:
            copy.wait_recv()

    gt, tmp = r["gt"], r["tmp"]
    part_c, out_c1, in_c1, out_c2, in_c2 = (
        r["part_c"], r["out_c1"], r["in_c1"], r["out_c2"], r["in_c2"]
    )
    out_c3, in_c3, out_c4, in_c4 = r["out_c3"], r["in_c3"], r["out_c4"], r["in_c4"]
    part_a, part_b, out_a1, out_b1 = r["part_a"], r["part_b"], r["out_a1"], r["out_b1"]

    def compute(g, first=0, last=4):
        def strip(i, carry):
            oy, ox = (3 - i) // 2, (3 - i) % 2
            own = (over(g) * 2 + (y + oy) % 2) * 2 + (x + ox) % 2
            gt[...] = gbuf[:, lanes(own, W)].T
            for e in range(each):
                col = (own + core * each + e) % chips
                tmp[e * W : (e + 1) * W] = jnp.dot(
                    gt[...], gbuf[:, lanes(col, W)], preferred_element_type=F32
                )
            col = 2 * ((own + half) % chips) + (core + own // half) % 2
            extra = jnp.dot(
                gt[pl.ds(pl.multiple_of(core * w, w), w), :], gbuf[:, lanes(col, w)],
                preferred_element_type=F32,
            )

            @pl.when(core == 0)
            def _():
                tmp[w:W, :w] = extra
                tmp[mid : mid + hs] = tmp[each * W - hs : each * W]

            @pl.when(core == 1)
            def _():
                tmp[each * W :, :w] = extra[: w // 2]
                tmp[each * W :, w:] = extra[w // 2 :]


            @pl.when(ox == 0)
            def _():
                part_a[g, oy] = tmp[:ra]

            @pl.when(ox == 1)
            def _():
                out_a1[g, oy] = tmp[:ra].astype(BF16)

            @pl.when(oy == 0)
            def _():
                part_b[g, ox] = tmp[ra : ra + rb]

            @pl.when(oy == 1)
            def _():
                out_b1[g, ox] = tmp[ra : ra + rb].astype(BF16)

            for h in range(2):
                ends = tmp[ra + rb + h * hc : ra + rb + (h + 1) * hc]
                if g % 2:
                    out_c1[g // 2, h, 3 - i] = ends.astype(BF16)
                else:
                    part_c[g // 2, h, 3 - i] = ends
            return carry

        lax.fori_loop(first, last, strip, 0)

    a1, b1, a2, b2, az, bz = {}, {}, {}, {}, {}, {}

    def first(g, o):
        a1[g, o] = to(out_a1.at[g, o], r["in_a1"].at[g, o], x_to, sent="a1")
        b1[g, o] = to(out_b1.at[g, o], r["in_b1"].at[g, o], y_to, sent="b1")

    def second(g):
        a1[g, 1].wait_recv()
        r["out_a2"][g] = (part_a[g, 1] + r["in_a1"][g, 1].astype(F32)).astype(BF16)
        a2[g] = to(r["out_a2"].at[g], r["in_a2"].at[g], y_to, sent="a2")
        b1[g, 1].wait_recv()
        r["out_b2"][g] = (part_b[g, 1] + r["in_b1"][g, 1].astype(F32)).astype(BF16)
        b2[g] = to(r["out_b2"].at[g], r["in_b2"].at[g], x_to, sent="b2")

    def third(g):
        a1[g, 0].wait_recv()
        a2[g].wait_recv()
        total_a = part_a[g, 0] + r["in_a1"][g, 0].astype(F32) + r["in_a2"][g].astype(F32)
        b1[g, 0].wait_recv()
        b2[g].wait_recv()
        total_b = part_b[g, 0] + r["in_b1"][g, 0].astype(F32) + r["in_b2"][g].astype(F32)
        if g == 0:
            part_a[0, 0] = total_a
            part_b[0, 0] = total_b
            return
        if g == 2:
            az[3].wait_recv()
            total_a = total_a + r["in_az"][2].astype(F32)
            bz[3].wait_recv()
            total_b = total_b + r["in_bz"][2].astype(F32)
        target = device(over(2 if g == 2 else 1), y, x, core)
        at = {3: 2, 2: 1, 1: 0}[g]
        r["out_az"][at] = total_a.astype(BF16)
        az[g] = to(r["out_az"].at[at], r["in_az"].at[at], target, sent="az")
        r["out_bz"][at] = total_b.astype(BF16)
        bz[g] = to(r["out_bz"].at[at], r["in_bz"].at[at], target, sent="bz")

    c1, c2, c3, c4 = {}, [], {}, {}
    few = pl.ds(0, hs)

    def c_first():
        for at in (1, 0):
            c1[at] = Either(
                out_c1.at[at], in_c1.at[at], (slice(None), slice(None), few),
                device(over(1), y, x, core),
            )

    def c_second():
        c1[1].wait_recv()
        out_c2[...] = (part_c[1] + in_c1[1].astype(F32)).astype(BF16)
        c2.append(
            Either(out_c2, in_c2, (slice(None), slice(None), few), device(over(2), y, x, core))
        )

    def c_third():
        c1[0].wait_recv()
        c2[0].wait_recv()
        part_c[0] = part_c[0] + in_c1[0].astype(F32) + in_c2[...].astype(F32)
        for o in range(2):
            out_c3[0, o] = part_c[0, 0, 2 * o + 1].astype(BF16)
            out_c3[1, o] = part_c[0, 1, 2 + o].astype(BF16)
        for h, target in ((0, x_to), (1, y_to)):
            c3[h] = Either(out_c3.at[h], in_c3.at[h], (slice(None), few), target)

    def c_fourth():
        for h, target in ((0, y_to), (1, x_to)):
            c3[h].wait_recv()
            out_c4[h] = (part_c[0, h, 2 - h] + in_c3[h, 1].astype(F32)).astype(BF16)
            c4[h] = Either(out_c4.at[h], in_c4.at[h], (few,), target)

    pp, in_p1, out_p2, in_p2, pfull = r["pp"], r["in_p1"], r["out_p2"], r["in_p2"], r["pfull"]
    sub = lambda oy, ox: (y + oy) % 2 * 2 + (x + ox) % 2
    p1, p2 = {}, {}

    def precondition(handed):
        own_copies[2].wait()
        bytes_of(fbuf.at[pl.ds(0, (2 * far - 1) * w)], came="f").wait_recv()
        for copy in handed:
            copy.wait_recv()
        pp[...] = jnp.dot(tbuf[...], fbuf[...], preferred_element_type=F32)
        for o in (1, 0):
            p1[0, o] = to(pp.at[pl.ds(0, mh), lanes(sub(o, 1), w)], in_p1.at[0, o], x_to)
            p1[1, o] = to(pp.at[pl.ds(mh, mh), lanes(sub(1, o), w)], in_p1.at[1, o], y_to)

    def precondition_second():
        p1[0, 1].wait_recv()
        out_p2[0] = pp[:mh, lanes(sub(1, 0), w)] + in_p1[0, 1]
        p2[0] = to(out_p2.at[0], in_p2.at[0], y_to)
        p1[1, 1].wait_recv()
        out_p2[1] = pp[mh:, lanes(sub(0, 1), w)] + in_p1[1, 1]
        p2[1] = to(out_p2.at[1], in_p2.at[1], x_to)

    def place(oy, ox, part=0, parts=1):
        return lanes((core * 4 + sub(oy, ox)) * parts + part, far * w // parts)

    def pass_on(where, target):
        return to(pfull.at[:, where], pfull.at[:, where], target)

    def gather_first():
        p1[0, 0].wait_recv()
        p2[0].wait_recv()
        own = lanes((core * 4 + sub(0, 0)) * far + z, w)
        pfull[:mh, own] = (pp[:mh, lanes(sub(0, 0), w)] + in_p1[0, 0] + in_p2[0]).astype(BF16)
        p1[1, 0].wait_recv()
        p2[1].wait_recv()
        pfull[mh:, own] = (pp[mh:, lanes(sub(0, 0), w)] + in_p1[1, 0] + in_p2[1]).astype(BF16)
        return [pass_on(own, device(over(g), y, x, core)) for g in (1, 2)]

    def gather_relay(along_z):
        along_z[1].wait_recv()
        there = lanes((core * 4 + sub(0, 0)) * far + over(2), w)
        return pass_on(there, device(over(1), y, x, core))

    def gather_second(along_z, relayed):
        along_z[0].wait_recv()
        relayed.wait_recv()
        gx = [pass_on(place(0, 0, i, 2), x_to) for i in range(2)]
        gy = [pass_on(place(0, 0, i, 2), y_to) for i in (1, 0)]
        return gx, gy, pass_on(place(0, 0), mate)

    def gather_third(gx, gy):
        gx[0].wait_recv()
        diagonal = [pass_on(place(0, 1, 0, 2), y_to)]
        gy[0].wait_recv()
        return diagonal + [pass_on(place(1, 0, 1, 2), x_to)]

    def gather_mates(gx, gy):
        gx[1].wait_recv()
        mates = [pass_on(place(0, 1), mate)]
        gy[1].wait_recv()
        return mates + [pass_on(place(1, 0), mate)]

    def gather_fourth(diagonal):
        for copy in diagonal:
            copy.wait_recv()
        return pass_on(place(1, 1), mate)

    def score(other, first, last):
        def chunk(i, carry):
            cc, at = (core + other) % 2, sub(i // 2, i % 2)
            left = jnp.concatenate(
                [gbuf[:rows, lanes((cc * far + zz) * 4 + at, w)] for zz in range(far)], axis=1
            )
            scores_ref[...] += lax.dot_general(
                left, pfull[:, lanes(cc * 4 + at, far * w)], (((1,), (1,)), ((), ())),
                preferred_element_type=F32,
            )
            return carry

        lax.fori_loop(first, last, chunk, 0)

    def scores_start():
        scores_ref[...] = jnp.zeros_like(scores_ref)

    msend, mrecv, msem, mrsem = r["msend"], r["mrecv"], r["msem"], r["mrsem"]
    dsend, drecv, xsend, xrecv = r["dsend"], r["drecv"], r["xsend"], r["xrecv"]

    def mirror_copy(e, side):
        d = core * each + e
        return pltpu.make_async_remote_copy(
            src_ref=msend.at[e, pl.ds(side * w, w)], dst_ref=mrecv.at[d],
            send_sem=msem.at[2 * e + side], recv_sem=mrsem.at[d],
            device_id={"dp": 2 * ((q + d) % chips) + side}, device_id_type=MESH,
        )

    def when_sent(e, act):
        if e:
            act()
        else:
            pl.when(core == 1)(act)

    def finish(part):
        if part < 2:
            sums, came, copies, size = (
                (part_a, r["in_az"], az, ra), (part_b, r["in_bz"], bz, rb)
            )[part]
            at = part * ra
            for g in (1, 2):
                copies[g].wait_recv()
            tmp[at : at + size] = sums[0, 0] + came[0].astype(F32) + came[1].astype(F32)
        else:
            at, size = ra + rb, s.rc
            for h in range(2):
                c4[h].wait_recv()
                tmp[at + h * hc : at + (h + 1) * hc] = (
                    part_c[0, h, 0] + in_c3[h, 0].astype(F32) + in_c4[h].astype(F32)
                )
            extra = r["extra"]

            @pl.when(core == 0)
            def _():
                tmp[each * W - hs : each * W] = tmp[mid : mid + hs]
                extra[...] = tmp[w:W, :w]

            @pl.when(core == 1)
            def _():
                extra[: w // 2] = tmp[each * W :, :w]
                extra[w // 2 :] = tmp[each * W :, w:]

        for e in range(each):
            if not at < (e + 1) * W <= at + size:
                continue
            msend[e] = tmp[e * W : (e + 1) * W].T.astype(BF16)

            def send(e=e):
                for side in range(2):
                    mirror_copy(e, side).start()

            when_sent(e, send)
            where = lanes((q + core * each + e) % chips, W)
            term_ref[:, where] = tmp[pl.ds(pl.multiple_of(e * W + core * w, w), w), :]
            other = pl.ds(pl.multiple_of(e * W + (1 - core) * w, w), w)
            dsend[:, e * W : (e + 1) * W] = tmp[other, :].astype(BF16)
            if e == 0:

                @pl.when(core == 0)
                def _():
                    dsend[:, :w] = tmp[:w, w:W].T.astype(BF16)

        if part < 2:
            return None
        direct = to(dsend, drecv, mate)
        col = 2 * ((q + half) % chips) + (core + q // half) % 2
        term_ref[:, lanes(col, w)] = extra[...]
        xsend[...] = extra[...].T.astype(BF16)
        mirrored = to(xsend, xrecv, col)
        return direct, mirrored

    def close(direct, mirrored):
        direct.wait_recv()
        for e in range(each):
            where = lanes((q + (1 - core) * each + e) % chips, W)
            term_ref[:, where] = drecv[:, e * W : (e + 1) * W].astype(F32)
        for d in range(1, half):
            pltpu.make_async_remote_copy(
                src_ref=mrecv.at[d], dst_ref=mrecv.at[d], send_sem=msem.at[0], recv_sem=mrsem.at[d],
                device_id={"dp": mate}, device_id_type=MESH,
            ).wait_recv()
            term_ref[:, lanes((q + chips - d) % chips, W)] = mrecv[d].astype(F32)
        mirrored.wait_recv()
        far_chip = (q + half) % chips
        col = 2 * far_chip + (core + far_chip // half) % 2
        term_ref[:, lanes(col, w)] = xrecv[...].astype(F32)

    def wait_sends():
        assert count == [s.sends, s.receipts]
        for copy in started:
            copy.wait_send()
        for name in ("a1", "b1", "a2", "b2", "az", "bz"):
            bytes_of(r["out_" + name], sent=name).wait_send()
        bytes_of(g_hbm, sent="g").wait_send()
        bytes_of(fbuf.at[pl.ds(0, (2 * far - 1) * w)], sent="f").wait_send()
        for e in range(each):

            def sent(e=e):
                for side in range(2):
                    mirror_copy(e, side).wait_send()

            when_sent(e, sent)

    meet_plane()
    swap_grads()
    t_copies += swap_tests()
    pl.when(z >= far // 2)(meet_line)
    own_copies[0].wait()
    bytes_of(gbuf.at[pl.ds(rows, rows), pl.ds(0, soon * W)], came="g0").wait_recv()
    compute(3, 0, 1)
    first(3, 1)
    pl.when(z < far // 2)(meet_line)
    swap_factor(0, 3)
    bytes_of(gbuf.at[pl.ds(rows, rows), pl.ds(soon * W, s.k - soon * W)], came="g1").wait_recv()
    compute(3, 1, 3)
    first(3, 0)
    compute(3, 3, 4)
    compute(2)
    first(2, 1)
    second(3)
    first(2, 0)
    relayed = relay_tests(t_copies)
    swap_factor(2, 1)
    early = hand_tests(t_copies)
    compute(1)
    early += hand_relayed(relayed)
    first(1, 1)
    c_first()
    third(3)
    precondition(early)
    precondition_second()
    second(2)
    first(1, 0)
    compute(0)
    c_second()
    first(0, 1)
    along_z = gather_first()
    second(1)
    first(0, 0)
    relayed = gather_relay(along_z)
    third(2)
    c_third()
    second(0)
    third(1)
    c_fourth()
    gx, gy, mate_own = gather_second(along_z, relayed)
    scores_start()
    score(0, 0, 1)
    third(0)
    diagonal = gather_third(gx, gy)
    finish(0)
    finish(1)
    direct, mirrored = finish(2)
    mates = gather_mates(gx, gy)
    score(0, 1, 3)
    arrived([mate_own] + mates)
    score(1, 0, 3)
    mate_diagonal = gather_fourth(diagonal)
    score(0, 3, 4)
    arrived([mate_diagonal])
    score(1, 3, 4)
    close(direct, mirrored)
    wait_sends()

def window(grads, covariance, test_grads, inverse_factor):
    n = lax.axis_size("dp")
    rows, k = grads.shape
    s = Sizes(n, rows, k, test_grads.shape[0])
    scratch = s.scratch()
    term, scores = pl.pallas_call(
        functools.partial(kernel, s, list(scratch)),
        out_shape=(
            jax.ShapeDtypeStruct((s.w, k), F32),
            jax.ShapeDtypeStruct((rows, s.tests), F32),
        ),
        in_specs=[pl.BlockSpec(memory_space=pltpu.HBM)] * 3,
        out_specs=(
            pl.BlockSpec(memory_space=pltpu.VMEM),
            pl.BlockSpec(memory_space=pltpu.VMEM),
        ),
        scratch_shapes=list(scratch.values()),
        compiler_params=pltpu.CompilerParams(
            collective_id=0, has_side_effects=True, vmem_limit_bytes=49 * 1024 * 1024
        ),
    )(*(pltpu.with_memory_space_constraint(a, pltpu.HBM) for a in (grads, test_grads, inverse_factor)))
    here = pl.BlockSpec(memory_space=pltpu.VMEM)
    there = pl.BlockSpec(memory_space=pl.ANY)
    return pl.pallas_call(
        functools.partial(ending, rows * n),
        out_shape=(
            jax.ShapeDtypeStruct(scores.shape, F32),
            jax.ShapeDtypeStruct(covariance.shape, F32),
        ),
        in_specs=[here, here, here],
        out_specs=(there, there),
        scratch_shapes=[
            pltpu.VMEM(covariance.shape, F32),
            pltpu.SemaphoreType.DMA((PIECES + 1,)),
        ],
        compiler_params=pltpu.CompilerParams(vmem_limit_bytes=8 * 1024 * 1024),
    )(scores, term, covariance)


PIECES = 4


def ending(examples, scores_ref, term_ref, before_ref, scores_out, after_out, after, sem):
    copies = [pltpu.make_async_copy(scores_ref, scores_out, sem.at[PIECES])]
    copies[0].start()
    piece = after.shape[0] // PIECES
    for i in range(PIECES):
        part = pl.ds(i * piece, piece)
        after[part] = 0.9 * before_ref[part] + term_ref[part] / examples
        copies.append(pltpu.make_async_copy(after.at[part], after_out.at[part], sem.at[i]))
        copies[-1].start()
    for copy in copies:
        copy.wait()


def solution(mesh):
    placed = (P("dp", "feat"), P("dp", "feat"), P("feat", "dp"), P("dp", None))
    whole = mesh.shape["feat"] == 1 and mesh.shape["dp"] == 32
    return jax.shard_map(
        window if whole else general,
        mesh=mesh,
        in_specs=placed,
        out_specs=(P("dp", "feat"), P("dp", "feat")),
        check_vma=False,
    )
```

```python
import functools

import jax
import jax.numpy as jnp
from jax import lax
from jax.experimental import pallas as pl
from jax.experimental.pallas import tpu as pltpu
from jax.sharding import PartitionSpec as P

F32 = jnp.float32
BF16 = jnp.bfloat16
MESH = pl.DeviceIdType.MESH


def general(grads, covariance, test_grads, inverse_factor):
    all_features = lax.all_gather(grads, "feat", axis=1, tiled=True)
    examples = grads.shape[0] * lax.axis_size("dp")
    tested = lax.dot_general(
        inverse_factor, test_grads, (((0,), (1,)), ((), ())), preferred_element_type=F32
    )
    term = lax.dot_general(
        all_features, grads, (((0,), (0,)), ((), ())), preferred_element_type=F32
    )
    joined = lax.psum_scatter(
        jnp.concatenate([term, tested], axis=1), "dp", scatter_dimension=0, tiled=True
    )
    width = grads.shape[1]
    owned_pre = joined[:, width:].astype(BF16)
    pre_columns = lax.all_gather(owned_pre, "dp", axis=0, tiled=True)
    scores = jnp.dot(all_features, pre_columns, preferred_element_type=F32)
    return scores, 0.9 * covariance + joined[:, :width] / examples


class Sizes:
    def __init__(self, n, rows, k, tests):
        self.n, self.rows, self.k, self.tests = n, rows, k, tests
        self.chips, self.far, self.w = n // 2, n // 8, k // n
        self.W = 2 * self.w
        self.half = self.chips // 2
        self.each = self.half // 2
        self.strip = self.each * self.W + self.w // 2
        self.rc = self.w
        self.hc = self.rc // 2
        self.hs = self.hc - self.w // 4
        self.ra = (self.strip - self.rc) // 2
        self.rb = self.ra
        self.mh = tests // 2

    def scratch(self):
        far, w, W, tests = self.far, self.w, self.W, self.tests
        far1 = max(far - 1, 1)
        v = pltpu.VMEM
        return dict(
            gbuf=v((2 * self.rows, self.k), BF16),
            gt=v((W, 2 * self.rows), BF16),
            tmp=v((self.strip, W), F32),
            part_a=v((far, 2, self.ra, W), F32),
            part_b=v((far, 2, self.rb, W), F32),
            out_a1=v((far, 2, self.ra, W), BF16),
            out_b1=v((far, 2, self.rb, W), BF16),
            in_a1=v((far, 2, self.ra, W), BF16),
            in_b1=v((far, 2, self.rb, W), BF16),
            out_a2=v((far, self.ra, W), BF16),
            out_b2=v((far, self.rb, W), BF16),
            in_a2=v((far, self.ra, W), BF16),
            in_b2=v((far, self.rb, W), BF16),
            out_az=v((far1, self.ra, W), BF16),
            out_bz=v((far1, self.rb, W), BF16),
            in_az=v((far1, self.ra, W), BF16),
            in_bz=v((far1, self.rb, W), BF16),
            part_c=v((2, 2, 4, self.hc, W), F32),
            out_c1=v((2, 2, 4, self.hc, W), BF16),
            in_c1=v((2, 2, 4, self.hc, W), BF16),
            out_c2=v((2, 4, self.hc, W), BF16),
            in_c2=v((2, 4, self.hc, W), BF16),
            out_c3=v((2, 2, self.hc, W), BF16),
            in_c3=v((2, 2, self.hc, W), BF16),
            out_c4=v((2, self.hc, W), BF16),
            in_c4=v((2, self.hc, W), BF16),
            extra=v((w, w), F32),
            fbuf=v((2 * far * w, 4 * w), BF16),
            tbuf=v((tests, 2 * far * w), BF16),
            pp=v((tests, 4 * w), F32),
            in_p1=v((2, 2, self.mh, w), F32),
            out_p2=v((2, self.mh, w), F32),
            in_p2=v((2, self.mh, w), F32),
            pfull=v((tests, self.k), BF16),
            msend=v((self.each, W, W), BF16),
            mrecv=v((self.half, w, W), BF16),
            xsend=v((w, w), BF16),
            xrecv=v((w, w), BF16),
            dsend=v((w, self.each * W), BF16),
            drecv=v((w, self.each * W), BF16),
            ssem=pltpu.SemaphoreType.DMA((self.sends,)),
            rsem=pltpu.SemaphoreType.DMA((self.receipts,)),
            msem=pltpu.SemaphoreType.DMA((2 * self.each,)),
            mrsem=pltpu.SemaphoreType.DMA((1,)),
            lsem=pltpu.SemaphoreType.DMA((4,)),
        )

    sends, receipts = 43, 68


def kernel(s, names, g_hbm, t_hbm, f_hbm, term_ref, scores_ref, *refs):
    r = dict(zip(names, refs))
    n, far, w, W, chips, half, each = s.n, s.far, s.w, s.W, s.chips, s.half, s.each
    rows, mh, ra, rb, hc, hs = s.rows, s.mh, s.ra, s.rb, s.hc, s.hs
    mid = ra + rb + hc
    me = lax.axis_index("dp")
    core, x, y, z = me % 2, me // 2 % 2, me // 4 % 2, me // 8
    q = me // 2

    def device(zz, yy, xx, cc):
        return ((zz * 2 + yy) * 2 + xx) * 2 + cc

    def over(g):
        return (z, z + 1 - 2 * (z % 2), (z + 2) % far, far - 1 - z)[g]

    mate = device(z, y, x, 1 - core)
    x_to = device(z, y, 1 - x, core)
    y_to = device(z, 1 - y, x, core)
    ssem, rsem = r["ssem"], r["rsem"]
    started = []
    count = [0, 0]
    shared = [{}, {}]

    def slot(kind, name):
        if name in shared[kind]:
            return shared[kind][name]
        i = count[kind]
        count[kind] += 1
        if name:
            shared[kind][name] = i
        return i

    def to(src, dst, target, start=True, sent=None, came=None):
        copy = pltpu.make_async_remote_copy(
            src_ref=src, dst_ref=dst, send_sem=ssem.at[slot(0, sent)],
            recv_sem=rsem.at[slot(1, came)], device_id={"dp": target}, device_id_type=MESH,
        )
        if start:
            copy.start()
        if not sent:
            started.append(copy)
        return copy

    def bytes_of(ref, sent=None, came=None):
        return pltpu.make_async_remote_copy(
            src_ref=ref, dst_ref=ref, send_sem=ssem.at[shared[0][sent] if sent else 0],
            recv_sem=rsem.at[shared[1][came] if came else 0],
            device_id={"dp": mate}, device_id_type=MESH,
        )

    class Either:
        def __init__(self, src, dst, small, target):
            i, j = slot(0, None), slot(1, None)
            self.copies = [
                pltpu.make_async_remote_copy(
                    src_ref=a, dst_ref=b, send_sem=ssem.at[i], recv_sem=rsem.at[j],
                    device_id={"dp": target}, device_id_type=MESH,
                )
                for a, b in ((src.at[small], dst.at[small]), (src, dst))
            ]
            started.append(self)
            self.each(lambda copy: copy.start())

        def each(self, act):
            for i in range(2):
                pl.when(core == i)(functools.partial(act, self.copies[i]))

        def wait_recv(self):
            self.each(lambda copy: copy.wait_recv())

        def wait_send(self):
            self.each(lambda copy: copy.wait_send())

    def lanes(block, width):
        return pl.ds(pl.multiple_of(block * width, width), width)

    gbuf, fbuf, tbuf = r["gbuf"], r["fbuf"], r["tbuf"]
    own_copies = [
        pltpu.make_async_copy(g_hbm, gbuf.at[pl.ds(0, rows)], r["lsem"].at[0]),
        pltpu.make_async_copy(t_hbm, tbuf.at[:, pl.ds(0, w)], r["lsem"].at[1]),
        pltpu.make_async_copy(
            f_hbm.at[:, lanes(core * far + z, 4 * w)], fbuf.at[pl.ds(0, w)], r["lsem"].at[2]
        ),
    ]

    barrier = pltpu.get_barrier_semaphore()

    def greet(targets):
        for target in targets:
            pl.semaphore_signal(barrier, inc=1, device_id={"dp": target}, device_id_type=MESH)

    def meet_plane():
        greet([mate, x_to, y_to])
        for copy in own_copies:
            copy.start()
        pl.semaphore_wait(barrier, 3 + z)
        greet([device(over(g), y, x, core) for g in range(1, far)])

    t_copies = []

    def meet_line():
        @pl.when(z < far - 1)
        def _():
            pl.semaphore_wait(barrier, far - 1 - z)

        for copy in t_copies:
            copy.start()

    soon = half // 2 + 2

    def swap_grads():
        there = 1 - core
        begin = (over(3) * 2 + 1 - y) * 2 + 1 - x
        last = half // 2
        steps = [0] + [i + last * there for i in range(1, last)]
        steps += [half - last * there, last + last * there]
        steps += [i - last * there for i in range(last + 1, half)] + list(range(half + 1, chips))
        parts = [lanes((begin + i) % chips, W) for i in steps]
        for i, part in enumerate(parts):
            to(
                g_hbm.at[:, part], gbuf.at[pl.ds(rows, rows), part], mate,
                sent="g", came="g0" if i < soon else "g1",
            )

    def hand(g, target, came):
        return to(tbuf.at[:, pl.ds(2 * g * w, w)], tbuf.at[:, pl.ds(came * w, w)], target)

    def swap_tests():
        return [
            to(t_hbm, tbuf.at[:, pl.ds(2 * g * w, w)], device(over(g), y, x, core), False)
            for g in (1, 2)
        ]

    def swap_factor(*groups):
        return [
            to(
                f_hbm.at[:, lanes((core + h) % 2 * far + over(g), 4 * w)],
                fbuf.at[pl.ds((2 * g + h) * w, w)],
                device(over(g), y, x, (core + h) % 2),
                sent="f", came="f",
            )
            for g in groups
            for h in range(2)
            if g or h
        ]

    def relay_tests(copies):
        copies[1].wait_recv()
        return hand(2, device(over(1), y, x, core), 6)

    def hand_tests(copies):
        own_copies[1].wait()
        copies[0].wait_recv()
        return [hand(g, mate, 2 * g + 1) for g in range(3)]

    def hand_relayed(copy):
        copy.wait_recv()
        return [hand(3, mate, 7)]

    def arrived(copies):
        for copy in copies:
            copy.wait_recv()

    gt, tmp = r["gt"], r["tmp"]
    part_c, out_c1, in_c1, out_c2, in_c2 = (
        r["part_c"], r["out_c1"], r["in_c1"], r["out_c2"], r["in_c2"]
    )
    out_c3, in_c3, out_c4, in_c4 = r["out_c3"], r["in_c3"], r["out_c4"], r["in_c4"]
    part_a, part_b, out_a1, out_b1 = r["part_a"], r["part_b"], r["out_a1"], r["out_b1"]

    def compute(g, first=0, last=4):
        def strip(i, carry):
            oy, ox = (3 - i) // 2, (3 - i) % 2
            own = (over(g) * 2 + (y + oy) % 2) * 2 + (x + ox) % 2
            gt[...] = gbuf[:, lanes(own, W)].T
            for e in range(each):
                col = (own + core * each + e) % chips
                tmp[e * W : (e + 1) * W] = jnp.dot(
                    gt[...], gbuf[:, lanes(col, W)], preferred_element_type=F32
                )
            col = 2 * ((own + half) % chips) + (core + own // half) % 2
            extra = jnp.dot(
                gt[pl.ds(pl.multiple_of(core * w, w), w), :], gbuf[:, lanes(col, w)],
                preferred_element_type=F32,
            )

            @pl.when(core == 0)
            def _():
                tmp[w:W, :w] = extra
                tmp[mid : mid + hs] = tmp[each * W - hs : each * W]

            @pl.when(core == 1)
            def _():
                tmp[each * W :, :w] = extra[: w // 2]
                tmp[each * W :, w:] = extra[w // 2 :]


            @pl.when(ox == 0)
            def _():
                part_a[g, oy] = tmp[:ra]

            @pl.when(ox == 1)
            def _():
                out_a1[g, oy] = tmp[:ra].astype(BF16)

            @pl.when(oy == 0)
            def _():
                part_b[g, ox] = tmp[ra : ra + rb]

            @pl.when(oy == 1)
            def _():
                out_b1[g, ox] = tmp[ra : ra + rb].astype(BF16)

            for h in range(2):
                ends = tmp[ra + rb + h * hc : ra + rb + (h + 1) * hc]
                if g % 2:
                    out_c1[g // 2, h, 3 - i] = ends.astype(BF16)
                else:
                    part_c[g // 2, h, 3 - i] = ends
            return carry

        lax.fori_loop(first, last, strip, 0)

    a1, b1, a2, b2, az, bz = {}, {}, {}, {}, {}, {}

    def first(g, o):
        a1[g, o] = to(out_a1.at[g, o], r["in_a1"].at[g, o], x_to, sent="a1")
        b1[g, o] = to(out_b1.at[g, o], r["in_b1"].at[g, o], y_to, sent="b1")

    def second(g):
        a1[g, 1].wait_recv()
        r["out_a2"][g] = (part_a[g, 1] + r["in_a1"][g, 1].astype(F32)).astype(BF16)
        a2[g] = to(r["out_a2"].at[g], r["in_a2"].at[g], y_to, sent="a2")
        b1[g, 1].wait_recv()
        r["out_b2"][g] = (part_b[g, 1] + r["in_b1"][g, 1].astype(F32)).astype(BF16)
        b2[g] = to(r["out_b2"].at[g], r["in_b2"].at[g], x_to, sent="b2")

    def third(g):
        target = device(over(2 if g == 2 else 1), y, x, core)
        at = {3: 2, 2: 1, 1: 0, 0: 0}[g]
        for name, part, one, two, along in (
            ("a", part_a, a1, a2, az), ("b", part_b, b1, b2, bz)
        ):
            one[g, 0].wait_recv()
            two[g].wait_recv()
            total = (
                part[g, 0] + r[f"in_{name}1"][g, 0].astype(F32) + r[f"in_{name}2"][g].astype(F32)
            )
            if g == 0:
                part[0, 0] = total
                continue
            out, came = r[f"out_{name}z"], r[f"in_{name}z"]
            if g == 2:
                along[3].wait_recv()
                total = total + came[2].astype(F32)
            out[at] = total.astype(BF16)
            along[g] = to(out.at[at], came.at[at], target, sent=name + "z")

    c1, c2, c3, c4 = {}, [], {}, {}
    few = pl.ds(0, hs)

    def c_first():
        for at in (1, 0):
            c1[at] = Either(
                out_c1.at[at], in_c1.at[at], (slice(None), slice(None), few),
                device(over(1), y, x, core),
            )

    def c_second():
        c1[1].wait_recv()
        out_c2[...] = (part_c[1] + in_c1[1].astype(F32)).astype(BF16)
        c2.append(
            Either(out_c2, in_c2, (slice(None), slice(None), few), device(over(2), y, x, core))
        )

    def c_third():
        c1[0].wait_recv()
        c2[0].wait_recv()
        part_c[0] = part_c[0] + in_c1[0].astype(F32) + in_c2[...].astype(F32)
        for o in range(2):
            out_c3[0, o] = part_c[0, 0, 2 * o + 1].astype(BF16)
            out_c3[1, o] = part_c[0, 1, 2 + o].astype(BF16)
        for h, target in ((0, x_to), (1, y_to)):
            c3[h] = Either(out_c3.at[h], in_c3.at[h], (slice(None), few), target)

    def c_fourth():
        for h, target in ((0, y_to), (1, x_to)):
            c3[h].wait_recv()
            out_c4[h] = (part_c[0, h, 2 - h] + in_c3[h, 1].astype(F32)).astype(BF16)
            c4[h] = Either(out_c4.at[h], in_c4.at[h], (few,), target)

    pp, in_p1, out_p2, in_p2, pfull = r["pp"], r["in_p1"], r["out_p2"], r["in_p2"], r["pfull"]
    sub = lambda oy, ox: (y + oy) % 2 * 2 + (x + ox) % 2
    p1, p2 = {}, {}

    def precondition(handed):
        own_copies[2].wait()
        bytes_of(fbuf.at[pl.ds(0, (2 * far - 1) * w)], came="f").wait_recv()
        for copy in handed:
            copy.wait_recv()
        pp[...] = jnp.dot(tbuf[...], fbuf[...], preferred_element_type=F32)
        for o in (1, 0):
            p1[0, o] = to(pp.at[pl.ds(0, mh), lanes(sub(o, 1), w)], in_p1.at[0, o], x_to)
            p1[1, o] = to(pp.at[pl.ds(mh, mh), lanes(sub(1, o), w)], in_p1.at[1, o], y_to)

    def precondition_second():
        p1[0, 1].wait_recv()
        out_p2[0] = pp[:mh, lanes(sub(1, 0), w)] + in_p1[0, 1]
        p2[0] = to(out_p2.at[0], in_p2.at[0], y_to)
        p1[1, 1].wait_recv()
        out_p2[1] = pp[mh:, lanes(sub(0, 1), w)] + in_p1[1, 1]
        p2[1] = to(out_p2.at[1], in_p2.at[1], x_to)

    def place(oy, ox, part=0, parts=1):
        return lanes((core * 4 + sub(oy, ox)) * parts + part, far * w // parts)

    def pass_on(where, target):
        return to(pfull.at[:, where], pfull.at[:, where], target)

    def gather_first():
        p1[0, 0].wait_recv()
        p2[0].wait_recv()
        own = lanes((core * 4 + sub(0, 0)) * far + z, w)
        pfull[:mh, own] = (pp[:mh, lanes(sub(0, 0), w)] + in_p1[0, 0] + in_p2[0]).astype(BF16)
        p1[1, 0].wait_recv()
        p2[1].wait_recv()
        pfull[mh:, own] = (pp[mh:, lanes(sub(0, 0), w)] + in_p1[1, 0] + in_p2[1]).astype(BF16)
        return [pass_on(own, device(over(g), y, x, core)) for g in (1, 2)]

    def gather_relay(along_z):
        along_z[1].wait_recv()
        there = lanes((core * 4 + sub(0, 0)) * far + over(2), w)
        return pass_on(there, device(over(1), y, x, core))

    def gather_second(along_z, relayed):
        along_z[0].wait_recv()
        relayed.wait_recv()
        gx = [pass_on(place(0, 0, i, 2), x_to) for i in range(2)]
        gy = [pass_on(place(0, 0, i, 2), y_to) for i in (1, 0)]
        return gx, gy, pass_on(place(0, 0), mate)

    def gather_third(gx, gy):
        gx[0].wait_recv()
        diagonal = [pass_on(place(0, 1, 0, 2), y_to)]
        gy[0].wait_recv()
        return diagonal + [pass_on(place(1, 0, 1, 2), x_to)]

    def gather_mates(gx, gy):
        gx[1].wait_recv()
        mates = [pass_on(place(0, 1), mate)]
        gy[1].wait_recv()
        return mates + [pass_on(place(1, 0), mate)]

    def gather_fourth(diagonal):
        for copy in diagonal:
            copy.wait_recv()
        return pass_on(place(1, 1), mate)

    def score(other, first, last):
        def chunk(i, carry):
            cc, at = (core + other) % 2, sub(i // 2, i % 2)
            left = jnp.concatenate(
                [gbuf[:rows, lanes((cc * far + zz) * 4 + at, w)] for zz in range(far)], axis=1
            )
            scores_ref[...] += lax.dot_general(
                left, pfull[:, lanes(cc * 4 + at, far * w)], (((1,), (1,)), ((), ())),
                preferred_element_type=F32,
            )
            return carry

        lax.fori_loop(first, last, chunk, 0)

    def scores_start():
        scores_ref[...] = jnp.zeros_like(scores_ref)

    msend, mrecv, msem, mrsem = r["msend"], r["mrecv"], r["msem"], r["mrsem"]
    dsend, drecv, xsend, xrecv = r["dsend"], r["drecv"], r["xsend"], r["xrecv"]

    def mirror_copy(e, side):
        d = core * each + e
        return pltpu.make_async_remote_copy(
            src_ref=msend.at[e, pl.ds(side * w, w)], dst_ref=mrecv.at[d],
            send_sem=msem.at[2 * e + side], recv_sem=mrsem.at[0],
            device_id={"dp": 2 * ((q + d) % chips) + side}, device_id_type=MESH,
        )

    def when_sent(e, act):
        if e:
            act()
        else:
            pl.when(core == 1)(act)

    def finish(part):
        if part < 2:
            sums, came, copies, size = (
                (part_a, r["in_az"], az, ra), (part_b, r["in_bz"], bz, rb)
            )[part]
            at = part * ra
            for g in (1, 2):
                copies[g].wait_recv()
            tmp[at : at + size] = sums[0, 0] + came[0].astype(F32) + came[1].astype(F32)
        else:
            at, size = ra + rb, s.rc
            for h in range(2):
                c4[h].wait_recv()
                tmp[at + h * hc : at + (h + 1) * hc] = (
                    part_c[0, h, 0] + in_c3[h, 0].astype(F32) + in_c4[h].astype(F32)
                )
            extra = r["extra"]

            @pl.when(core == 0)
            def _():
                tmp[each * W - hs : each * W] = tmp[mid : mid + hs]
                extra[...] = tmp[w:W, :w]

            @pl.when(core == 1)
            def _():
                extra[: w // 2] = tmp[each * W :, :w]
                extra[w // 2 :] = tmp[each * W :, w:]

        for e in range(each):
            if not at < (e + 1) * W <= at + size:
                continue
            msend[e] = tmp[e * W : (e + 1) * W].T.astype(BF16)

            def send(e=e):
                for side in range(2):
                    mirror_copy(e, side).start()

            when_sent(e, send)
            where = lanes((q + core * each + e) % chips, W)
            term_ref[:, where] = tmp[pl.ds(pl.multiple_of(e * W + core * w, w), w), :]
            other = pl.ds(pl.multiple_of(e * W + (1 - core) * w, w), w)
            dsend[:, e * W : (e + 1) * W] = tmp[other, :].astype(BF16)
            if e == 0:

                @pl.when(core == 0)
                def _():
                    dsend[:, :w] = tmp[:w, w:W].T.astype(BF16)

        if part < 2:
            return None
        direct = to(dsend, drecv, mate)
        col = 2 * ((q + half) % chips) + (core + q // half) % 2
        term_ref[:, lanes(col, w)] = extra[...]
        xsend[...] = extra[...].T.astype(BF16)
        mirrored = to(xsend, xrecv, col)
        return direct, mirrored

    def close(direct, mirrored):
        direct.wait_recv()
        for e in range(each):
            where = lanes((q + (1 - core) * each + e) % chips, W)
            term_ref[:, where] = drecv[:, e * W : (e + 1) * W].astype(F32)
        all_of_them = mrecv.at[pl.ds(1, half - 1)]
        pltpu.make_async_remote_copy(
            src_ref=all_of_them, dst_ref=all_of_them, send_sem=msem.at[0], recv_sem=mrsem.at[0],
            device_id={"dp": mate}, device_id_type=MESH,
        ).wait_recv()
        for d in range(1, half):
            term_ref[:, lanes((q + chips - d) % chips, W)] = mrecv[d].astype(F32)
        mirrored.wait_recv()
        far_chip = (q + half) % chips
        col = 2 * far_chip + (core + far_chip // half) % 2
        term_ref[:, lanes(col, w)] = xrecv[...].astype(F32)

    def wait_sends():
        assert count == [s.sends, s.receipts]
        for copy in started:
            copy.wait_send()
        for name in ("a1", "b1", "a2", "b2", "az", "bz"):
            bytes_of(r["out_" + name], sent=name).wait_send()
        bytes_of(g_hbm, sent="g").wait_send()
        bytes_of(fbuf.at[pl.ds(0, (2 * far - 1) * w)], sent="f").wait_send()
        for e in range(each):

            def sent(e=e):
                for side in range(2):
                    mirror_copy(e, side).wait_send()

            when_sent(e, sent)

    meet_plane()
    swap_grads()
    t_copies += swap_tests()
    pl.when(z >= far // 2)(meet_line)
    own_copies[0].wait()
    bytes_of(gbuf.at[pl.ds(rows, rows), pl.ds(0, soon * W)], came="g0").wait_recv()
    compute(3, 0, 1)
    first(3, 1)
    pl.when(z < far // 2)(meet_line)
    swap_factor(0, 3)
    bytes_of(gbuf.at[pl.ds(rows, rows), pl.ds(soon * W, s.k - soon * W)], came="g1").wait_recv()
    compute(3, 1, 3)
    first(3, 0)
    compute(3, 3, 4)
    compute(2)
    first(2, 1)
    second(3)
    first(2, 0)
    relayed = relay_tests(t_copies)
    swap_factor(2, 1)
    early = hand_tests(t_copies)
    compute(1)
    early += hand_relayed(relayed)
    first(1, 1)
    c_first()
    third(3)
    precondition(early)
    precondition_second()
    second(2)
    first(1, 0)
    compute(0)
    c_second()
    first(0, 1)
    along_z = gather_first()
    second(1)
    first(0, 0)
    relayed = gather_relay(along_z)
    third(2)
    c_third()
    second(0)
    third(1)
    c_fourth()
    gx, gy, mate_own = gather_second(along_z, relayed)
    scores_start()
    score(0, 0, 1)
    third(0)
    diagonal = gather_third(gx, gy)
    finish(0)
    finish(1)
    direct, mirrored = finish(2)
    mates = gather_mates(gx, gy)
    score(0, 1, 3)
    arrived([mate_own] + mates)
    score(1, 0, 3)
    mate_diagonal = gather_fourth(diagonal)
    score(0, 3, 4)
    arrived([mate_diagonal])
    score(1, 3, 4)
    close(direct, mirrored)
    wait_sends()

def window(grads, covariance, test_grads, inverse_factor):
    n = lax.axis_size("dp")
    rows, k = grads.shape
    s = Sizes(n, rows, k, test_grads.shape[0])
    scratch = s.scratch()
    term, scores = pl.pallas_call(
        functools.partial(kernel, s, list(scratch)),
        out_shape=(
            jax.ShapeDtypeStruct((s.w, k), F32),
            jax.ShapeDtypeStruct((rows, s.tests), F32),
        ),
        in_specs=[pl.BlockSpec(memory_space=pltpu.HBM)] * 3,
        out_specs=(
            pl.BlockSpec(memory_space=pltpu.VMEM),
            pl.BlockSpec(memory_space=pltpu.VMEM),
        ),
        scratch_shapes=list(scratch.values()),
        compiler_params=pltpu.CompilerParams(
            collective_id=0, has_side_effects=True, vmem_limit_bytes=49 * 1024 * 1024
        ),
    )(*(pltpu.with_memory_space_constraint(a, pltpu.HBM) for a in (grads, test_grads, inverse_factor)))
    here = pl.BlockSpec(memory_space=pltpu.VMEM)
    there = pl.BlockSpec(memory_space=pl.ANY)
    return pl.pallas_call(
        functools.partial(ending, rows * n),
        out_shape=(
            jax.ShapeDtypeStruct(scores.shape, F32),
            jax.ShapeDtypeStruct(covariance.shape, F32),
        ),
        in_specs=[here, here, here],
        out_specs=(there, there),
        scratch_shapes=[
            pltpu.VMEM(covariance.shape, F32),
            pltpu.SemaphoreType.DMA((PIECES + 1,)),
        ],
        compiler_params=pltpu.CompilerParams(vmem_limit_bytes=8 * 1024 * 1024),
    )(scores, term, covariance)


PIECES = 4


def ending(examples, scores_ref, term_ref, before_ref, scores_out, after_out, after, sem):
    copies = [pltpu.make_async_copy(scores_ref, scores_out, sem.at[PIECES])]
    copies[0].start()
    piece = after.shape[0] // PIECES
    for i in range(PIECES):
        part = pl.ds(i * piece, piece)
        after[part] = 0.9 * before_ref[part] + term_ref[part] / examples
        copies.append(pltpu.make_async_copy(after.at[part], after_out.at[part], sem.at[i]))
        copies[-1].start()
    for copy in copies:
        copy.wait()


def solution(mesh):
    placed = (P("dp", "feat"), P("dp", "feat"), P("feat", "dp"), P("dp", None))
    whole = mesh.shape["feat"] == 1 and mesh.shape["dp"] == 32
    return jax.shard_map(
        window if whole else general,
        mesh=mesh,
        in_specs=placed,
        out_specs=(P("dp", "feat"), P("dp", "feat")),
        check_vma=False,
    )
```

```python
import functools

import jax
import jax.numpy as jnp
from jax import lax
from jax.experimental import pallas as pl
from jax.experimental.pallas import tpu as pltpu
from jax.sharding import PartitionSpec as P

F32 = jnp.float32
BF16 = jnp.bfloat16
MESH = pl.DeviceIdType.MESH


def general(grads, covariance, test_grads, inverse_factor):
    all_features = lax.all_gather(grads, "feat", axis=1, tiled=True)
    examples = grads.shape[0] * lax.axis_size("dp")
    tested = lax.dot_general(
        inverse_factor, test_grads, (((0,), (1,)), ((), ())), preferred_element_type=F32
    )
    term = lax.dot_general(
        all_features, grads, (((0,), (0,)), ((), ())), preferred_element_type=F32
    )
    joined = lax.psum_scatter(
        jnp.concatenate([term, tested], axis=1), "dp", scatter_dimension=0, tiled=True
    )
    width = grads.shape[1]
    owned_pre = joined[:, width:].astype(BF16)
    pre_columns = lax.all_gather(owned_pre, "dp", axis=0, tiled=True)
    scores = jnp.dot(all_features, pre_columns, preferred_element_type=F32)
    return scores, 0.9 * covariance + joined[:, :width] / examples


class Sizes:
    def __init__(self, n, rows, k, tests):
        self.n, self.rows, self.k, self.tests = n, rows, k, tests
        self.chips, self.far, self.w = n // 2, n // 8, k // n
        self.W = 2 * self.w
        self.half = self.chips // 2
        self.each = self.half // 2
        self.strip = self.each * self.W + self.w // 2
        self.rc = self.w
        self.hc = self.rc // 2
        self.hs = self.hc - self.w // 4
        self.ra = (self.strip - self.rc) // 2 + self.w // 8
        self.rb = self.strip - self.rc - self.ra
        self.mh = tests // 2

    def scratch(self):
        far, w, W, tests = self.far, self.w, self.W, self.tests
        far1 = max(far - 1, 1)
        v = pltpu.VMEM
        return dict(
            gbuf=v((2 * self.rows, self.k), BF16),
            gt=v((W, 2 * self.rows), BF16),
            tmp=v((self.strip, W), F32),
            part_a=v((far, 2, self.ra, W), F32),
            part_b=v((far, 2, self.rb, W), F32),
            out_a1=v((far, 2, self.ra, W), BF16),
            out_b1=v((far, 2, self.rb, W), BF16),
            in_a1=v((far, 2, self.ra, W), BF16),
            in_b1=v((far, 2, self.rb, W), BF16),
            out_a2=v((far, self.ra, W), BF16),
            out_b2=v((far, self.rb, W), BF16),
            in_a2=v((far, self.ra, W), BF16),
            in_b2=v((far, self.rb, W), BF16),
            out_az=v((far1, self.ra, W), BF16),
            out_bz=v((far1, self.rb, W), BF16),
            in_az=v((far1, self.ra, W), BF16),
            in_bz=v((far1, self.rb, W), BF16),
            part_c=v((2, 2, 4, self.hc, W), F32),
            out_c1=v((2, 2, 4, self.hc, W), BF16),
            in_c1=v((2, 2, 4, self.hc, W), BF16),
            out_c2=v((2, 4, self.hc, W), BF16),
            in_c2=v((2, 4, self.hc, W), BF16),
            out_c3=v((2, 2, self.hc, W), BF16),
            in_c3=v((2, 2, self.hc, W), BF16),
            out_c4=v((2, self.hc, W), BF16),
            in_c4=v((2, self.hc, W), BF16),
            extra=v((w, w), F32),
            fbuf=v((2 * far * w, 4 * w), BF16),
            tbuf=v((tests, 2 * far * w), BF16),
            pp=v((tests, 4 * w), F32),
            in_p1=v((2, 2, self.mh, w), F32),
            out_p2=v((2, self.mh, w), F32),
            in_p2=v((2, self.mh, w), F32),
            pfull=v((tests, self.k), BF16),
            msend=v((self.each, W, W), BF16),
            mrecv=v((self.half, w, W), BF16),
            xsend=v((w, w), BF16),
            xrecv=v((w, w), BF16),
            dsend=v((w, self.each * W), BF16),
            drecv=v((w, self.each * W), BF16),
            ssem=pltpu.SemaphoreType.DMA((self.sends,)),
            rsem=pltpu.SemaphoreType.DMA((self.receipts,)),
            msem=pltpu.SemaphoreType.DMA((2 * self.each,)),
            mrsem=pltpu.SemaphoreType.DMA((1,)),
            lsem=pltpu.SemaphoreType.DMA((4,)),
        )

    sends, receipts = 43, 69


def kernel(s, names, g_hbm, t_hbm, f_hbm, term_ref, scores_ref, *refs):
    r = dict(zip(names, refs))
    n, far, w, W, chips, half, each = s.n, s.far, s.w, s.W, s.chips, s.half, s.each
    rows, mh, ra, rb, hc, hs = s.rows, s.mh, s.ra, s.rb, s.hc, s.hs
    mid = ra + rb + hc
    me = lax.axis_index("dp")
    core, x, y, z = me % 2, me // 2 % 2, me // 4 % 2, me // 8
    q = me // 2

    def device(zz, yy, xx, cc):
        return ((zz * 2 + yy) * 2 + xx) * 2 + cc

    def over(g):
        return (z, z + 1 - 2 * (z % 2), (z + 2) % far, far - 1 - z)[g]

    mate = device(z, y, x, 1 - core)
    x_to = device(z, y, 1 - x, core)
    y_to = device(z, 1 - y, x, core)
    ssem, rsem = r["ssem"], r["rsem"]
    started = []
    count = [0, 0]
    shared = [{}, {}]

    def slot(kind, name):
        if name in shared[kind]:
            return shared[kind][name]
        i = count[kind]
        count[kind] += 1
        if name:
            shared[kind][name] = i
        return i

    def to(src, dst, target, start=True, sent=None, came=None):
        copy = pltpu.make_async_remote_copy(
            src_ref=src, dst_ref=dst, send_sem=ssem.at[slot(0, sent)],
            recv_sem=rsem.at[slot(1, came)], device_id={"dp": target}, device_id_type=MESH,
        )
        if start:
            copy.start()
        if not sent:
            started.append(copy)
        return copy

    def bytes_of(ref, sent=None, came=None):
        return pltpu.make_async_remote_copy(
            src_ref=ref, dst_ref=ref, send_sem=ssem.at[shared[0][sent] if sent else 0],
            recv_sem=rsem.at[shared[1][came] if came else 0],
            device_id={"dp": mate}, device_id_type=MESH,
        )

    class Either:
        def __init__(self, src, dst, small, target):
            i, j = slot(0, None), slot(1, None)
            self.copies = [
                pltpu.make_async_remote_copy(
                    src_ref=a, dst_ref=b, send_sem=ssem.at[i], recv_sem=rsem.at[j],
                    device_id={"dp": target}, device_id_type=MESH,
                )
                for a, b in ((src.at[small], dst.at[small]), (src, dst))
            ]
            started.append(self)
            self.each(lambda copy: copy.start())

        def each(self, act):
            for i in range(2):
                pl.when(core == i)(functools.partial(act, self.copies[i]))

        def wait_recv(self):
            self.each(lambda copy: copy.wait_recv())

        def wait_send(self):
            self.each(lambda copy: copy.wait_send())

    def lanes(block, width):
        return pl.ds(pl.multiple_of(block * width, width), width)

    gbuf, fbuf, tbuf = r["gbuf"], r["fbuf"], r["tbuf"]
    own_copies = [
        pltpu.make_async_copy(g_hbm, gbuf.at[pl.ds(0, rows)], r["lsem"].at[0]),
        pltpu.make_async_copy(t_hbm, tbuf.at[:, pl.ds(0, w)], r["lsem"].at[1]),
        pltpu.make_async_copy(
            f_hbm.at[:, lanes(core * far + z, 4 * w)], fbuf.at[pl.ds(0, w)], r["lsem"].at[2]
        ),
    ]

    barrier = pltpu.get_barrier_semaphore()

    def greet(targets):
        for target in targets:
            pl.semaphore_signal(barrier, inc=1, device_id={"dp": target}, device_id_type=MESH)

    def meet_plane():
        greet([mate, x_to, y_to])
        for copy in own_copies:
            copy.start()
        pl.semaphore_wait(barrier, 3 + z)
        greet([device(over(g), y, x, core) for g in range(1, far)])

    t_copies = []

    def meet_line():
        @pl.when(z < far - 1)
        def _():
            pl.semaphore_wait(barrier, far - 1 - z)

        for copy in t_copies:
            copy.start()

    soon = half // 2 + 2

    def swap_grads():
        there = 1 - core
        begin = (over(3) * 2 + 1 - y) * 2 + 1 - x
        last = half // 2
        steps = [0] + [i + (last - 1) * there for i in range(1, last)]
        steps += [half - there, last + last * there]
        steps += [i - last * there for i in range(last + 1, half)] + list(range(half + 1, chips))
        parts = [lanes((begin + i) % chips, W) for i in steps]
        for i, part in enumerate(parts):
            to(
                g_hbm.at[:, part], gbuf.at[pl.ds(rows, rows), part], mate,
                sent="g", came="g0" if i < 3 else "g1" if i < soon else "g2",
            )

    def hand(g, target, came):
        return to(tbuf.at[:, pl.ds(2 * g * w, w)], tbuf.at[:, pl.ds(came * w, w)], target)

    def swap_tests():
        return [
            to(t_hbm, tbuf.at[:, pl.ds(2 * g * w, w)], device(over(g), y, x, core), False)
            for g in (1, 2)
        ]

    def swap_factor(*groups):
        return [
            to(
                f_hbm.at[:, lanes((core + h) % 2 * far + over(g), 4 * w)],
                fbuf.at[pl.ds((2 * g + h) * w, w)],
                device(over(g), y, x, (core + h) % 2),
                sent="f", came="f",
            )
            for g in groups
            for h in range(2)
            if g or h
        ]

    def relay_tests(copies):
        copies[1].wait_recv()
        return hand(2, device(over(1), y, x, core), 6)

    def hand_tests(copies):
        own_copies[1].wait()
        copies[0].wait_recv()
        return [hand(g, mate, 2 * g + 1) for g in range(3)]

    def hand_relayed(copy):
        copy.wait_recv()
        return [hand(3, mate, 7)]

    def arrived(copies):
        for copy in copies:
            copy.wait_recv()

    gt, tmp = r["gt"], r["tmp"]
    part_c, out_c1, in_c1, out_c2, in_c2 = (
        r["part_c"], r["out_c1"], r["in_c1"], r["out_c2"], r["in_c2"]
    )
    out_c3, in_c3, out_c4, in_c4 = r["out_c3"], r["in_c3"], r["out_c4"], r["in_c4"]
    part_a, part_b, out_a1, out_b1 = r["part_a"], r["part_b"], r["out_a1"], r["out_b1"]

    def owner(g, i):
        oy, ox = (3 - i) // 2, (3 - i) % 2
        return oy, ox, (over(g) * 2 + (y + oy) % 2) * 2 + (x + ox) % 2

    def superblocks(own, which):
        for e in which:
            col = (own + core * each + e) % chips
            tmp[e * W : (e + 1) * W] = jnp.dot(
                gt[...], gbuf[:, lanes(col, W)], preferred_element_type=F32
            )

    def last_rows(g, i, own):
        col = 2 * ((own + half) % chips) + (core + own // half) % 2
        extra = jnp.dot(
            gt[pl.ds(pl.multiple_of(core * w, w), w), :], gbuf[:, lanes(col, w)],
            preferred_element_type=F32,
        )

        @pl.when(core == 0)
        def _():
            tmp[w:W, :w] = extra
            tmp[mid : mid + hs] = tmp[each * W - hs : each * W]

        @pl.when(core == 1)
        def _():
            tmp[each * W :, :w] = extra[: w // 2]
            tmp[each * W :, w:] = extra[w // 2 :]

        for h in range(2):
            ends = tmp[ra + rb + h * hc : ra + rb + (h + 1) * hc]
            if g % 2:
                out_c1[g // 2, h, 3 - i] = ends.astype(BF16)
            else:
                part_c[g // 2, h, 3 - i] = ends

    def compute_first(g):
        oy, ox, own = owner(g, 0)
        bytes_of(gbuf.at[pl.ds(rows, rows), pl.ds(0, 3 * W)], came="g0").wait_recv()
        gt[...] = gbuf[:, lanes(own, W)].T
        superblocks(own, range(each // 2))
        bytes_of(gbuf.at[pl.ds(rows, rows), pl.ds(0, (soon - 3) * W)], came="g1").wait_recv()
        col = 2 * ((own + half) % chips) + core + own // half

        @pl.when(core == 0)
        def _():
            tmp[w:W, :w] = jnp.dot(
                gt[:w, :], gbuf[:, lanes(col, w)], preferred_element_type=F32
            )

        out_a1[g, 1] = tmp[:ra].astype(BF16)
        a1[g, 1] = to(out_a1.at[g, 1], r["in_a1"].at[g, 1], x_to, sent="a1")
        superblocks(own, range(each // 2, each))
        out_b1[g, 1] = tmp[ra : ra + rb].astype(BF16)
        b1[g, 1] = to(out_b1.at[g, 1], r["in_b1"].at[g, 1], y_to, sent="b1")
        last_rows(g, 0, own)

    def compute(g, first=0, last=4):
        def strip(i, carry):
            oy, ox, own = owner(g, i)
            gt[...] = gbuf[:, lanes(own, W)].T
            superblocks(own, range(each))
            last_rows(g, i, own)

            @pl.when(ox == 0)
            def _():
                part_a[g, oy] = tmp[:ra]

            @pl.when(ox == 1)
            def _():
                out_a1[g, oy] = tmp[:ra].astype(BF16)

            @pl.when(oy == 0)
            def _():
                part_b[g, ox] = tmp[ra : ra + rb]

            @pl.when(oy == 1)
            def _():
                out_b1[g, ox] = tmp[ra : ra + rb].astype(BF16)

            return carry

        lax.fori_loop(first, last, strip, 0)

    a1, b1, a2, b2, az, bz = {}, {}, {}, {}, {}, {}

    def first(g, o):
        a1[g, o] = to(out_a1.at[g, o], r["in_a1"].at[g, o], x_to, sent="a1")
        b1[g, o] = to(out_b1.at[g, o], r["in_b1"].at[g, o], y_to, sent="b1")

    def second(g):
        a1[g, 1].wait_recv()
        r["out_a2"][g] = (part_a[g, 1] + r["in_a1"][g, 1].astype(F32)).astype(BF16)
        a2[g] = to(r["out_a2"].at[g], r["in_a2"].at[g], y_to, sent="a2")
        b1[g, 1].wait_recv()
        r["out_b2"][g] = (part_b[g, 1] + r["in_b1"][g, 1].astype(F32)).astype(BF16)
        b2[g] = to(r["out_b2"].at[g], r["in_b2"].at[g], x_to, sent="b2")

    def third(g):
        target = device(over(2 if g == 2 else 1), y, x, core)
        at = {3: 2, 2: 1, 1: 0, 0: 0}[g]
        for name, part, one, two, along in (
            ("a", part_a, a1, a2, az), ("b", part_b, b1, b2, bz)
        ):
            one[g, 0].wait_recv()
            two[g].wait_recv()
            total = (
                part[g, 0] + r[f"in_{name}1"][g, 0].astype(F32) + r[f"in_{name}2"][g].astype(F32)
            )
            if g == 0:
                part[0, 0] = total
                continue
            out, came = r[f"out_{name}z"], r[f"in_{name}z"]
            if g == 2:
                along[3].wait_recv()
                total = total + came[2].astype(F32)
            out[at] = total.astype(BF16)
            along[g] = to(out.at[at], came.at[at], target, sent=name + "z")

    c1, c2, c3, c4 = {}, [], {}, {}
    few = pl.ds(0, hs)

    def c_first():
        for at in (1, 0):
            c1[at] = Either(
                out_c1.at[at], in_c1.at[at], (slice(None), slice(None), few),
                device(over(1), y, x, core),
            )

    def c_second():
        c1[1].wait_recv()
        out_c2[...] = (part_c[1] + in_c1[1].astype(F32)).astype(BF16)
        c2.append(
            Either(out_c2, in_c2, (slice(None), slice(None), few), device(over(2), y, x, core))
        )

    def c_third():
        c1[0].wait_recv()
        c2[0].wait_recv()
        part_c[0] = part_c[0] + in_c1[0].astype(F32) + in_c2[...].astype(F32)
        for o in range(2):
            out_c3[0, o] = part_c[0, 0, 2 * o + 1].astype(BF16)
            out_c3[1, o] = part_c[0, 1, 2 + o].astype(BF16)
        for h, target in ((0, x_to), (1, y_to)):
            c3[h] = Either(out_c3.at[h], in_c3.at[h], (slice(None), few), target)

    def c_fourth():
        for h, target in ((0, y_to), (1, x_to)):
            c3[h].wait_recv()
            out_c4[h] = (part_c[0, h, 2 - h] + in_c3[h, 1].astype(F32)).astype(BF16)
            c4[h] = Either(out_c4.at[h], in_c4.at[h], (few,), target)

    pp, in_p1, out_p2, in_p2, pfull = r["pp"], r["in_p1"], r["out_p2"], r["in_p2"], r["pfull"]
    sub = lambda oy, ox: (y + oy) % 2 * 2 + (x + ox) % 2
    p1, p2 = {}, {}

    def precondition(handed):
        own_copies[2].wait()
        bytes_of(fbuf.at[pl.ds(0, (2 * far - 1) * w)], came="f").wait_recv()
        for copy in handed:
            copy.wait_recv()
        pp[...] = jnp.dot(tbuf[...], fbuf[...], preferred_element_type=F32)
        for o in (1, 0):
            p1[0, o] = to(pp.at[pl.ds(0, mh), lanes(sub(o, 1), w)], in_p1.at[0, o], x_to)
            p1[1, o] = to(pp.at[pl.ds(mh, mh), lanes(sub(1, o), w)], in_p1.at[1, o], y_to)

    def precondition_second():
        p1[0, 1].wait_recv()
        out_p2[0] = pp[:mh, lanes(sub(1, 0), w)] + in_p1[0, 1]
        p2[0] = to(out_p2.at[0], in_p2.at[0], y_to)
        p1[1, 1].wait_recv()
        out_p2[1] = pp[mh:, lanes(sub(0, 1), w)] + in_p1[1, 1]
        p2[1] = to(out_p2.at[1], in_p2.at[1], x_to)

    def place(oy, ox, part=0, parts=1):
        return lanes((core * 4 + sub(oy, ox)) * parts + part, far * w // parts)

    def pass_on(where, target):
        return to(pfull.at[:, where], pfull.at[:, where], target)

    def gather_first():
        p1[0, 0].wait_recv()
        p2[0].wait_recv()
        own = lanes((core * 4 + sub(0, 0)) * far + z, w)
        pfull[:mh, own] = (pp[:mh, lanes(sub(0, 0), w)] + in_p1[0, 0] + in_p2[0]).astype(BF16)
        p1[1, 0].wait_recv()
        p2[1].wait_recv()
        pfull[mh:, own] = (pp[mh:, lanes(sub(0, 0), w)] + in_p1[1, 0] + in_p2[1]).astype(BF16)
        return [pass_on(own, device(over(g), y, x, core)) for g in (1, 2)]

    def gather_relay(along_z):
        along_z[1].wait_recv()
        there = lanes((core * 4 + sub(0, 0)) * far + over(2), w)
        return pass_on(there, device(over(1), y, x, core))

    def gather_second(along_z, relayed):
        along_z[0].wait_recv()
        relayed.wait_recv()
        gx = [pass_on(place(0, 0, i, 2), x_to) for i in range(2)]
        gy = [pass_on(place(0, 0, i, 2), y_to) for i in (1, 0)]
        return gx, gy, pass_on(place(0, 0), mate)

    def gather_third(gx, gy):
        gx[0].wait_recv()
        diagonal = [pass_on(place(0, 1, 0, 2), y_to)]
        gy[0].wait_recv()
        return diagonal + [pass_on(place(1, 0, 1, 2), x_to)]

    def gather_mates(gx, gy):
        gx[1].wait_recv()
        mates = [pass_on(place(0, 1), mate)]
        gy[1].wait_recv()
        return mates + [pass_on(place(1, 0), mate)]

    def gather_fourth(diagonal):
        for copy in diagonal:
            copy.wait_recv()
        return pass_on(place(1, 1), mate)

    def score(other, first, last):
        def chunk(i, carry):
            cc, at = (core + other) % 2, sub(i // 2, i % 2)
            left = jnp.concatenate(
                [gbuf[:rows, lanes((cc * far + zz) * 4 + at, w)] for zz in range(far)], axis=1
            )
            scores_ref[...] += lax.dot_general(
                left, pfull[:, lanes(cc * 4 + at, far * w)], (((1,), (1,)), ((), ())),
                preferred_element_type=F32,
            )
            return carry

        lax.fori_loop(first, last, chunk, 0)

    def scores_start():
        scores_ref[...] = jnp.zeros_like(scores_ref)

    msend, mrecv, msem, mrsem = r["msend"], r["mrecv"], r["msem"], r["mrsem"]
    dsend, drecv, xsend, xrecv = r["dsend"], r["drecv"], r["xsend"], r["xrecv"]

    def mirror_copy(e, side):
        d = core * each + e
        return pltpu.make_async_remote_copy(
            src_ref=msend.at[e, pl.ds(side * w, w)], dst_ref=mrecv.at[d],
            send_sem=msem.at[2 * e + side], recv_sem=mrsem.at[0],
            device_id={"dp": 2 * ((q + d) % chips) + side}, device_id_type=MESH,
        )

    def when_sent(e, act):
        if e:
            act()
        else:
            pl.when(core == 1)(act)

    def finish(part):
        if part < 2:
            sums, came, copies, size = (
                (part_a, r["in_az"], az, ra), (part_b, r["in_bz"], bz, rb)
            )[part]
            at = part * ra
            for g in (1, 2):
                copies[g].wait_recv()
            tmp[at : at + size] = sums[0, 0] + came[0].astype(F32) + came[1].astype(F32)
        else:
            at, size = ra + rb, s.rc
            for h in range(2):
                c4[h].wait_recv()
                tmp[at + h * hc : at + (h + 1) * hc] = (
                    part_c[0, h, 0] + in_c3[h, 0].astype(F32) + in_c4[h].astype(F32)
                )
            extra = r["extra"]

            @pl.when(core == 0)
            def _():
                tmp[each * W - hs : each * W] = tmp[mid : mid + hs]
                extra[...] = tmp[w:W, :w]

            @pl.when(core == 1)
            def _():
                extra[: w // 2] = tmp[each * W :, :w]
                extra[w // 2 :] = tmp[each * W :, w:]

        for e in range(each):
            if not at < (e + 1) * W <= at + size:
                continue
            msend[e] = tmp[e * W : (e + 1) * W].T.astype(BF16)

            def send(e=e):
                for side in range(2):
                    mirror_copy(e, side).start()

            when_sent(e, send)
            where = lanes((q + core * each + e) % chips, W)
            term_ref[:, where] = tmp[pl.ds(pl.multiple_of(e * W + core * w, w), w), :]
            other = pl.ds(pl.multiple_of(e * W + (1 - core) * w, w), w)
            dsend[:, e * W : (e + 1) * W] = tmp[other, :].astype(BF16)
            if e == 0:

                @pl.when(core == 0)
                def _():
                    dsend[:, :w] = tmp[:w, w:W].T.astype(BF16)

        if part < 2:
            return None
        direct = to(dsend, drecv, mate)
        col = 2 * ((q + half) % chips) + (core + q // half) % 2
        term_ref[:, lanes(col, w)] = extra[...]
        xsend[...] = extra[...].T.astype(BF16)
        mirrored = to(xsend, xrecv, col)
        return direct, mirrored

    def close(direct, mirrored):
        direct.wait_recv()
        for e in range(each):
            where = lanes((q + (1 - core) * each + e) % chips, W)
            term_ref[:, where] = drecv[:, e * W : (e + 1) * W].astype(F32)
        all_of_them = mrecv.at[pl.ds(1, half - 1)]
        pltpu.make_async_remote_copy(
            src_ref=all_of_them, dst_ref=all_of_them, send_sem=msem.at[0], recv_sem=mrsem.at[0],
            device_id={"dp": mate}, device_id_type=MESH,
        ).wait_recv()
        for d in range(1, half):
            term_ref[:, lanes((q + chips - d) % chips, W)] = mrecv[d].astype(F32)
        mirrored.wait_recv()
        far_chip = (q + half) % chips
        col = 2 * far_chip + (core + far_chip // half) % 2
        term_ref[:, lanes(col, w)] = xrecv[...].astype(F32)

    def wait_sends():
        assert count == [s.sends, s.receipts]
        for copy in started:
            copy.wait_send()
        for name in ("a1", "b1", "a2", "b2", "az", "bz"):
            bytes_of(r["out_" + name], sent=name).wait_send()
        bytes_of(g_hbm, sent="g").wait_send()
        bytes_of(fbuf.at[pl.ds(0, (2 * far - 1) * w)], sent="f").wait_send()
        for e in range(each):

            def sent(e=e):
                for side in range(2):
                    mirror_copy(e, side).wait_send()

            when_sent(e, sent)

    meet_plane()
    swap_grads()
    t_copies += swap_tests()
    pl.when(z >= far // 2)(meet_line)
    own_copies[0].wait()
    compute_first(3)
    pl.when(z < far // 2)(meet_line)
    swap_factor(0, 3)
    bytes_of(gbuf.at[pl.ds(rows, rows), pl.ds(soon * W, s.k - soon * W)], came="g2").wait_recv()
    compute(3, 1, 3)
    first(3, 0)
    compute(3, 3, 4)
    compute(2)
    first(2, 1)
    second(3)
    first(2, 0)
    relayed = relay_tests(t_copies)
    swap_factor(2, 1)
    early = hand_tests(t_copies)
    compute(1)
    early += hand_relayed(relayed)
    first(1, 1)
    c_first()
    third(3)
    precondition(early)
    precondition_second()
    second(2)
    first(1, 0)
    compute(0)
    first(0, 1)
    c_second()
    second(1)
    along_z = gather_first()
    first(0, 0)
    relayed = gather_relay(along_z)
    third(2)
    c_third()
    second(0)
    third(1)
    c_fourth()
    gx, gy, mate_own = gather_second(along_z, relayed)
    scores_start()
    score(0, 0, 1)
    third(0)
    diagonal = gather_third(gx, gy)
    finish(0)
    finish(1)
    direct, mirrored = finish(2)
    mates = gather_mates(gx, gy)
    score(0, 1, 3)
    arrived([mate_own] + mates)
    score(1, 0, 3)
    mate_diagonal = gather_fourth(diagonal)
    score(0, 3, 4)
    arrived([mate_diagonal])
    score(1, 3, 4)
    close(direct, mirrored)
    wait_sends()

def window(grads, covariance, test_grads, inverse_factor):
    n = lax.axis_size("dp")
    rows, k = grads.shape
    s = Sizes(n, rows, k, test_grads.shape[0])
    scratch = s.scratch()
    term, scores = pl.pallas_call(
        functools.partial(kernel, s, list(scratch)),
        out_shape=(
            jax.ShapeDtypeStruct((s.w, k), F32),
            jax.ShapeDtypeStruct((rows, s.tests), F32),
        ),
        in_specs=[pl.BlockSpec(memory_space=pltpu.HBM)] * 3,
        out_specs=(
            pl.BlockSpec(memory_space=pltpu.VMEM),
            pl.BlockSpec(memory_space=pltpu.VMEM),
        ),
        scratch_shapes=list(scratch.values()),
        compiler_params=pltpu.CompilerParams(
            collective_id=0, has_side_effects=True, vmem_limit_bytes=49 * 1024 * 1024
        ),
    )(*(pltpu.with_memory_space_constraint(a, pltpu.HBM) for a in (grads, test_grads, inverse_factor)))
    here = pl.BlockSpec(memory_space=pltpu.VMEM)
    there = pl.BlockSpec(memory_space=pl.ANY)
    return pl.pallas_call(
        functools.partial(ending, rows * n),
        out_shape=(
            jax.ShapeDtypeStruct(scores.shape, F32),
            jax.ShapeDtypeStruct(covariance.shape, F32),
        ),
        in_specs=[here, here, here],
        out_specs=(there, there),
        scratch_shapes=[
            pltpu.VMEM(covariance.shape, F32),
            pltpu.SemaphoreType.DMA((PIECES + 1,)),
        ],
        compiler_params=pltpu.CompilerParams(vmem_limit_bytes=8 * 1024 * 1024),
    )(scores, term, covariance)


PIECES = 4


def ending(examples, scores_ref, term_ref, before_ref, scores_out, after_out, after, sem):
    copies = [pltpu.make_async_copy(scores_ref, scores_out, sem.at[PIECES])]
    copies[0].start()
    piece = after.shape[0] // PIECES
    for i in range(PIECES):
        part = pl.ds(i * piece, piece)
        after[part] = 0.9 * before_ref[part] + term_ref[part] / examples
        copies.append(pltpu.make_async_copy(after.at[part], after_out.at[part], sem.at[i]))
        copies[-1].start()
    for copy in copies:
        copy.wait()


def solution(mesh):
    placed = (P("dp", "feat"), P("dp", "feat"), P("feat", "dp"), P("dp", None))
    whole = mesh.shape["feat"] == 1 and mesh.shape["dp"] == 32
    return jax.shard_map(
        window if whole else general,
        mesh=mesh,
        in_specs=placed,
        out_specs=(P("dp", "feat"), P("dp", "feat")),
        check_vma=False,
    )
```
